32 devices in a mesh: dp: 1 (over z), tp: 32 (over y, x, core).
Axes of the slice: x: 4, y: 4, z: 1, core: 2. Of those that a mesh axis runs over, the one named last changes fastest.
The devices are a block of a 4x4x8 slice.
Arguments:
- x_saved: bfloat16 [2, 1024, 3072], P('dp')
- h1_saved: bfloat16 [2, 1024, 3072], P('dp')
- grad_y: bfloat16 [2, 1024, 3072], P('dp')
- mean_one: float32 [2, 1024], P('dp')
- rstd_one: float32 [2, 1024], P('dp')
- mean_two: float32 [2, 1024], P('dp')
- rstd_two: float32 [2, 1024], P('dp')
- gain_one: bfloat16 [3072], replicated
- gain_two: bfloat16 [3072], replicated
- w_qkv: bfloat16 [3072, 32, 3, 96], P(None, 'tp')
- w_out: bfloat16 [32, 96, 3072], P('tp')
- w_up: bfloat16 [3072, 12288], P(None, 'tp')
- w_down: bfloat16 [12288, 3072], P('tp')
Outputs:
- output 1: bfloat16 [2, 1024, 3072], P('dp')
- output 2: bfloat16 [3072, 32, 3, 96], P('dp', 'tp')
- output 3: bfloat16 [32, 96, 3072], P(('dp', 'tp'))
- output 4: bfloat16 [3072, 12288], P('dp', 'tp')
- output 5: bfloat16 [12288, 3072], P(('dp', 'tp'))
All inputs are finite; a program needn't handle non-finite values.
Results may differ from the reference program's by a relative error of at most 0.0199183.
Values are sent between devices in bfloat16 or wider.
A program may use at most 768 MiB of HBM per device.

```python
import math
import jax
import jax.numpy as jnp
from jax import lax
from functools import partial

HIDDEN = 3072
NUM_HEADS = 32
FFN_DIM = 12288
SEQ_LEN = 1024
MICROBATCHES = 2

HEAD_DIM = HIDDEN // NUM_HEADS
TOKENS = MICROBATCHES * SEQ_LEN
GELU_C = 0.7978845608028654
GELU_A = 0.044715
NORM_EPS = 1e-5
wide_dot = partial(jnp.dot, preferred_element_type=jnp.float32)


def row_stats(acts):
    row_vals = acts.astype(jnp.float32)
    row_mean = jnp.mean(row_vals, axis=-1)
    row_var = jnp.mean(jnp.square(row_vals - row_mean[..., None]), axis=-1)
    return row_mean, lax.rsqrt(row_var + NORM_EPS)


def setup_inputs(seed: int = 0, part: int = 0) -> dict:
    shared_key, part_root = jax.random.split(jax.random.key(seed))
    act_keys = jax.random.split(jax.random.fold_in(part_root, part), 7)
    weight_keys = jax.random.split(shared_key, 6)
    act_shape = (MICROBATCHES, SEQ_LEN, HIDDEN)
    row_shape = (MICROBATCHES, SEQ_LEN, 1)
    x_saved = (jax.random.normal(act_keys[0], row_shape)
               + jax.random.uniform(act_keys[1], row_shape, minval=0.5, maxval=2.0)
               * jax.random.normal(act_keys[2], act_shape)).astype(jnp.bfloat16)
    h1_saved = (0.5 * jax.random.normal(act_keys[3], row_shape)
                + jax.random.uniform(act_keys[4], row_shape, minval=0.4, maxval=1.2)
                * jax.random.normal(act_keys[5], act_shape)).astype(jnp.bfloat16)
    grad_y = jax.random.normal(act_keys[6], act_shape).astype(jnp.bfloat16)
    mean_one, rstd_one = row_stats(x_saved)
    mean_two, rstd_two = row_stats(h1_saved)
    gain_one = jax.random.uniform(weight_keys[0], (HIDDEN,), minval=0.5, maxval=1.5).astype(jnp.bfloat16)
    gain_two = jax.random.uniform(weight_keys[1], (HIDDEN,), minval=0.5, maxval=1.5).astype(jnp.bfloat16)
    qk_gain = math.sqrt(math.log(SEQ_LEN))
    head_gain = jnp.array([qk_gain, 1.0, 1.0], dtype=jnp.float32)[:, None]
    w_qkv = (jax.random.normal(weight_keys[2], (HIDDEN, NUM_HEADS, 3, HEAD_DIM)) * head_gain
             * HIDDEN ** -0.5).astype(jnp.bfloat16)
    w_out = (jax.random.normal(weight_keys[3], (NUM_HEADS, HEAD_DIM, HIDDEN)) * HIDDEN ** -0.5).astype(jnp.bfloat16)
    w_up = (jax.random.normal(weight_keys[4], (HIDDEN, FFN_DIM)) * HIDDEN ** -0.5).astype(jnp.bfloat16)
    w_down = (jax.random.normal(weight_keys[5], (FFN_DIM, HIDDEN)) * FFN_DIM ** -0.5).astype(jnp.bfloat16)
    return {'x_saved': x_saved, 'h1_saved': h1_saved, 'grad_y': grad_y,
            'mean_one': mean_one, 'rstd_one': rstd_one, 'mean_two': mean_two, 'rstd_two': rstd_two,
            'gain_one': gain_one, 'gain_two': gain_two,
            'w_qkv': w_qkv, 'w_out': w_out, 'w_up': w_up, 'w_down': w_down}


def gelu_tanh(pre_act):
    inner_arg = GELU_C * (pre_act + GELU_A * pre_act * pre_act * pre_act)
    return 0.5 * pre_act * (1.0 + jnp.tanh(inner_arg))


def gelu_slope(pre_act):
    inner_arg = GELU_C * (pre_act + GELU_A * pre_act * pre_act * pre_act)
    tanh_val = jnp.tanh(inner_arg)
    return (0.5 * (1.0 + tanh_val)
            + 0.5 * pre_act * (1.0 - tanh_val * tanh_val) * GELU_C * (1.0 + 3.0 * GELU_A * pre_act * pre_act))


def norm_backward(grad_norm, xhat, gain, rstd):
    scaled = grad_norm * gain.astype(jnp.float32)
    mean_scaled = jnp.mean(scaled, axis=-1, keepdims=True)
    mean_cross = jnp.mean(scaled * xhat, axis=-1, keepdims=True)
    return rstd[..., None] * (scaled - mean_scaled - xhat * mean_cross)


def head_backward(operands):
    q_heads, k_heads, v_heads, grad_o = operands
    score_scale = HEAD_DIM ** -0.5
    scores = wide_dot(q_heads, k_heads.T) * score_scale
    causal = jnp.arange(SEQ_LEN)[:, None] >= jnp.arange(SEQ_LEN)[None, :]
    attn_prob = jax.nn.softmax(jnp.where(causal, scores, -1e30), axis=-1)
    prob_bf16 = attn_prob.astype(jnp.bfloat16)
    attn_out = wide_dot(prob_bf16, v_heads).astype(jnp.bfloat16)
    grad_v = wide_dot(prob_bf16.T, grad_o).astype(jnp.bfloat16)
    grad_p = wide_dot(grad_o, v_heads.T)
    row_dot = jnp.sum(attn_prob * grad_p, axis=-1, keepdims=True)
    grad_s = (attn_prob * (grad_p - row_dot) * score_scale).astype(jnp.bfloat16)
    grad_q = wide_dot(grad_s, k_heads).astype(jnp.bfloat16)
    grad_k = wide_dot(grad_s.T, q_heads).astype(jnp.bfloat16)
    return attn_out, jnp.stack([grad_q, grad_k, grad_v], axis=1)


def split_heads(rows):
    return rows.reshape(MICROBATCHES, SEQ_LEN, NUM_HEADS, HEAD_DIM).transpose(0, 2, 1, 3).reshape(
        MICROBATCHES * NUM_HEADS, SEQ_LEN, HEAD_DIM)


def reference(x_saved, h1_saved, grad_y, mean_one, rstd_one, mean_two, rstd_two,
              gain_one, gain_two, w_qkv, w_out, w_up, w_down):
    x_rows = x_saved.reshape(TOKENS, HIDDEN)
    h1_rows = h1_saved.reshape(TOKENS, HIDDEN)
    dy_rows = grad_y.reshape(TOKENS, HIDDEN)
    xhat_two = (h1_rows.astype(jnp.float32) - mean_two.reshape(TOKENS, 1)) * rstd_two.reshape(TOKENS, 1)
    norm_two = (xhat_two * gain_two.astype(jnp.float32)).astype(jnp.bfloat16)
    pre_act = wide_dot(norm_two, w_up)
    act_out = gelu_tanh(pre_act).astype(jnp.bfloat16)
    grad_down = wide_dot(act_out.T, dy_rows).astype(jnp.bfloat16)
    grad_pre = (wide_dot(dy_rows, w_down.T) * gelu_slope(pre_act)).astype(jnp.bfloat16)
    grad_up = wide_dot(norm_two.T, grad_pre).astype(jnp.bfloat16)
    grad_norm_two = wide_dot(grad_pre, w_up.T)
    grad_h1 = (dy_rows.astype(jnp.float32)
               + norm_backward(grad_norm_two, xhat_two, gain_two, rstd_two.reshape(TOKENS))).astype(jnp.bfloat16)
    xhat_one = (x_rows.astype(jnp.float32) - mean_one.reshape(TOKENS, 1)) * rstd_one.reshape(TOKENS, 1)
    norm_one = (xhat_one * gain_one.astype(jnp.float32)).astype(jnp.bfloat16)
    qkv_flat = w_qkv.reshape(HIDDEN, 3 * HIDDEN)
    qkv_acts = wide_dot(norm_one, qkv_flat).astype(jnp.bfloat16).reshape(TOKENS, NUM_HEADS, 3, HEAD_DIM)
    grad_o = wide_dot(grad_h1, w_out.reshape(HIDDEN, HIDDEN).T).astype(jnp.bfloat16)
    attn_heads, grad_heads = lax.map(head_backward, (split_heads(qkv_acts[:, :, 0]), split_heads(qkv_acts[:, :, 1]),
                                                     split_heads(qkv_acts[:, :, 2]), split_heads(grad_o)))
    attn_rows = attn_heads.reshape(MICROBATCHES, NUM_HEADS, SEQ_LEN, HEAD_DIM).transpose(0, 2, 1, 3).reshape(
        TOKENS, HIDDEN)
    grad_qkv = grad_heads.reshape(MICROBATCHES, NUM_HEADS, SEQ_LEN, 3, HEAD_DIM).transpose(0, 2, 1, 3, 4).reshape(
        TOKENS, 3 * HIDDEN)
    grad_out_w = wide_dot(attn_rows.T, grad_h1).astype(jnp.bfloat16).reshape(NUM_HEADS, HEAD_DIM, HIDDEN)
    grad_qkv_w = wide_dot(norm_one.T, grad_qkv).astype(jnp.bfloat16).reshape(HIDDEN, NUM_HEADS, 3, HEAD_DIM)
    grad_norm_one = wide_dot(grad_qkv, qkv_flat.T)
    grad_x = (grad_h1.astype(jnp.float32)
              + norm_backward(grad_norm_one, xhat_one, gain_one, rstd_one.reshape(TOKENS))).astype(jnp.bfloat16)
    return grad_x.reshape(MICROBATCHES, SEQ_LEN, HIDDEN), grad_qkv_w, grad_out_w, grad_up, grad_down
```

```python
import math
import jax
import jax.numpy as jnp
from jax import lax
from jax.experimental import pallas as pl
from jax.experimental.pallas import tpu as pltpu
from jax.sharding import PartitionSpec as P
from functools import partial

GELU_C = 0.7978845608028654
GELU_A = 0.044715
F32 = jnp.float32
BF16 = jnp.bfloat16
ANY = pl.ANY
VMEM = pltpu.VMEM
wide_einsum = partial(jnp.einsum, preferred_element_type=F32)


def gelu_tanh(pre_act):
    inner_arg = GELU_C * (pre_act + GELU_A * pre_act * pre_act * pre_act)
    return 0.5 * pre_act * (1.0 + jnp.tanh(inner_arg))


def gelu_slope(pre_act):
    inner_arg = GELU_C * (pre_act + GELU_A * pre_act * pre_act * pre_act)
    tanh_val = jnp.tanh(inner_arg)
    return (0.5 * (1.0 + tanh_val)
            + 0.5 * pre_act * (1.0 - tanh_val * tanh_val) * GELU_C * (1.0 + 3.0 * GELU_A * pre_act * pre_act))


def attention_backward(q_heads, k_heads, v_heads, grad_o, score_scale):
    seq_len = q_heads.shape[1]
    scores = wide_einsum('bqnd,bknd->bnqk', q_heads, k_heads) * score_scale
    causal = jnp.arange(seq_len)[:, None] >= jnp.arange(seq_len)[None, :]
    attn_prob = jax.nn.softmax(jnp.where(causal, scores, -1e30), axis=-1)
    prob_bf16 = attn_prob.astype(BF16)
    attn_out = wide_einsum('bnqk,bknd->bqnd', prob_bf16, v_heads).astype(BF16)
    grad_v = wide_einsum('bnqk,bqnd->bknd', prob_bf16, grad_o).astype(BF16)
    grad_p = wide_einsum('bqnd,bknd->bnqk', grad_o, v_heads)
    row_dot = jnp.sum(attn_prob * grad_p, axis=-1, keepdims=True)
    grad_s = (attn_prob * (grad_p - row_dot) * score_scale).astype(BF16)
    grad_q = wide_einsum('bnqk,bknd->bqnd', grad_s, k_heads).astype(BF16)
    grad_k = wide_einsum('bnqk,bqnd->bknd', grad_s, q_heads).astype(BF16)
    return attn_out, jnp.stack([grad_q, grad_k, grad_v], axis=3)


NB = 2
SEMS = 32


class Comm:
    def __init__(self, n, rows, cols):
        self.side = math.isqrt(n // 2)
        assert self.side == 4 and 2 * self.side * self.side == n
        self.rows, self.cols = rows, cols
        self.blk = rows // NB
        self.half = self.blk // 2
        self.l1 = self.half // self.side
        self.l2 = self.l1 // self.side
        self.hw = cols // 2

    def scratch(self):
        l1, l2, w, hw = self.l1, self.l2, self.cols, self.hw
        return [
            VMEM((NB, self.half, w), BF16),
            VMEM((NB, self.half, w), BF16),
            VMEM((NB, 6, l1, hw), BF16),
            VMEM((NB, 6, l2, hw), BF16),
            VMEM((self.rows, w), BF16),
            VMEM((NB, l2, w), BF16),
            VMEM((NB, l2, w), BF16),
            VMEM((NB, l2, 8), F32),
            pltpu.SemaphoreType.DMA((NB, SEMS)),
            pltpu.SemaphoreType.DMA((NB, SEMS)),
            pltpu.SemaphoreType.DMA((NB, 8)),
        ]

    N_SCRATCH = 11

    def bind(self, part, saved, resid, stats, gain, out, scratch, mb, stat_col):
        (self.own, self.pair, self.ring1, self.ring2, self.full, self.zrow, self.rrow, self.srow,
         self.ssem, self.rsem, self.lsem) = scratch
        self.part, self.saved, self.resid, self.stats, self.gain, self.out = part, saved, resid, stats, gain, out
        self.mb, self.stat_col = mb, stat_col
        side = self.side
        me = lax.axis_index('tp')
        core = lax.rem(me, 2)
        x = lax.rem(lax.div(me, 2), side)
        y = lax.div(me, 2 * side)
        self.core = core
        self.p1 = x * (1 - core) + y * core
        self.p2 = y * (1 - core) + x * core

        def dev(p1, p2):
            p1, p2 = lax.rem(p1 + side, side), lax.rem(p2 + side, side)
            xx = p1 * (1 - core) + p2 * core
            yy = p2 * (1 - core) + p1 * core
            return (yy * side + xx) * 2 + core

        self.partner = me + 1 - 2 * core
        self.ring_devs = {1: (dev(self.p1 + 1, self.p2), dev(self.p1 - 1, self.p2)),
                          2: (dev(self.p1, self.p2 + 1), dev(self.p1, self.p2 - 1))}
        self.sent = []
        self.pending = {}

    def m(self, j):
        return lax.rem(j + self.side, self.side)

    def ds(self, off, size):
        return pl.ds(pl.multiple_of(off, 16), size)

    def send(self, s, key, idx, src, dst, device):
        copy = pltpu.make_async_remote_copy(src_ref=src, dst_ref=dst, send_sem=self.ssem.at[s, idx],
                                            recv_sem=self.rsem.at[s, idx], device_id={'tp': device},
                                            device_id_type=pl.DeviceIdType.MESH)
        copy.start()
        return copy

    def desc(self, s, idx, src, dst, device):
        return pltpu.make_async_remote_copy(src_ref=src, dst_ref=dst, send_sem=self.ssem.at[s, idx],
                                            recv_sem=self.rsem.at[s, idx], device_id={'tp': device},
                                            device_id_type=pl.DeviceIdType.MESH)

    def copies(self, s):
        side, l1, l2, hw, w = self.side, self.l1, self.l2, self.hw, self.cols
        c, p1, p2, m, ds = self.core, self.p1, self.p2, self.m, self.ds
        left, right = pl.ds(0, hw), pl.ds(hw, hw)
        own, full = self.own.at[s], self.full
        row0 = self.mb * 0 + s * self.blk
        out = {}
        out['pair'] = (0, self.part.at[ds(row0 + (1 - c) * self.half, self.half), :], self.pair.at[s], self.partner)

        def ring(tag, first, base, size, p, bufs, devs):
            plus, minus = devs

            def chunk(j, cols):
                return own.at[ds(base + m(j) * size, size), cols]

            out[tag + 'xp'] = (first + 0, chunk(p + 2, left), bufs.at[s, 0], plus)
            out[tag + 'xm'] = (first + 1, chunk(p + 2, right), bufs.at[s, 1], minus)
            out[tag + 'dp'] = (first + 2, chunk(p + 1, right), bufs.at[s, 2], plus)
            out[tag + 'dm'] = (first + 3, chunk(p - 1, left), bufs.at[s, 3], minus)
            out[tag + 'rp'] = (first + 4, chunk(p + 1, left), bufs.at[s, 4], plus)
            out[tag + 'rm'] = (first + 5, chunk(p - 1, right), bufs.at[s, 5], minus)

        ring('a', 1, 0, l1, p1, self.ring1, self.ring_devs[1])
        ring('b', 7, p1 * l1, l2, p2, self.ring2, self.ring_devs[2])

        def gather(tag, first, base, size, p, devs):
            plus, minus = devs

            def chunk(j, cols):
                return full.at[ds(base + m(j) * size, size), cols]

            every = pl.ds(0, w)
            for name, idx, view, to in (('sp', 0, chunk(p, every), plus), ('sm', 1, chunk(p, every), minus),
                                        ('yp', 2, chunk(p - 1, left), plus), ('ym', 3, chunk(p + 1, right), minus)):
                out[tag + name] = (first + idx, view, view, to)

        half0 = row0 + c * self.half
        gather('c', 13, half0 + p1 * l1, l2, p2, self.ring_devs[2])
        gather('d', 17, half0, l1, p1, self.ring_devs[1])
        for j in range(side):
            view = full.at[ds(half0 + m(p1 + j) * l1, l1), :]
            out['k%d' % j] = (21 + j, view, view, self.partner)
        return out

    def get(self, s, name):
        idx, src, dst, to = self.copies(s)[name]
        return self.desc(s, idx, src, dst, to)

    def start(self, s, *names):
        for name in names:
            self.get(s, name).start()
            self.sent.append((s, name))

    def arrived(self, s, *names):
        for name in names:
            self.get(s, name).wait_recv()

    def local(self, s, idx):
        row0 = s * self.blk
        mine = row0 + self.core * self.half + self.p1 * self.l1 + self.p2 * self.l2
        c, half = self.core, self.half
        if idx == 0:
            src, dst = self.part.at[self.ds(row0 + c * half, half), :], self.own.at[s]
        elif idx == 1:
            src, dst = self.saved.at[self.mb, self.ds(mine, self.l2), :], self.zrow.at[s]
        elif idx == 2:
            src, dst = self.resid(self.ds(mine, self.l2)), self.rrow.at[s]
        elif idx == 3:
            src, dst = self.stats.at[self.mb, self.ds(mine, self.l2), :], self.srow.at[s]
        elif idx == 4:
            rows = self.ds(row0 + c * half, half)
            src, dst = self.full.at[rows, :], self.out.at[rows, :]
        else:
            rows = self.ds(row0 + (1 - c) * half, half)
            src, dst = self.full.at[rows, :], self.out.at[rows, :]
        return pltpu.make_async_copy(src, dst, self.lsem.at[s, idx])

    def barrier(self):
        sem = pltpu.get_barrier_semaphore()
        peers = (self.partner,) + self.ring_devs[1] + self.ring_devs[2]
        for peer in peers:
            pl.semaphore_signal(sem, inc=1, device_id={'tp': peer}, device_id_type=pl.DeviceIdType.MESH)
        pl.semaphore_wait(sem, len(peers))

    def begin(self):
        for s in range(NB):
            self.local(s, 0).start()
        for s in range(NB):
            for idx in (1, 2, 3):
                self.local(s, idx).start()
        self.barrier()
        for s in range(NB):
            self.start(s, 'pair')

    def rs1_start(self, s):
        self.local(s, 0).wait()
        self.arrived(s, 'pair')
        step = self.l1

        def add(i, carry):
            rows = pl.ds(pl.multiple_of(i * step, step), step)
            self.own[s, rows, :] = (self.own[s, rows, :].astype(F32) + self.pair[s, rows, :].astype(F32)).astype(BF16)
            return carry

        lax.fori_loop(0, self.half // step, add, 0)
        self.start(s, 'axp', 'axm', 'adp', 'adm')

    def relay(self, s, tag, bufs, base, size, p):
        for buf, j, col0, got, nxt in ((0, p + 1, 0, 'xp', 'rp'), (1, p - 1, self.hw, 'xm', 'rm')):
            self.arrived(s, tag + got)
            rows = self.ds(base + self.m(j) * size, size)
            cols = pl.ds(col0, self.hw)
            self.own[s, rows, cols] = (self.own[s, rows, cols].astype(F32) + bufs[s, buf].astype(F32)).astype(BF16)
            self.start(s, tag + nxt)

    def final(self, s, tag, bufs, base, size, p):
        self.arrived(s, tag + 'rp', tag + 'dm', tag + 'rm', tag + 'dp')
        rows = self.ds(base + p * size, size)
        sums = []
        for col0, one, two in ((0, 4, 3), (self.hw, 5, 2)):
            sums.append(self.own[s, rows, pl.ds(col0, self.hw)].astype(F32)
                        + bufs[s, one].astype(F32) + bufs[s, two].astype(F32))
        return rows, sums

    def rs1_relay(self, s):
        self.relay(s, 'a', self.ring1, 0, self.l1, self.p1)

    def rs2_start(self, s):
        rows, sums = self.final(s, 'a', self.ring1, 0, self.l1, self.p1)
        for k in range(2):
            self.own[s, rows, pl.ds(k * self.hw, self.hw)] = sums[k].astype(BF16)
        self.start(s, 'bxp', 'bxm', 'bdp', 'bdm')

    def rs2_relay(self, s):
        self.relay(s, 'b', self.ring2, self.p1 * self.l1, self.l2, self.p2)

    def norm_gather(self, s):
        _, sums = self.final(s, 'b', self.ring2, self.p1 * self.l1, self.l2, self.p2)
        for idx in (1, 2, 3):
            self.local(s, idx).wait()
        mu = self.srow[s, :, self.stat_col:self.stat_col + 1]
        r = self.srow[s, :, self.stat_col + 1:self.stat_col + 2]
        us, xs = [], []
        for k in range(2):
            cols = pl.ds(k * self.hw, self.hw)
            us.append(sums[k] * self.gain[:, cols].astype(F32))
            xs.append((self.zrow[s, :, cols].astype(F32) - mu) * r)
        inv = 1.0 / self.cols
        mean_u = (jnp.sum(us[0], axis=-1, keepdims=True) + jnp.sum(us[1], axis=-1, keepdims=True)) * inv
        mean_c = (jnp.sum(us[0] * xs[0], axis=-1, keepdims=True)
                  + jnp.sum(us[1] * xs[1], axis=-1, keepdims=True)) * inv
        mine = self.ds(s * self.blk + self.core * self.half + self.p1 * self.l1 + self.p2 * self.l2, self.l2)
        for k in range(2):
            cols = pl.ds(k * self.hw, self.hw)
            grad = self.rrow[s, :, cols].astype(F32) + r * (us[k] - mean_u - xs[k] * mean_c)
            self.full[mine, cols] = grad.astype(BF16)
        self.start(s, 'csp', 'csm')

    def ag2_relay(self, s):
        self.arrived(s, 'csp')
        self.start(s, 'cyp')
        self.arrived(s, 'csm')
        self.start(s, 'cym')

    def ag1_start(self, s):
        self.arrived(s, 'cyp', 'cym')
        self.start(s, 'dsp', 'dsm', 'k0')

    def ag1_relay(self, s):
        self.arrived(s, 'dsp')
        self.start(s, 'dyp')
        self.arrived(s, 'dsm')
        self.start(s, 'dym', 'k3', 'k1')

    def ag1_final(self, s):
        self.arrived(s, 'dyp', 'dym')
        self.start(s, 'k2')
        self.local(s, 4).start()

    def finish(self, s):
        self.arrived(s, 'k0', 'k1', 'k2', 'k3')
        self.local(s, 5).start()

    def end(self):
        for s, name in self.sent:
            self.get(s, name).wait_send()
        for s in range(NB):
            self.local(s, 4).wait()
            self.local(s, 5).wait()

    def ticks(self):
        f = partial
        return [self.begin,
                f(self.rs1_start, 0), f(self.rs1_start, 1), f(self.rs1_relay, 0), f(self.rs2_start, 0),
                f(self.rs1_relay, 1), f(self.rs2_relay, 0), f(self.norm_gather, 0), f(self.rs2_start, 1),
                f(self.ag2_relay, 0), f(self.rs2_relay, 1), f(self.ag1_start, 0), f(self.norm_gather, 1),
                f(self.ag2_relay, 1), f(self.ag1_relay, 0), f(self.ag1_start, 1), f(self.ag1_final, 0),
                f(self.ag1_relay, 1), f(self.finish, 0), f(self.ag1_final, 1), f(self.finish, 1), self.end]


def reduce_norm_gather(n, part, saved, resid, resid_mb, stats, gain, mb, stat_col, cid):
    rows, cols = part.shape
    comm = Comm(n, rows, cols)

    def kernel(part_ref, saved_ref, resid_ref, stats_ref, gain_ref, out_ref, *scratch):
        if resid_mb:
            resid_at = lambda r: resid_ref.at[mb, r, :]
        else:
            resid_at = lambda r: resid_ref.at[r, :]
        comm.bind(part_ref, saved_ref, resid_at, stats_ref, gain_ref, out_ref, scratch, mb, stat_col)
        for tick in comm.ticks():
            tick()

    return pl.pallas_call(
        kernel,
        out_shape=jax.ShapeDtypeStruct((rows, cols), BF16),
        in_specs=[pl.BlockSpec(memory_space=ANY)] * 4 + [pl.BlockSpec(memory_space=VMEM)],
        out_specs=pl.BlockSpec(memory_space=ANY),
        scratch_shapes=comm.scratch(),
        compiler_params=pltpu.CompilerParams(collective_id=cid, has_side_effects=True,
                                             vmem_limit_bytes=48 * 1024 * 1024),
        name='sum_norm_gather_%d' % cid,
    )(part, saved, resid, stats, gain)


def solution(mesh):
    act_spec = P('dp', None, None)
    stat_spec = P('dp', None)
    in_specs = (act_spec, act_spec, act_spec, stat_spec, stat_spec, stat_spec, stat_spec, P(), P(),
                P(None, 'tp', None, None), P('tp', None, None), P(None, 'tp'), P('tp', None))
    out_specs = (act_spec, P('dp', 'tp', None, None), P(('dp', 'tp'), None, None), P('dp', 'tp'),
                 P(('dp', 'tp'), None))
    n = mesh.shape['tp']

    def local_backward(x_saved, h1_saved, grad_y, mean_one, rstd_one, mean_two, rstd_two,
                       gain_one, gain_two, w_qkv, w_out, w_up, w_down):
        score_scale = w_qkv.shape[3] ** -0.5
        mbs = x_saved.shape[0]
        stats = jnp.stack([mean_one, rstd_one, mean_two, rstd_two] * 2, axis=-1)
        g1, g2 = gain_one[None, :], gain_two[None, :]
        part_two, n2, da, act = [], [], [], []
        for b in range(mbs):
            xhat = (h1_saved[b].astype(F32) - mean_two[b][:, None]) * rstd_two[b][:, None]
            norm_two = (xhat * gain_two.astype(F32)).astype(BF16)
            pre_act = wide_einsum('sh,hf->sf', norm_two, w_up)
            act.append(gelu_tanh(pre_act).astype(BF16))
            grad_pre = (wide_einsum('sh,fh->sf', grad_y[b], w_down) * gelu_slope(pre_act)).astype(BF16)
            part_two.append(wide_einsum('sf,hf->sh', grad_pre, w_up).astype(BF16))
            n2.append(norm_two)
            da.append(grad_pre)
        dh1 = [reduce_norm_gather(n, part_two[b], h1_saved, grad_y, True, stats, g2, b, 2, b) for b in range(mbs)]
        norm_two, grad_pre, act_out = jnp.stack(n2), jnp.stack(da), jnp.stack(act)
        grad_down = wide_einsum('msf,msh->fh', act_out, grad_y).astype(BF16)
        grad_up = wide_einsum('msh,msf->hf', norm_two, grad_pre).astype(BF16)
        attn_all, gqkv_all, n1_all, dx = [], [], [], []
        for b in range(mbs):
            xhat = (x_saved[b].astype(F32) - mean_one[b][:, None]) * rstd_one[b][:, None]
            norm_one = (xhat * gain_one.astype(F32)).astype(BF16)[None]
            qkv_acts = wide_einsum('msh,hncd->msncd', norm_one, w_qkv).astype(BF16)
            grad_o = wide_einsum('msh,ndh->msnd', dh1[b][None], w_out).astype(BF16)
            attn_out, grad_qkv = attention_backward(qkv_acts[:, :, :, 0], qkv_acts[:, :, :, 1], qkv_acts[:, :, :, 2],
                                                    grad_o, score_scale)
            part_one = wide_einsum('msncd,hncd->msh', grad_qkv, w_qkv).astype(BF16)[0]
            dx.append(reduce_norm_gather(n, part_one, x_saved, dh1[b], False, stats, g1, b, 0, mbs + b))
            attn_all.append(attn_out[0])
            gqkv_all.append(grad_qkv[0])
            n1_all.append(norm_one[0])
        attn_out, grad_qkv, norm_one = jnp.stack(attn_all), jnp.stack(gqkv_all), jnp.stack(n1_all)
        grad_h1 = jnp.stack(dh1)
        grad_out_w = wide_einsum('msnd,msh->ndh', attn_out, grad_h1).astype(BF16)
        grad_qkv_w = wide_einsum('msh,msncd->hncd', norm_one, grad_qkv).astype(BF16)
        return jnp.stack(dx), grad_qkv_w, grad_out_w, grad_up, grad_down

    return jax.shard_map(local_backward, mesh=mesh, in_specs=in_specs, out_specs=out_specs, check_vma=False)
```

```python
import math
import jax
import jax.numpy as jnp
from jax import lax
from jax.experimental import pallas as pl
from jax.experimental.pallas import tpu as pltpu
from jax.sharding import PartitionSpec as P
from functools import partial

GELU_C = 0.7978845608028654
GELU_A = 0.044715
F32 = jnp.float32
BF16 = jnp.bfloat16
ANY = pl.ANY
VMEM = pltpu.VMEM
wide_einsum = partial(jnp.einsum, preferred_element_type=F32)


def gelu_tanh(pre_act):
    inner_arg = GELU_C * (pre_act + GELU_A * pre_act * pre_act * pre_act)
    return 0.5 * pre_act * (1.0 + jnp.tanh(inner_arg))


def gelu_slope(pre_act):
    inner_arg = GELU_C * (pre_act + GELU_A * pre_act * pre_act * pre_act)
    tanh_val = jnp.tanh(inner_arg)
    return (0.5 * (1.0 + tanh_val)
            + 0.5 * pre_act * (1.0 - tanh_val * tanh_val) * GELU_C * (1.0 + 3.0 * GELU_A * pre_act * pre_act))


def attention_backward(q_heads, k_heads, v_heads, grad_o, score_scale):
    seq_len = q_heads.shape[1]
    scores = wide_einsum('bqnd,bknd->bnqk', q_heads, k_heads) * score_scale
    causal = jnp.arange(seq_len)[:, None] >= jnp.arange(seq_len)[None, :]
    attn_prob = jax.nn.softmax(jnp.where(causal, scores, -1e30), axis=-1)
    prob_bf16 = attn_prob.astype(BF16)
    attn_out = wide_einsum('bnqk,bknd->bqnd', prob_bf16, v_heads).astype(BF16)
    grad_v = wide_einsum('bnqk,bqnd->bknd', prob_bf16, grad_o).astype(BF16)
    grad_p = wide_einsum('bqnd,bknd->bnqk', grad_o, v_heads)
    row_dot = jnp.sum(attn_prob * grad_p, axis=-1, keepdims=True)
    grad_s = (attn_prob * (grad_p - row_dot) * score_scale).astype(BF16)
    grad_q = wide_einsum('bnqk,bknd->bqnd', grad_s, k_heads).astype(BF16)
    grad_k = wide_einsum('bnqk,bqnd->bknd', grad_s, q_heads).astype(BF16)
    return attn_out, jnp.stack([grad_q, grad_k, grad_v], axis=3)


BLOCK = 512
SEMS = 32
LINK = {'1+': 85e3, '1-': 85e3, '2+': 85e3, '2-': 85e3, 'D': 450e3}
LATENCY = 2.3
TICK = 0.3


class Comm:
    def __init__(self, n, rows, cols):
        self.side = math.isqrt(n // 2)
        assert self.side == 4 and 2 * self.side * self.side == n
        self.rows, self.cols = rows, cols
        self.blk = BLOCK
        self.streams = rows // BLOCK
        self.half = self.blk // 2
        self.l1 = self.half // self.side
        self.l2 = self.l1 // self.side
        self.hw = cols // 2

    N_SCRATCH = 12

    def scratch(self):
        l1, l2, w, hw, ns = self.l1, self.l2, self.cols, self.hw, self.streams
        return [
            VMEM((ns, self.half, w), BF16),
            VMEM((ns, self.half, w), BF16),
            VMEM((ns, 6, l1, hw), BF16),
            VMEM((ns, 6, l2, hw), BF16),
            VMEM((self.rows, w), BF16),
            VMEM((ns, l2, w), BF16),
            VMEM((ns, l2, w), BF16),
            VMEM((self.rows, 128), F32),
            VMEM((self.rows, 128), F32),
            pltpu.SemaphoreType.DMA((ns, SEMS)),
            pltpu.SemaphoreType.DMA((ns, SEMS)),
            pltpu.SemaphoreType.DMA((ns, 8)),
            pltpu.SemaphoreType.REGULAR((ns,)),
        ]

    def bind(self, part, saved, resid, mean, rstd, gain, out, scratch):
        (self.own, self.pair, self.ring1, self.ring2, self.full, self.zrow, self.rrow, self.mu, self.rs,
         self.ssem, self.rsem, self.lsem, self.freed) = scratch
        self.part, self.saved, self.resid, self.gain, self.out = part, saved, resid, gain, out
        self.mean, self.rstd = mean, rstd
        side = self.side
        me = lax.axis_index('tp')
        core = lax.rem(me, 2)
        x = lax.rem(lax.div(me, 2), side)
        y = lax.div(me, 2 * side)
        self.core = core
        self.p1 = x * (1 - core) + y * core
        self.p2 = y * (1 - core) + x * core

        def dev(p1, p2):
            p1, p2 = lax.rem(p1 + side, side), lax.rem(p2 + side, side)
            xx = p1 * (1 - core) + p2 * core
            yy = p2 * (1 - core) + p1 * core
            return (yy * side + xx) * 2 + core

        self.partner = me + 1 - 2 * core
        self.ring_devs = {1: (dev(self.p1 + 1, self.p2), dev(self.p1 - 1, self.p2)),
                          2: (dev(self.p1, self.p2 + 1), dev(self.p1, self.p2 - 1))}
        self.sent = []

    def m(self, j):
        return lax.rem(j + self.side, self.side)

    def ds(self, off, size):
        return pl.ds(pl.multiple_of(off, 16), size)

    def half_rows(self, s, which):
        c = self.core if which == 0 else 1 - self.core
        return self.ds(s * self.blk + c * self.half, self.half)

    def copies(self, s):
        side, l1, l2, hw, w = self.side, self.l1, self.l2, self.hw, self.cols
        c, p1, p2, m, ds = self.core, self.p1, self.p2, self.m, self.ds
        left, right = pl.ds(0, hw), pl.ds(hw, hw)
        own, full = self.own.at[s], self.full
        row0 = s * self.blk
        out = {}
        source = self.full if self.part is None else self.part
        out['pair'] = (0, source.at[self.half_rows(s, 1), :], self.pair.at[s], self.partner)

        def ring(tag, first, base, size, p, bufs, devs):
            plus, minus = devs

            def chunk(j, cols):
                return own.at[ds(base + m(j) * size, size), cols]

            out[tag + 'xp'] = (first + 0, chunk(p + 2, left), bufs.at[s, 0], plus)
            out[tag + 'xm'] = (first + 1, chunk(p + 2, right), bufs.at[s, 1], minus)
            out[tag + 'dp'] = (first + 2, chunk(p + 1, right), bufs.at[s, 2], plus)
            out[tag + 'dm'] = (first + 3, chunk(p - 1, left), bufs.at[s, 3], minus)
            out[tag + 'rp'] = (first + 4, chunk(p + 1, left), bufs.at[s, 4], plus)
            out[tag + 'rm'] = (first + 5, chunk(p - 1, right), bufs.at[s, 5], minus)

        ring('a', 1, 0, l1, p1, self.ring1, self.ring_devs[1])
        ring('b', 7, p1 * l1, l2, p2, self.ring2, self.ring_devs[2])

        def gather(tag, first, base, size, p, devs):
            plus, minus = devs

            def chunk(j, cols):
                return full.at[ds(base + m(j) * size, size), cols]

            every = pl.ds(0, w)
            for name, idx, view, to in (('sp', 0, chunk(p, every), plus), ('sm', 1, chunk(p, every), minus),
                                        ('yp', 2, chunk(p - 1, left), plus), ('ym', 3, chunk(p + 1, right), minus)):
                out[tag + name] = (first + idx, view, view, to)

        half0 = row0 + c * self.half
        gather('c', 13, half0 + p1 * l1, l2, p2, self.ring_devs[2])
        gather('d', 17, half0, l1, p1, self.ring_devs[1])
        for j in range(side):
            view = full.at[ds(half0 + m(p1 + j) * l1, l1), :]
            out['k%d' % j] = (21 + j, view, view, self.partner)
        return out

    def get(self, s, name):
        idx, src, dst, to = self.copies(s)[name]
        return pltpu.make_async_remote_copy(src_ref=src, dst_ref=dst, send_sem=self.ssem.at[s, idx],
                                            recv_sem=self.rsem.at[s, idx], device_id={'tp': to},
                                            device_id_type=pl.DeviceIdType.MESH)

    def start(self, s, *names):
        for name in names:
            self.get(s, name).start()
            self.sent.append((s, name))

    def arrived(self, s, *names):
        for name in names:
            self.get(s, name).wait_recv()

    def mine(self, s):
        return self.ds(s * self.blk + self.core * self.half + self.p1 * self.l1 + self.p2 * self.l2, self.l2)

    def local(self, s, idx):
        if idx == 0:
            src, dst = self.part.at[self.half_rows(s, 0), :], self.own.at[s]
        elif idx == 1:
            src, dst = self.saved.at[self.mine(s), :], self.zrow.at[s]
        elif idx == 2:
            src, dst = self.resid.at[self.mine(s), :], self.rrow.at[s]
        else:
            rows = self.half_rows(s, idx - 4)
            src, dst = self.full.at[rows, :], self.out.at[rows, :]
        return pltpu.make_async_copy(src, dst, self.lsem.at[s, idx])

    def barrier(self):
        sem = pltpu.get_barrier_semaphore()
        peers = (self.partner,) + self.ring_devs[1] + self.ring_devs[2]
        for peer in peers:
            pl.semaphore_signal(sem, inc=1, device_id={'tp': peer}, device_id_type=pl.DeviceIdType.MESH)
        pl.semaphore_wait(sem, len(peers))

    def columns(self):
        per = self.mean.shape[1]
        for src, dst in ((self.mean, self.mu), (self.rstd, self.rs)):
            for i in range(self.rows // 128):
                b, off = divmod(i * 128, per)
                row = src[b:b + 1, off:off + 128]
                dst[pl.ds(i * 128, 128), :] = jnp.transpose(jnp.broadcast_to(row, (128, 128)))

    def begin(self):
        for s in range(self.streams):
            if self.part is not None:
                self.local(s, 0).start()
            self.local(s, 1).start()
            self.local(s, 2).start()
        self.barrier()
        if self.part is not None:
            for s in range(self.streams):
                self.start(s, 'pair')
        self.columns()

    def rs1_start(self, s):
        if self.part is not None:
            self.local(s, 0).wait()
        self.arrived(s, 'pair')
        step = self.l1

        def add(i, carry):
            rows = pl.ds(pl.multiple_of(i * step, step), step)
            self.own[s, rows, :] = (self.own[s, rows, :].astype(F32) + self.pair[s, rows, :].astype(F32)).astype(BF16)
            return carry

        lax.fori_loop(0, self.half // step, add, 0)
        self.start(s, 'axp', 'axm', 'adp', 'adm')
        if self.part is None:
            self.get(s, 'pair').wait_send()
            pl.semaphore_signal(self.freed.at[s], inc=1, device_id={'tp': self.partner},
                                device_id_type=pl.DeviceIdType.MESH)

    def relay(self, s, tag, bufs, base, size, p):
        for buf, j, col0, got, nxt in ((0, p + 1, 0, 'xp', 'rp'), (1, p - 1, self.hw, 'xm', 'rm')):
            self.arrived(s, tag + got)
            rows = self.ds(base + self.m(j) * size, size)
            cols = pl.ds(col0, self.hw)
            self.own[s, rows, cols] = (self.own[s, rows, cols].astype(F32) + bufs[s, buf].astype(F32)).astype(BF16)
            self.start(s, tag + nxt)

    def final(self, s, tag, bufs, base, size, p):
        self.arrived(s, tag + 'rp', tag + 'dm', tag + 'rm', tag + 'dp')
        rows = self.ds(base + p * size, size)
        sums = []
        for col0, one, two in ((0, 4, 3), (self.hw, 5, 2)):
            sums.append(self.own[s, rows, pl.ds(col0, self.hw)].astype(F32)
                        + bufs[s, one].astype(F32) + bufs[s, two].astype(F32))
        return rows, sums

    def rs1_relay(self, s):
        self.relay(s, 'a', self.ring1, 0, self.l1, self.p1)

    def rs2_start(self, s):
        rows, sums = self.final(s, 'a', self.ring1, 0, self.l1, self.p1)
        for k in range(2):
            self.own[s, rows, pl.ds(k * self.hw, self.hw)] = sums[k].astype(BF16)
        self.start(s, 'bxp', 'bxm', 'bdp', 'bdm')

    def rs2_relay(self, s):
        self.relay(s, 'b', self.ring2, self.p1 * self.l1, self.l2, self.p2)

    def norm_gather(self, s):
        _, sums = self.final(s, 'b', self.ring2, self.p1 * self.l1, self.l2, self.p2)
        self.local(s, 1).wait()
        self.local(s, 2).wait()
        mine = self.mine(s)
        mu = self.mu[mine, 0:1]
        r = self.rs[mine, 0:1]
        us, xs = [], []
        for k in range(2):
            cols = pl.ds(k * self.hw, self.hw)
            us.append(sums[k] * self.gain[:, cols].astype(F32))
            xs.append((self.zrow[s, :, cols].astype(F32) - mu) * r)
        inv = 1.0 / self.cols
        mean_u = (jnp.sum(us[0], axis=-1, keepdims=True) + jnp.sum(us[1], axis=-1, keepdims=True)) * inv
        mean_c = (jnp.sum(us[0] * xs[0], axis=-1, keepdims=True)
                  + jnp.sum(us[1] * xs[1], axis=-1, keepdims=True)) * inv
        for k in range(2):
            cols = pl.ds(k * self.hw, self.hw)
            grad = self.rrow[s, :, cols].astype(F32) + r * (us[k] - mean_u - xs[k] * mean_c)
            self.full[mine, cols] = grad.astype(BF16)
        self.start(s, 'csp', 'csm')

    def ag2_relay(self, s):
        self.arrived(s, 'csp')
        self.start(s, 'cyp')
        self.arrived(s, 'csm')
        self.start(s, 'cym')

    def ag1_start(self, s):
        self.arrived(s, 'cyp', 'cym')
        if self.part is None:
            pl.semaphore_wait(self.freed.at[s], 1)
        self.start(s, 'dsp', 'dsm', 'k0')

    def ag1_relay(self, s):
        self.arrived(s, 'dsp')
        self.start(s, 'dyp')
        self.arrived(s, 'dsm')
        self.start(s, 'dym', 'k3', 'k1')

    def ag1_final(self, s):
        self.arrived(s, 'dyp', 'dym')
        self.start(s, 'k2')
        self.local(s, 4).start()

    def finish(self, s):
        self.arrived(s, 'k0', 'k1', 'k2', 'k3')
        self.local(s, 5).start()

    def end(self):
        for s, name in self.sent:
            if name != 'pair' or self.part is not None:
                self.get(s, name).wait_send()
        for s in range(self.streams):
            self.local(s, 4).wait()
            self.local(s, 5).wait()

    def stages(self):
        x1, x2 = self.l1 * self.hw * 2, self.l2 * self.hw * 2
        return [
            ('rs1_start', ['pair', 'own'], [('axp', '1+', x1), ('axm', '1-', x1), ('adp', '1+', x1), ('adm', '1-', x1)]),
            ('rs1_relay', ['axp', 'axm'], [('arp', '1+', x1), ('arm', '1-', x1)]),
            ('rs2_start', ['arp', 'arm', 'adp', 'adm'],
             [('bxp', '2+', x2), ('bxm', '2-', x2), ('bdp', '2+', x2), ('bdm', '2-', x2)]),
            ('rs2_relay', ['bxp', 'bxm'], [('brp', '2+', x2), ('brm', '2-', x2)]),
            ('norm_gather', ['brp', 'brm', 'bdp', 'bdm'], [('csp', '2+', 2 * x2), ('csm', '2-', 2 * x2)]),
            ('ag2_relay', ['csp', 'csm'], [('cyp', '2+', x2), ('cym', '2-', x2)]),
            ('ag1_start', ['cyp', 'cym'], [('dsp', '1+', 2 * x1), ('dsm', '1-', 2 * x1), ('k0', 'D', 2 * x1)]),
            ('ag1_relay', ['dsp', 'dsm'], [('dyp', '1+', x1), ('dym', '1-', x1), ('k3', 'D', 2 * x1), ('k1', 'D', 2 * x1)]),
            ('ag1_final', ['dyp', 'dym'], [('k2', 'D', 2 * x1)]),
            ('finish', ['k0', 'k1', 'k2', 'k3'], []),
        ]

    def plan(self, points):
        stages = self.stages()
        pair_bytes = self.half * self.cols * 2
        free = dict.fromkeys(LINK, 0.0)
        done = {}
        at = [0] * self.streams
        now = 0.0

        def push(s, name, link, size):
            free[link] = max(free[link], now) + size / LINK[link]
            done[s, name] = free[link] + LATENCY

        def ready(s):
            if at[s] >= len(stages):
                return math.inf
            return max(done.get((s, need), math.inf) for need in stages[at[s]][1])

        plans = []
        for i, (cost, gives) in enumerate(points):
            now += cost
            todo = []
            for s, what in gives:
                if what == 'pair':
                    push(s, 'pair', 'D', pair_bytes)
                    if self.part_given is False:
                        todo.append(('send_pair', s))
                else:
                    done[s, 'own'] = now
            last = i == len(points) - 1
            while True:
                s = min(range(self.streams), key=ready)
                t = ready(s)
                if t == math.inf or (t > now and not last):
                    break
                now = max(now, t) + TICK
                name, _, sends = stages[at[s]]
                for copy, link, size in sends:
                    push(s, copy, link, size)
                at[s] += 1
                todo.append((name, s))
            plans.append(todo)
        assert all(a == len(stages) for a in at)
        self.estimate = now
        return plans

    def send_pair(self, s):
        self.start(s, 'pair')

    part_given = False


VMEM_LIMIT = 64 * 1024 * 1024 - 64 * 1024


def reduce_norm_gather(n, part, saved, resid, mean, rstd, gain, cid):
    rows, cols = part.shape
    comm = Comm(n, rows, cols)
    comm.part_given = True
    plans = comm.plan([(3.0, [(s, w) for s in range(comm.streams) for w in ('pair', 'own')])])

    def kernel(part_ref, saved_ref, resid_ref, mean_ref, rstd_ref, gain_ref, out_ref, *scratch):
        comm.bind(part_ref, saved_ref, resid_ref, mean_ref, rstd_ref, gain_ref, out_ref, scratch)
        comm.begin()
        for name, s in plans[0]:
            getattr(comm, name)(s)
        comm.end()

    return pl.pallas_call(
        kernel,
        out_shape=jax.ShapeDtypeStruct((rows, cols), BF16),
        in_specs=[pl.BlockSpec(memory_space=ANY)] * 3 + [pl.BlockSpec(memory_space=VMEM)] * 3,
        out_specs=pl.BlockSpec(memory_space=ANY),
        scratch_shapes=comm.scratch(),
        compiler_params=pltpu.CompilerParams(collective_id=cid, has_side_effects=True, vmem_limit_bytes=VMEM_LIMIT),
        name='sum_norm_gather_%d' % cid,
    )(part, saved, resid, mean, rstd, gain)


def dot(a, b, ca=1, cb=0):
    return lax.dot_general(a, b, (((ca,), (cb,)), ((), ())), preferred_element_type=F32)


def mlp_stage(n, h1, dy, mean, rstd, gain, w_up, w_down, cid):
    rows, cols = h1.shape
    ffn = w_up.shape[1]
    comm = Comm(n, rows, cols)
    tile = comm.half
    n_tiles = rows // tile
    cb = 256
    n_cols = cols // cb
    grid = n_tiles + n_cols
    points = []
    for i in range(n_tiles):
        points += [(1.6, []), (1.2, []), (1.2, [(i // 2, 'pair' if i % 2 == 0 else 'own')])]
    for i in range(n_cols):
        points += [(0.6, []), (0.8, []), (0.8, [])]
    plans = comm.plan(points)

    def kernel(h1_tile, dy_tile, h1_col, dy_col, w1, w2, mean_ref, rstd_ref, gain_ref, h1_all, dy_all,
               dh1_ref, dw1_ref, dw2_ref, act, da, *scratch):
        comm.bind(None, h1_all, dy_all, mean_ref, rstd_ref, gain_ref, dh1_ref, scratch)
        i = pl.program_id(0)
        full, own = comm.full, comm.own

        def ticks(steps, k):
            for step in steps:
                todo = plans[step * 3 + k]
                if todo:
                    @pl.when(i == step)
                    def _():
                        for name, s in todo:
                            getattr(comm, name)(s)

        @pl.when(i == 0)
        def _():
            comm.begin()

        first = range(n_tiles)
        rest = range(n_tiles, grid)
        tidx = lax.div(i, 2) * 2 + lax.rem(i, 2) * comm.core + (1 - lax.rem(i, 2)) * (1 - comm.core)
        trow = pl.ds(pl.multiple_of(tidx * tile, tile), tile)
        pre_ref, dg_ref = comm.pre, comm.dg

        @pl.when(i < n_tiles)
        def _():
            z = (h1_tile[...].astype(F32) - comm.mu[trow, 0:1]) * comm.rs[trow, 0:1]
            n2 = (z * gain_ref[...]).astype(BF16)
            pre_ref[...] = dot(n2, w1[...])
        ticks(first, 0)

        @pl.when(i < n_tiles)
        def _():
            dg_ref[...] = dot(dy_tile[...], w2[...], 1, 1)
        ticks(first, 1)

        @pl.when(i < n_tiles)
        def _():
            pre = pre_ref[...]
            act[trow, :] = gelu_tanh(pre).astype(BF16)
            grad_pre = (dg_ref[...] * gelu_slope(pre)).astype(BF16)
            da[trow, :] = grad_pre
            part = dot(grad_pre, w1[...], 1, 1).astype(BF16)

            @pl.when(lax.rem(i, 2) == 0)
            def _():
                full[trow, :] = part

            @pl.when(lax.rem(i, 2) == 1)
            def _():
                own[lax.div(i, 2)] = part
        ticks(first, 2)

        @pl.when(i >= n_tiles)
        def _():
            c0 = pl.multiple_of((i - n_tiles) * cb, cb)
            z = (h1_col[...].astype(F32) - comm.mu[:, 0:1]) * comm.rs[:, 0:1]
            comm.n2c[...] = (z * gain_ref[:, pl.ds(c0, cb)]).astype(BF16)
        ticks(rest, 0)

        @pl.when(i >= n_tiles)
        def _():
            dw1_ref[...] = dot(comm.n2c[...], da[...], 0, 0).astype(BF16)
        ticks(rest, 1)

        @pl.when(i >= n_tiles)
        def _():
            dw2_ref[...] = dot(act[...], dy_col[...], 0, 0).astype(BF16)
        ticks(rest, 2)

        @pl.when(i == grid - 1)
        def _():
            comm.end()

    def wrapped(*refs):
        *most, pre, dg, n2c = refs
        comm.pre, comm.dg, comm.n2c = pre, dg, n2c
        kernel(*most)

    def tile_map(i):
        core = lax.rem(lax.axis_index('tp'), 2)
        ii = jnp.minimum(i, n_tiles - 1)
        odd = lax.rem(ii, 2)
        return lax.div(ii, 2) * 2 + odd * core + (1 - odd) * (1 - core), 0

    def col_at(i):
        return jnp.maximum(i - n_tiles, 0)

    whole = pl.BlockSpec(memory_space=VMEM)
    hbm = pl.BlockSpec(memory_space=ANY)
    return pl.pallas_call(
        wrapped,
        grid=(grid,),
        out_shape=(jax.ShapeDtypeStruct((rows, cols), BF16), jax.ShapeDtypeStruct((cols, ffn), BF16),
                   jax.ShapeDtypeStruct((ffn, cols), BF16)),
        in_specs=[pl.BlockSpec((tile, cols), tile_map), pl.BlockSpec((tile, cols), tile_map),
                  pl.BlockSpec((rows, cb), lambda i: (0, col_at(i))), pl.BlockSpec((rows, cb), lambda i: (0, col_at(i))),
                  whole, whole, whole, whole, whole, hbm, hbm],
        out_specs=(hbm, pl.BlockSpec((cb, ffn), lambda i: (col_at(i), 0)),
                   pl.BlockSpec((ffn, cb), lambda i: (0, col_at(i)))),
        scratch_shapes=[VMEM((rows, ffn), BF16), VMEM((rows, ffn), BF16)] + comm.scratch()
        + [VMEM((tile, ffn), F32), VMEM((tile, ffn), F32), VMEM((rows, cb), BF16)],
        compiler_params=pltpu.CompilerParams(collective_id=cid, has_side_effects=True, vmem_limit_bytes=VMEM_LIMIT,
                                             dimension_semantics=('arbitrary',)),
        name='mlp_stage',
    )(h1, dy, h1, dy, w_up, w_down, mean, rstd, gain, h1, dy)


def solution(mesh):
    act_spec = P('dp', None, None)
    stat_spec = P('dp', None)
    in_specs = (act_spec, act_spec, act_spec, stat_spec, stat_spec, stat_spec, stat_spec, P(), P(),
                P(None, 'tp', None, None), P('tp', None, None), P(None, 'tp'), P('tp', None))
    out_specs = (act_spec, P('dp', 'tp', None, None), P(('dp', 'tp'), None, None), P('dp', 'tp'),
                 P(('dp', 'tp'), None))
    n = mesh.shape['tp']

    def local_backward(x_saved, h1_saved, grad_y, mean_one, rstd_one, mean_two, rstd_two,
                       gain_one, gain_two, w_qkv, w_out, w_up, w_down):
        score_scale = w_qkv.shape[3] ** -0.5
        shape = x_saved.shape
        flat = (shape[0] * shape[1], shape[2])
        g1, g2 = gain_one.astype(F32)[None, :], gain_two.astype(F32)[None, :]
        dh1, grad_up, grad_down = mlp_stage(n, h1_saved.reshape(flat), grad_y.reshape(flat), mean_two, rstd_two, g2,
                                            w_up, w_down, 0)
        grad_h1 = dh1.reshape(shape)
        value_a8 = (x_saved.astype(F32) - mean_one[..., None]) * rstd_one[..., None]
        norm_one = (value_a8 * gain_one.astype(F32)).astype(BF16)
        qkv_acts = wide_einsum('msh,hncd->msncd', norm_one, w_qkv).astype(BF16)
        grad_o = wide_einsum('msh,ndh->msnd', grad_h1, w_out).astype(BF16)
        attn_out, grad_qkv = attention_backward(qkv_acts[:, :, :, 0], qkv_acts[:, :, :, 1], qkv_acts[:, :, :, 2],
                                                grad_o, score_scale)
        grad_out_w = wide_einsum('msnd,msh->ndh', attn_out, grad_h1).astype(BF16)
        grad_qkv_w = wide_einsum('msh,msncd->hncd', norm_one, grad_qkv).astype(BF16)
        part_one = wide_einsum('msncd,hncd->msh', grad_qkv, w_qkv).astype(BF16)
        dx = reduce_norm_gather(n, part_one.reshape(flat), x_saved.reshape(flat), dh1, mean_one, rstd_one, g1, 1)
        return dx.reshape(shape), grad_qkv_w, grad_out_w, grad_up, grad_down

    return jax.shard_map(local_backward, mesh=mesh, in_specs=in_specs, out_specs=out_specs, check_vma=False)
```

```python
import math
import jax
import jax.numpy as jnp
from jax import lax
from jax.experimental import pallas as pl
from jax.experimental.pallas import tpu as pltpu
from jax.sharding import PartitionSpec as P

GELU_C = 0.7978845608028654
GELU_A = 0.044715
F32 = jnp.float32
BF16 = jnp.bfloat16
ANY = pl.ANY
VMEM = pltpu.VMEM


def gelu_tanh(pre_act):
    inner_arg = GELU_C * (pre_act + GELU_A * pre_act * pre_act * pre_act)
    return 0.5 * pre_act * (1.0 + jnp.tanh(inner_arg))


def gelu_slope(pre_act):
    inner_arg = GELU_C * (pre_act + GELU_A * pre_act * pre_act * pre_act)
    tanh_val = jnp.tanh(inner_arg)
    return (0.5 * (1.0 + tanh_val)
            + 0.5 * pre_act * (1.0 - tanh_val * tanh_val) * GELU_C * (1.0 + 3.0 * GELU_A * pre_act * pre_act))


BLOCK = 512
SEMS = 32
LINK = {'1+': 85e3, '1-': 85e3, '2+': 85e3, '2-': 85e3, 'D': 450e3}
LATENCY = 2.3
TICK = 0.3


class Comm:
    def __init__(self, n, rows, cols):
        self.side = math.isqrt(n // 2)
        assert self.side == 4 and 2 * self.side * self.side == n
        self.rows, self.cols = rows, cols
        self.blk = BLOCK
        self.streams = rows // BLOCK
        self.half = self.blk // 2
        self.l1 = self.half // self.side
        self.l2 = self.l1 // self.side
        self.hw = cols // 2

    N_SCRATCH = 12

    def scratch(self):
        l1, l2, w, hw, ns = self.l1, self.l2, self.cols, self.hw, self.streams
        return [
            VMEM((ns, self.half, w), BF16),
            VMEM((ns, self.half, w), BF16),
            VMEM((ns, 6, l1, hw), BF16),
            VMEM((ns, 6, l2, hw), BF16),
            VMEM((self.rows, w), BF16),
            VMEM((ns, l2, w), BF16),
            VMEM((ns, l2, w), BF16),
            VMEM((self.rows, 128), F32),
            VMEM((self.rows, 128), F32),
            pltpu.SemaphoreType.DMA((ns, SEMS)),
            pltpu.SemaphoreType.DMA((ns, SEMS)),
            pltpu.SemaphoreType.DMA((ns, 8)),
            pltpu.SemaphoreType.REGULAR((ns,)),
        ]

    def bind(self, part, saved, resid, mean, rstd, gain, out, scratch):
        (self.own, self.pair, self.ring1, self.ring2, self.full, self.zrow, self.rrow, self.mu, self.rs,
         self.ssem, self.rsem, self.lsem, self.freed) = scratch
        self.part, self.saved, self.resid, self.gain, self.out = part, saved, resid, gain, out
        self.mean, self.rstd = mean, rstd
        side = self.side
        me = lax.axis_index('tp')
        core = lax.rem(me, 2)
        x = lax.rem(lax.div(me, 2), side)
        y = lax.div(me, 2 * side)
        self.core = core
        self.p1 = x * (1 - core) + y * core
        self.p2 = y * (1 - core) + x * core

        def dev(p1, p2):
            p1, p2 = lax.rem(p1 + side, side), lax.rem(p2 + side, side)
            xx = p1 * (1 - core) + p2 * core
            yy = p2 * (1 - core) + p1 * core
            return (yy * side + xx) * 2 + core

        self.partner = me + 1 - 2 * core
        self.ring_devs = {1: (dev(self.p1 + 1, self.p2), dev(self.p1 - 1, self.p2)),
                          2: (dev(self.p1, self.p2 + 1), dev(self.p1, self.p2 - 1))}
        self.sent = []

    def m(self, j):
        return lax.rem(j + self.side, self.side)

    def ds(self, off, size):
        return pl.ds(pl.multiple_of(off, 16), size)

    def half_rows(self, s, which):
        c = self.core if which == 0 else 1 - self.core
        return self.ds(s * self.blk + c * self.half, self.half)

    def copies(self, s):
        side, l1, l2, hw, w = self.side, self.l1, self.l2, self.hw, self.cols
        c, p1, p2, m, ds = self.core, self.p1, self.p2, self.m, self.ds
        left, right = pl.ds(0, hw), pl.ds(hw, hw)
        own, full = self.own.at[s], self.full
        row0 = s * self.blk
        out = {}
        source = self.full if self.part is None else self.part
        out['pair'] = (0, source.at[self.half_rows(s, 1), :], self.pair.at[s], self.partner)

        def ring(tag, first, base, size, p, bufs, devs):
            plus, minus = devs

            def chunk(j, cols):
                return own.at[ds(base + m(j) * size, size), cols]

            out[tag + 'xp'] = (first + 0, chunk(p + 2, left), bufs.at[s, 0], plus)
            out[tag + 'xm'] = (first + 1, chunk(p + 2, right), bufs.at[s, 1], minus)
            out[tag + 'dp'] = (first + 2, chunk(p + 1, right), bufs.at[s, 2], plus)
            out[tag + 'dm'] = (first + 3, chunk(p - 1, left), bufs.at[s, 3], minus)
            out[tag + 'rp'] = (first + 4, chunk(p + 1, left), bufs.at[s, 4], plus)
            out[tag + 'rm'] = (first + 5, chunk(p - 1, right), bufs.at[s, 5], minus)

        ring('a', 1, 0, l1, p1, self.ring1, self.ring_devs[1])
        ring('b', 7, p1 * l1, l2, p2, self.ring2, self.ring_devs[2])

        def gather(tag, first, base, size, p, devs):
            plus, minus = devs

            def chunk(j, cols):
                return full.at[ds(base + m(j) * size, size), cols]

            every = pl.ds(0, w)
            for name, idx, view, to in (('sp', 0, chunk(p, every), plus), ('sm', 1, chunk(p, every), minus),
                                        ('yp', 2, chunk(p - 1, left), plus), ('ym', 3, chunk(p + 1, right), minus)):
                out[tag + name] = (first + idx, view, view, to)

        half0 = row0 + c * self.half
        gather('c', 13, half0 + p1 * l1, l2, p2, self.ring_devs[2])
        gather('d', 17, half0, l1, p1, self.ring_devs[1])
        for j in range(side):
            view = full.at[ds(half0 + m(p1 + j) * l1, l1), :]
            out['k%d' % j] = (21 + j, view, view, self.partner)
        return out

    def get(self, s, name):
        idx, src, dst, to = self.copies(s)[name]
        return pltpu.make_async_remote_copy(src_ref=src, dst_ref=dst, send_sem=self.ssem.at[s, idx],
                                            recv_sem=self.rsem.at[s, idx], device_id={'tp': to},
                                            device_id_type=pl.DeviceIdType.MESH)

    def start(self, s, *names):
        for name in names:
            self.get(s, name).start()
            self.sent.append((s, name))

    def arrived(self, s, *names):
        for name in names:
            self.get(s, name).wait_recv()

    def mine(self, s):
        return self.ds(s * self.blk + self.core * self.half + self.p1 * self.l1 + self.p2 * self.l2, self.l2)

    def local(self, s, idx):
        if idx == 0:
            src, dst = self.part.at[self.half_rows(s, 0), :], self.own.at[s]
        elif idx == 1:
            src, dst = self.saved.at[self.mine(s), :], self.zrow.at[s]
        elif idx == 2:
            src, dst = self.resid.at[self.mine(s), :], self.rrow.at[s]
        else:
            rows = self.half_rows(s, idx - 4)
            src, dst = self.full.at[rows, :], self.out.at[rows, :]
        return pltpu.make_async_copy(src, dst, self.lsem.at[s, idx])

    def barrier(self):
        sem = pltpu.get_barrier_semaphore()
        peers = (self.partner,) + self.ring_devs[1] + self.ring_devs[2]
        for peer in peers:
            pl.semaphore_signal(sem, inc=1, device_id={'tp': peer}, device_id_type=pl.DeviceIdType.MESH)
        pl.semaphore_wait(sem, len(peers))

    def columns(self):
        per = self.mean.shape[1]
        for src, dst in ((self.mean, self.mu), (self.rstd, self.rs)):
            for i in range(self.rows // 128):
                b, off = divmod(i * 128, per)
                row = src[b:b + 1, off:off + 128]
                dst[pl.ds(i * 128, 128), :] = jnp.transpose(jnp.broadcast_to(row, (128, 128)))

    def begin(self):
        for s in range(self.streams):
            if self.part is not None:
                self.local(s, 0).start()
            self.local(s, 1).start()
            self.local(s, 2).start()
        self.barrier()
        if self.part is not None:
            for s in range(self.streams):
                self.start(s, 'pair')
        self.columns()

    def rs1_start(self, s):
        if self.part is not None:
            self.local(s, 0).wait()
        self.arrived(s, 'pair')
        step = self.l1

        def add(i, carry):
            rows = pl.ds(pl.multiple_of(i * step, step), step)
            self.own[s, rows, :] = (self.own[s, rows, :].astype(F32) + self.pair[s, rows, :].astype(F32)).astype(BF16)
            return carry

        lax.fori_loop(0, self.half // step, add, 0)
        self.start(s, 'axp', 'axm', 'adp', 'adm')
        if self.part is None:
            self.get(s, 'pair').wait_send()
            pl.semaphore_signal(self.freed.at[s], inc=1, device_id={'tp': self.partner},
                                device_id_type=pl.DeviceIdType.MESH)

    def relay(self, s, tag, bufs, base, size, p):
        for buf, j, col0, got, nxt in ((0, p + 1, 0, 'xp', 'rp'), (1, p - 1, self.hw, 'xm', 'rm')):
            self.arrived(s, tag + got)
            rows = self.ds(base + self.m(j) * size, size)
            cols = pl.ds(col0, self.hw)
            self.own[s, rows, cols] = (self.own[s, rows, cols].astype(F32) + bufs[s, buf].astype(F32)).astype(BF16)
            self.start(s, tag + nxt)

    def final(self, s, tag, bufs, base, size, p):
        self.arrived(s, tag + 'rp', tag + 'dm', tag + 'rm', tag + 'dp')
        rows = self.ds(base + p * size, size)
        sums = []
        for col0, one, two in ((0, 4, 3), (self.hw, 5, 2)):
            sums.append(self.own[s, rows, pl.ds(col0, self.hw)].astype(F32)
                        + bufs[s, one].astype(F32) + bufs[s, two].astype(F32))
        return rows, sums

    def rs1_relay(self, s):
        self.relay(s, 'a', self.ring1, 0, self.l1, self.p1)

    def rs2_start(self, s):
        rows, sums = self.final(s, 'a', self.ring1, 0, self.l1, self.p1)
        for k in range(2):
            self.own[s, rows, pl.ds(k * self.hw, self.hw)] = sums[k].astype(BF16)
        self.start(s, 'bxp', 'bxm', 'bdp', 'bdm')

    def rs2_relay(self, s):
        self.relay(s, 'b', self.ring2, self.p1 * self.l1, self.l2, self.p2)

    def norm_gather(self, s):
        _, sums = self.final(s, 'b', self.ring2, self.p1 * self.l1, self.l2, self.p2)
        self.local(s, 1).wait()
        self.local(s, 2).wait()
        mine = self.mine(s)
        mu = self.mu[mine, 0:1]
        r = self.rs[mine, 0:1]
        us, xs = [], []
        for k in range(2):
            cols = pl.ds(k * self.hw, self.hw)
            us.append(sums[k] * self.gain[:, cols].astype(F32))
            xs.append((self.zrow[s, :, cols].astype(F32) - mu) * r)
        inv = 1.0 / self.cols
        mean_u = (jnp.sum(us[0], axis=-1, keepdims=True) + jnp.sum(us[1], axis=-1, keepdims=True)) * inv
        mean_c = (jnp.sum(us[0] * xs[0], axis=-1, keepdims=True)
                  + jnp.sum(us[1] * xs[1], axis=-1, keepdims=True)) * inv
        for k in range(2):
            cols = pl.ds(k * self.hw, self.hw)
            grad = self.rrow[s, :, cols].astype(F32) + r * (us[k] - mean_u - xs[k] * mean_c)
            self.full[mine, cols] = grad.astype(BF16)
        self.start(s, 'csp', 'csm')

    def ag2_relay(self, s):
        self.arrived(s, 'csp')
        self.start(s, 'cyp')
        self.arrived(s, 'csm')
        self.start(s, 'cym')

    def ag1_start(self, s):
        self.arrived(s, 'cyp', 'cym')
        if self.part is None:
            pl.semaphore_wait(self.freed.at[s], 1)
        self.start(s, 'dsp', 'dsm', 'k0')

    def ag1_relay(self, s):
        self.arrived(s, 'dsp')
        self.start(s, 'dyp')
        self.arrived(s, 'dsm')
        self.start(s, 'dym', 'k3', 'k1')

    def ag1_final(self, s):
        self.arrived(s, 'dyp', 'dym')
        self.start(s, 'k2')
        self.local(s, 4).start()

    def finish(self, s):
        self.arrived(s, 'k0', 'k1', 'k2', 'k3')
        self.local(s, 5).start()

    def end(self):
        for s, name in self.sent:
            if name != 'pair' or self.part is not None:
                self.get(s, name).wait_send()
        for s in range(self.streams):
            self.local(s, 4).wait()
            self.local(s, 5).wait()

    def stages(self):
        x1, x2 = self.l1 * self.hw * 2, self.l2 * self.hw * 2
        return [
            ('rs1_start', ['pair', 'own'], [('axp', '1+', x1), ('axm', '1-', x1), ('adp', '1+', x1), ('adm', '1-', x1)]),
            ('rs1_relay', ['axp', 'axm'], [('arp', '1+', x1), ('arm', '1-', x1)]),
            ('rs2_start', ['arp', 'arm', 'adp', 'adm'],
             [('bxp', '2+', x2), ('bxm', '2-', x2), ('bdp', '2+', x2), ('bdm', '2-', x2)]),
            ('rs2_relay', ['bxp', 'bxm'], [('brp', '2+', x2), ('brm', '2-', x2)]),
            ('norm_gather', ['brp', 'brm', 'bdp', 'bdm'], [('csp', '2+', 2 * x2), ('csm', '2-', 2 * x2)]),
            ('ag2_relay', ['csp', 'csm'], [('cyp', '2+', x2), ('cym', '2-', x2)]),
            ('ag1_start', ['cyp', 'cym'], [('dsp', '1+', 2 * x1), ('dsm', '1-', 2 * x1), ('k0', 'D', 2 * x1)]),
            ('ag1_relay', ['dsp', 'dsm'], [('dyp', '1+', x1), ('dym', '1-', x1), ('k3', 'D', 2 * x1), ('k1', 'D', 2 * x1)]),
            ('ag1_final', ['dyp', 'dym'], [('k2', 'D', 2 * x1)]),
            ('finish', ['k0', 'k1', 'k2', 'k3'], []),
        ]

    def plan(self, points):
        stages = self.stages()
        pair_bytes = self.half * self.cols * 2
        free = dict.fromkeys(LINK, 0.0)
        done = {}
        at = [0] * self.streams
        now = 0.0

        def push(s, name, link, size):
            free[link] = max(free[link], now) + size / LINK[link]
            done[s, name] = free[link] + LATENCY

        def ready(s):
            if at[s] >= len(stages):
                return math.inf
            return max(done.get((s, need), math.inf) for need in stages[at[s]][1])

        plans = []
        for i, (cost, gives) in enumerate(points):
            now += cost
            todo = []
            for s, what in gives:
                if what == 'pair':
                    push(s, 'pair', 'D', pair_bytes)
                    if self.part_given is False:
                        todo.append(('send_pair', s))
                else:
                    done[s, 'own'] = now
            last = i == len(points) - 1
            while True:
                s = min(range(self.streams), key=ready)
                t = ready(s)
                if t == math.inf or (t > now and not last):
                    break
                now = max(now, t) + TICK
                name, _, sends = stages[at[s]]
                for copy, link, size in sends:
                    push(s, copy, link, size)
                at[s] += 1
                todo.append((name, s))
            plans.append(todo)
        assert all(a == len(stages) for a in at)
        self.estimate = now
        return plans

    def send_pair(self, s):
        self.start(s, 'pair')

    part_given = False


VMEM_LIMIT = 64 * 1024 * 1024 - 64 * 1024


def dot(a, b, ca=1, cb=0):
    return lax.dot_general(a, b, (((ca,), (cb,)), ((), ())), preferred_element_type=F32)


def mlp_stage(n, h1, dy, mean, rstd, gain, w_up, w_down, cid):
    rows, cols = h1.shape
    ffn = w_up.shape[1]
    comm = Comm(n, rows, cols)
    tile = comm.half
    n_tiles = rows // tile
    cb = 256
    n_cols = cols // cb
    grid = n_tiles + n_cols
    points = []
    for i in range(n_tiles):
        points += [(1.6, []), (1.2, []), (1.2, [(i // 2, 'pair' if i % 2 == 0 else 'own')])]
    for i in range(n_cols):
        points += [(0.6, []), (0.8, []), (0.8, [])]
    plans = comm.plan(points)

    def kernel(h1_tile, dy_tile, h1_col, dy_col, w1, w2, mean_ref, rstd_ref, gain_ref, h1_all, dy_all,
               dh1_ref, dw1_ref, dw2_ref, act, da, *scratch):
        comm.bind(None, h1_all, dy_all, mean_ref, rstd_ref, gain_ref, dh1_ref, scratch)
        i = pl.program_id(0)
        full, own = comm.full, comm.own

        def ticks(steps, k):
            for step in steps:
                todo = plans[step * 3 + k]
                if todo:
                    @pl.when(i == step)
                    def _():
                        for name, s in todo:
                            getattr(comm, name)(s)

        @pl.when(i == 0)
        def _():
            comm.begin()

        first = range(n_tiles)
        rest = range(n_tiles, grid)
        tidx = lax.div(i, 2) * 2 + lax.rem(i, 2) * comm.core + (1 - lax.rem(i, 2)) * (1 - comm.core)
        trow = pl.ds(pl.multiple_of(tidx * tile, tile), tile)
        pre_ref, dg_ref = comm.pre, comm.dg

        @pl.when(i < n_tiles)
        def _():
            z = (h1_tile[...].astype(F32) - comm.mu[trow, 0:1]) * comm.rs[trow, 0:1]
            n2 = (z * gain_ref[...]).astype(BF16)
            pre_ref[...] = dot(n2, w1[...])
        ticks(first, 0)

        @pl.when(i < n_tiles)
        def _():
            dg_ref[...] = dot(dy_tile[...], w2[...], 1, 1)
        ticks(first, 1)

        @pl.when(i < n_tiles)
        def _():
            pre = pre_ref[...]
            act[trow, :] = gelu_tanh(pre).astype(BF16)
            grad_pre = (dg_ref[...] * gelu_slope(pre)).astype(BF16)
            da[trow, :] = grad_pre
            part = dot(grad_pre, w1[...], 1, 1).astype(BF16)

            @pl.when(lax.rem(i, 2) == 0)
            def _():
                full[trow, :] = part

            @pl.when(lax.rem(i, 2) == 1)
            def _():
                own[lax.div(i, 2)] = part
        ticks(first, 2)

        @pl.when(i >= n_tiles)
        def _():
            c0 = pl.multiple_of((i - n_tiles) * cb, cb)
            z = (h1_col[...].astype(F32) - comm.mu[:, 0:1]) * comm.rs[:, 0:1]
            comm.n2c[...] = (z * gain_ref[:, pl.ds(c0, cb)]).astype(BF16)
        ticks(rest, 0)

        @pl.when(i >= n_tiles)
        def _():
            dw1_ref[...] = dot(comm.n2c[...], da[...], 0, 0).astype(BF16)
        ticks(rest, 1)

        @pl.when(i >= n_tiles)
        def _():
            dw2_ref[...] = dot(act[...], dy_col[...], 0, 0).astype(BF16)
        ticks(rest, 2)

        @pl.when(i == grid - 1)
        def _():
            comm.end()

    def wrapped(*refs):
        *most, pre, dg, n2c = refs
        comm.pre, comm.dg, comm.n2c = pre, dg, n2c
        kernel(*most)

    def tile_map(i):
        core = lax.rem(lax.axis_index('tp'), 2)
        ii = jnp.minimum(i, n_tiles - 1)
        odd = lax.rem(ii, 2)
        return lax.div(ii, 2) * 2 + odd * core + (1 - odd) * (1 - core), 0

    def col_at(i):
        return jnp.maximum(i - n_tiles, 0)

    whole = pl.BlockSpec(memory_space=VMEM)
    hbm = pl.BlockSpec(memory_space=ANY)
    return pl.pallas_call(
        wrapped,
        grid=(grid,),
        out_shape=(jax.ShapeDtypeStruct((rows, cols), BF16), jax.ShapeDtypeStruct((cols, ffn), BF16),
                   jax.ShapeDtypeStruct((ffn, cols), BF16)),
        in_specs=[pl.BlockSpec((tile, cols), tile_map), pl.BlockSpec((tile, cols), tile_map),
                  pl.BlockSpec((rows, cb), lambda i: (0, col_at(i))), pl.BlockSpec((rows, cb), lambda i: (0, col_at(i))),
                  whole, whole, whole, whole, whole, hbm, hbm],
        out_specs=(hbm, pl.BlockSpec((cb, ffn), lambda i: (col_at(i), 0)),
                   pl.BlockSpec((ffn, cb), lambda i: (0, col_at(i)))),
        scratch_shapes=[VMEM((rows, ffn), BF16), VMEM((rows, ffn), BF16)] + comm.scratch()
        + [VMEM((tile, ffn), F32), VMEM((tile, ffn), F32), VMEM((rows, cb), BF16)],
        compiler_params=pltpu.CompilerParams(collective_id=cid, has_side_effects=True, vmem_limit_bytes=VMEM_LIMIT,
                                             dimension_semantics=('arbitrary',)),
        name='mlp_stage',
    )(h1, dy, h1, dy, w_up, w_down, mean, rstd, gain, h1, dy)


def attention_stage(n, mbs, x, dh1, mean, rstd, gain, w_qkv, w_out, score_scale, cid):
    rows, cols = x.shape
    seq = rows // mbs
    hd = w_out.shape[0]
    qkv_w = w_qkv.shape[1]
    comm = Comm(n, rows, cols)
    tile = comm.half
    per_mb = seq // tile
    n_seq = 2 * per_mb * mbs
    cb = 256
    n_cols = cols // cb
    grid = n_seq + n_cols
    points = []
    for b in range(mbs):
        points += [(1.4, []), (0.4, []), (0.4, [])] * per_mb
        for j in range(per_mb - 1, -1, -1):
            s = b * (per_mb // 2) + j // 2
            points += [(1.4, []), (1.4, []), (1.2, [(s, 'pair'), (s, 'own')] if j % 2 == 0 else [])]
    for i in range(n_cols):
        points += [(0.7, []), (0.8, []), (0.6, [])]
    plans = comm.plan(points)

    def kernel(x_tile, dh_tile, x_col, dh_col, wqkv, wo, mean_ref, rstd_ref, gain_ref, x_all, dh_all,
               dx_ref, dwqkv_ref, dwo_ref, qkv, do, o_all, dqkv, dk_acc, dv_acc, n1c, p_ref, *scratch):
        comm.bind(None, x_all, dh_all, mean_ref, rstd_ref, gain_ref, dx_ref, scratch)
        i = pl.program_id(0)
        full, own = comm.full, comm.own

        def ticks(steps, k):
            for step in steps:
                todo = plans[step * 3 + k]
                if todo:
                    @pl.when(i == step)
                    def _():
                        for name, s in todo:
                            getattr(comm, name)(s)

        @pl.when(i == 0)
        def _():
            comm.begin()

        span = 2 * per_mb
        first = range(n_seq)
        rest = range(n_seq, grid)
        b = lax.div(i, span)
        at = lax.rem(i, span)
        in_seq = i < n_seq
        loading = jnp.logical_and(in_seq, at < per_mb)
        base = b * seq
        trow = pl.ds(pl.multiple_of(jnp.minimum(base + at * tile, rows - tile), tile), tile)

        @pl.when(loading)
        def _():
            z = (x_tile[...].astype(F32) - comm.mu[trow, 0:1]) * comm.rs[trow, 0:1]
            n1 = (z * gain_ref[...]).astype(BF16)
            qkv[trow, :] = dot(n1, wqkv[...]).astype(BF16)

        def variants(fn):
            for j in range(per_mb):
                @pl.when(jnp.logical_and(in_seq, at == 2 * per_mb - 1 - j))
                def _():
                    fn(j)

        def part_a(j):
            size = (j + 1) * tile
            mine = pl.ds(pl.multiple_of(base + j * tile, tile), tile)
            keys = pl.ds(pl.multiple_of(base, tile), size)
            s = dot(qkv[mine, 0:hd], qkv[keys, hd:2 * hd], 1, 1) * score_scale
            row = lax.broadcasted_iota(jnp.int32, (tile, size), 0) + j * tile
            col = lax.broadcasted_iota(jnp.int32, (tile, size), 1)
            s = jnp.where(row >= col, s, -1e30)
            e = jnp.exp(s - jnp.max(s, axis=-1, keepdims=True))
            p = e / jnp.sum(e, axis=-1, keepdims=True)
            p_ref[:, 0:size] = p
            pb = p.astype(BF16)
            o_all[mine, :] = dot(pb, qkv[keys, 2 * hd:3 * hd]).astype(BF16)
            dv = dot(pb, do[mine, :], 0, 0)
            if j == per_mb - 1:
                dv_acc[...] = dv
            else:
                dv_acc[0:size, :] += dv

        def part_b(j):
            size = (j + 1) * tile
            mine = pl.ds(pl.multiple_of(base + j * tile, tile), tile)
            keys = pl.ds(pl.multiple_of(base, tile), size)
            p = p_ref[:, 0:size]
            dp = dot(do[mine, :], qkv[keys, 2 * hd:3 * hd], 1, 1)
            rd = jnp.sum(p * dp, axis=-1, keepdims=True)
            ds = (p * (dp - rd) * score_scale).astype(BF16)
            dqkv[mine, 0:hd] = dot(ds, qkv[keys, hd:2 * hd]).astype(BF16)
            dk = dot(ds, qkv[mine, 0:hd], 0, 0)
            if j == per_mb - 1:
                dk_acc[...] = dk
            else:
                dk_acc[0:size, :] += dk
            dqkv[mine, hd:2 * hd] = dk_acc[j * tile:size, :].astype(BF16)
            dqkv[mine, 2 * hd:3 * hd] = dv_acc[j * tile:size, :].astype(BF16)

        def part_c(j):
            mine = pl.ds(pl.multiple_of(base + j * tile, tile), tile)
            part = dot(dqkv[mine, :], wqkv[...], 1, 1).astype(BF16)

            @pl.when(comm.core == j % 2)
            def _():
                own[b * (per_mb // 2) + j // 2] = part

            @pl.when(comm.core != j % 2)
            def _():
                full[mine, :] = part

        variants(part_a)
        ticks(first, 0)

        @pl.when(loading)
        def _():
            do[trow, :] = dot(dh_tile[...], wo[...], 1, 1).astype(BF16)

        variants(part_b)
        ticks(first, 1)
        variants(part_c)
        ticks(first, 2)

        @pl.when(i >= n_seq)
        def _():
            c0 = pl.multiple_of((i - n_seq) * cb, cb)
            z = (x_col[...].astype(F32) - comm.mu[:, 0:1]) * comm.rs[:, 0:1]
            n1c[...] = (z * gain_ref[:, pl.ds(c0, cb)]).astype(BF16)
        ticks(rest, 0)

        @pl.when(i >= n_seq)
        def _():
            dwqkv_ref[...] = dot(n1c[...], dqkv[...], 0, 0).astype(BF16)
        ticks(rest, 1)

        @pl.when(i >= n_seq)
        def _():
            dwo_ref[...] = dot(o_all[...], dh_col[...], 0, 0).astype(BF16)
        ticks(rest, 2)

        @pl.when(i == grid - 1)
        def _():
            comm.end()

    def tile_map(i):
        ii = jnp.minimum(i, n_seq - 1)
        return lax.div(ii, 2 * per_mb) * per_mb + jnp.minimum(lax.rem(ii, 2 * per_mb), per_mb - 1), 0

    def col_at(i):
        return jnp.maximum(i - n_seq, 0)

    whole = pl.BlockSpec(memory_space=VMEM)
    hbm = pl.BlockSpec(memory_space=ANY)
    return pl.pallas_call(
        kernel,
        grid=(grid,),
        out_shape=(jax.ShapeDtypeStruct((rows, cols), BF16), jax.ShapeDtypeStruct((cols, qkv_w), BF16),
                   jax.ShapeDtypeStruct((hd, cols), BF16)),
        in_specs=[pl.BlockSpec((tile, cols), tile_map), pl.BlockSpec((tile, cols), tile_map),
                  pl.BlockSpec((rows, cb), lambda i: (0, col_at(i))), pl.BlockSpec((rows, cb), lambda i: (0, col_at(i))),
                  whole, whole, whole, whole, whole, hbm, hbm],
        out_specs=(hbm, pl.BlockSpec((cb, qkv_w), lambda i: (col_at(i), 0)),
                   pl.BlockSpec((hd, cb), lambda i: (0, col_at(i)))),
        scratch_shapes=[VMEM((rows, qkv_w), BF16), VMEM((rows, hd), BF16), VMEM((rows, hd), BF16),
                        VMEM((rows, qkv_w), BF16), VMEM((seq, hd), F32), VMEM((seq, hd), F32), VMEM((rows, cb), BF16),
                        VMEM((tile, seq), F32)] + comm.scratch(),
        compiler_params=pltpu.CompilerParams(collective_id=cid, has_side_effects=True, vmem_limit_bytes=VMEM_LIMIT,
                                             dimension_semantics=('arbitrary',)),
        name='attention_stage',
    )(x, dh1, x, dh1, w_qkv, w_out, mean, rstd, gain, x, dh1)


def spread_copy(arr):
    rows, cols = arr.shape
    tile = 256

    def kernel(src, dst):
        dst[...] = src[...]

    return pl.pallas_call(
        kernel,
        grid=(rows // tile,),
        out_shape=jax.ShapeDtypeStruct(arr.shape, arr.dtype),
        in_specs=[pl.BlockSpec((tile, cols), lambda i: (i, 0))],
        out_specs=pl.BlockSpec((tile, cols), lambda i: (i, 0)),
        name='spread_copy',
    )(arr)


def solution(mesh):
    act_spec = P('dp', None, None)
    stat_spec = P('dp', None)
    in_specs = (act_spec, act_spec, act_spec, stat_spec, stat_spec, stat_spec, stat_spec, P(), P(),
                P(None, 'tp', None, None), P('tp', None, None), P(None, 'tp'), P('tp', None))
    out_specs = (act_spec, P('dp', 'tp', None, None), P(('dp', 'tp'), None, None), P('dp', 'tp'),
                 P(('dp', 'tp'), None))
    n = mesh.shape['tp']

    def local_backward(x_saved, h1_saved, grad_y, mean_one, rstd_one, mean_two, rstd_two,
                       gain_one, gain_two, w_qkv, w_out, w_up, w_down):
        score_scale = w_qkv.shape[3] ** -0.5
        shape = x_saved.shape
        flat = (shape[0] * shape[1], shape[2])
        g1, g2 = gain_one.astype(F32)[None, :], gain_two.astype(F32)[None, :]
        dh1, grad_up, grad_down = mlp_stage(n, h1_saved.reshape(flat), grad_y.reshape(flat), mean_two, rstd_two, g2,
                                            w_up, w_down, 0)
        heads, _, width = w_qkv.shape[1:]
        pad = -width % 128
        wide_qkv = jnp.pad(w_qkv[:, 0], ((0, 0), (0, 0), (0, pad))).reshape(flat[1], -1)
        wide_out = jnp.pad(w_out[0], ((0, pad), (0, 0)))
        dx, dqkv_w, dout_w = attention_stage(n, shape[0], x_saved.reshape(flat), dh1, mean_one, rstd_one, g1,
                                             wide_qkv, wide_out, score_scale, 1)
        grad_qkv_w = dqkv_w.reshape(flat[1], heads, 3, width + pad)[..., :width]
        grad_out_w = dout_w[None, :width]
        return spread_copy(dx).reshape(shape), grad_qkv_w, grad_out_w, grad_up, grad_down

    return jax.shard_map(local_backward, mesh=mesh, in_specs=in_specs, out_specs=out_specs, check_vma=False)
```

```python
import math
import jax
import jax.numpy as jnp
from jax import lax
from jax.experimental import pallas as pl
from jax.experimental.pallas import tpu as pltpu
from jax.sharding import PartitionSpec as P

GELU_C = 0.7978845608028654
GELU_A = 0.044715
F32 = jnp.float32
BF16 = jnp.bfloat16
ANY = pl.ANY
VMEM = pltpu.VMEM


def gelu_tanh(pre_act):
    inner_arg = GELU_C * (pre_act + GELU_A * pre_act * pre_act * pre_act)
    return 0.5 * pre_act * (1.0 + jnp.tanh(inner_arg))


def gelu_slope(pre_act):
    inner_arg = GELU_C * (pre_act + GELU_A * pre_act * pre_act * pre_act)
    tanh_val = jnp.tanh(inner_arg)
    return (0.5 * (1.0 + tanh_val)
            + 0.5 * pre_act * (1.0 - tanh_val * tanh_val) * GELU_C * (1.0 + 3.0 * GELU_A * pre_act * pre_act))


BLOCK = 512
SEMS = 32
LINK = {'+': 90e3, '-': 90e3, 'D': 450e3}
LATENCY = 2.6
TICK = 0.3


class Comm:
    def __init__(self, n, rows, cols):
        self.side = math.isqrt(n // 2)
        assert self.side == 4 and 2 * self.side * self.side == n
        self.rows, self.cols = rows, cols
        self.blk = BLOCK
        self.streams = rows // BLOCK
        self.half = self.blk // 2
        self.l1 = self.half // self.side
        self.l2 = self.l1 // self.side
        self.hw = cols // 2

    N_SCRATCH = 12

    def scratch(self):
        l1, l2, w, hw, ns = self.l1, self.l2, self.cols, self.hw, self.streams
        return [
            VMEM((ns, self.half, w), BF16),
            VMEM((ns, self.half, w), BF16),
            VMEM((ns, 6, l1, hw), BF16),
            VMEM((ns, 6, l2, hw), BF16),
            VMEM((self.rows, w), BF16),
            VMEM((ns, l2, w), BF16),
            VMEM((ns, l2, w), BF16),
            VMEM((self.rows, 128), F32),
            VMEM((self.rows, 128), F32),
            VMEM((1, w), F32),
            pltpu.SemaphoreType.DMA((ns, SEMS)),
            pltpu.SemaphoreType.DMA((ns, SEMS)),
            pltpu.SemaphoreType.DMA((ns, 8)),
            pltpu.SemaphoreType.REGULAR((ns,)),
        ]

    def bind(self, part, saved, resid, mean, rstd, gain, out, scratch):
        (self.own, self.pair, self.ring1, self.ring2, self.full, self.zrow, self.rrow, self.mu, self.rs, self.gain,
         self.ssem, self.rsem, self.lsem, self.freed) = scratch
        self.part, self.saved, self.resid, self.gain_in, self.out = part, saved, resid, gain, out
        self.mean, self.rstd = mean, rstd
        side = self.side
        me = lax.axis_index('tp')
        core = lax.rem(me, 2)
        x = lax.rem(lax.div(me, 2), side)
        y = lax.div(me, 2 * side)
        self.core = core
        self.p1 = x * (1 - core) + y * core
        self.p2 = y * (1 - core) + x * core

        def dev(p1, p2):
            p1, p2 = lax.rem(p1 + side, side), lax.rem(p2 + side, side)
            xx = p1 * (1 - core) + p2 * core
            yy = p2 * (1 - core) + p1 * core
            return (yy * side + xx) * 2 + core

        self.partner = me + 1 - 2 * core
        self.ring_devs = {1: (dev(self.p1 + 1, self.p2), dev(self.p1 - 1, self.p2)),
                          2: (dev(self.p1, self.p2 + 1), dev(self.p1, self.p2 - 1))}
        self.sent = []

    def m(self, j):
        return lax.rem(j + self.side, self.side)

    def ds(self, off, size):
        return pl.ds(pl.multiple_of(off, 16), size)

    def half_rows(self, s, which):
        c = self.core if which == 0 else 1 - self.core
        return self.ds(s * self.blk + c * self.half, self.half)

    def copies(self, s):
        side, l1, l2, hw, w = self.side, self.l1, self.l2, self.hw, self.cols
        c, p1, p2, m, ds = self.core, self.p1, self.p2, self.m, self.ds
        left, right = pl.ds(0, hw), pl.ds(hw, hw)
        own, full = self.own.at[s], self.full
        row0 = s * self.blk
        out = {}
        source = self.full if self.part is None else self.part
        out['pair'] = (0, source.at[self.half_rows(s, 1), :], self.pair.at[s], self.partner)

        def ring(tag, first, base, size, p, bufs, devs):
            plus, minus = devs

            def chunk(j, cols):
                return own.at[ds(base + m(j) * size, size), cols]

            out[tag + 'xp'] = (first + 0, chunk(p + 2, left), bufs.at[s, 0], plus)
            out[tag + 'xm'] = (first + 1, chunk(p + 2, right), bufs.at[s, 1], minus)
            out[tag + 'dp'] = (first + 2, chunk(p + 1, right), bufs.at[s, 2], plus)
            out[tag + 'dm'] = (first + 3, chunk(p - 1, left), bufs.at[s, 3], minus)
            out[tag + 'rp'] = (first + 4, chunk(p + 1, left), bufs.at[s, 4], plus)
            out[tag + 'rm'] = (first + 5, chunk(p - 1, right), bufs.at[s, 5], minus)

        ring('a', 1, 0, l1, p1, self.ring1, self.ring_devs[1])
        ring('b', 7, p1 * l1, l2, p2, self.ring2, self.ring_devs[2])

        def gather(tag, first, base, size, p, devs):
            plus, minus = devs

            def chunk(j, cols):
                return full.at[ds(base + m(j) * size, size), cols]

            every = pl.ds(0, w)
            for name, idx, view, to in (('sp', 0, chunk(p, every), plus), ('sm', 1, chunk(p, every), minus),
                                        ('yp', 2, chunk(p - 1, left), plus), ('ym', 3, chunk(p + 1, right), minus)):
                out[tag + name] = (first + idx, view, view, to)

        half0 = row0 + c * self.half
        gather('c', 13, half0 + p1 * l1, l2, p2, self.ring_devs[2])
        gather('d', 17, half0, l1, p1, self.ring_devs[1])
        for j in range(side):
            view = full.at[ds(half0 + m(p1 + j) * l1, l1), :]
            out['k%d' % j] = (21 + j, view, view, self.partner)
        return out

    def get(self, s, name):
        idx, src, dst, to = self.copies(s)[name]
        return pltpu.make_async_remote_copy(src_ref=src, dst_ref=dst, send_sem=self.ssem.at[s, idx],
                                            recv_sem=self.rsem.at[s, idx], device_id={'tp': to},
                                            device_id_type=pl.DeviceIdType.MESH)

    def start(self, s, *names):
        for name in names:
            self.get(s, name).start()
            self.sent.append((s, name))

    def arrived(self, s, *names):
        for name in names:
            self.get(s, name).wait_recv()

    def mine(self, s):
        return self.ds(s * self.blk + self.core * self.half + self.p1 * self.l1 + self.p2 * self.l2, self.l2)

    def local(self, s, idx):
        if idx == 0:
            src, dst = self.part.at[self.half_rows(s, 0), :], self.own.at[s]
        elif idx == 1:
            src, dst = self.saved.at[self.mine(s), :], self.zrow.at[s]
        elif idx == 2:
            src, dst = self.resid.at[self.mine(s), :], self.rrow.at[s]
        else:
            rows = self.half_rows(s, idx - 4)
            src, dst = self.full.at[rows, :], self.out.at[rows, :]
        return pltpu.make_async_copy(src, dst, self.lsem.at[s, idx])

    def barrier(self):
        sem = pltpu.get_barrier_semaphore()
        peers = (self.partner,) + self.ring_devs[1] + self.ring_devs[2]
        for peer in peers:
            pl.semaphore_signal(sem, inc=1, device_id={'tp': peer}, device_id_type=pl.DeviceIdType.MESH)
        pl.semaphore_wait(sem, len(peers))

    def columns(self):
        self.gain[...] = self.gain_in[...].astype(F32)[None, :]
        per = self.mean.shape[1]
        for src, dst in ((self.mean, self.mu), (self.rstd, self.rs)):
            for i in range(self.rows // 128):
                b, off = divmod(i * 128, per)
                row = src[b:b + 1, off:off + 128]
                dst[pl.ds(i * 128, 128), :] = jnp.transpose(jnp.broadcast_to(row, (128, 128)))

    def begin(self):
        for s in range(self.streams):
            if self.part is not None:
                self.local(s, 0).start()
            self.local(s, 1).start()
            self.local(s, 2).start()
        self.barrier()
        if self.part is not None:
            for s in range(self.streams):
                self.start(s, 'pair')
        self.columns()

    def rs1_start(self, s):
        if self.part is not None:
            self.local(s, 0).wait()
        self.arrived(s, 'pair')
        step = self.l1

        def add(i, carry):
            rows = pl.ds(pl.multiple_of(i * step, step), step)
            self.own[s, rows, :] = (self.own[s, rows, :].astype(F32) + self.pair[s, rows, :].astype(F32)).astype(BF16)
            return carry

        lax.fori_loop(0, self.half // step, add, 0)
        self.start(s, 'axp', 'axm', 'adp', 'adm')
        if self.part is None:
            self.get(s, 'pair').wait_send()
            pl.semaphore_signal(self.freed.at[s], inc=1, device_id={'tp': self.partner},
                                device_id_type=pl.DeviceIdType.MESH)

    def relay(self, s, tag, bufs, base, size, p):
        for buf, j, col0, got, nxt in ((0, p + 1, 0, 'xp', 'rp'), (1, p - 1, self.hw, 'xm', 'rm')):
            self.arrived(s, tag + got)
            rows = self.ds(base + self.m(j) * size, size)
            cols = pl.ds(col0, self.hw)
            self.own[s, rows, cols] = (self.own[s, rows, cols].astype(F32) + bufs[s, buf].astype(F32)).astype(BF16)
            self.start(s, tag + nxt)

    def final(self, s, tag, bufs, base, size, p):
        self.arrived(s, tag + 'rp', tag + 'dm', tag + 'rm', tag + 'dp')
        rows = self.ds(base + p * size, size)
        sums = []
        for col0, one, two in ((0, 4, 3), (self.hw, 5, 2)):
            sums.append(self.own[s, rows, pl.ds(col0, self.hw)].astype(F32)
                        + bufs[s, one].astype(F32) + bufs[s, two].astype(F32))
        return rows, sums

    def rs1_relay(self, s):
        self.relay(s, 'a', self.ring1, 0, self.l1, self.p1)

    def rs2_start(self, s):
        rows, sums = self.final(s, 'a', self.ring1, 0, self.l1, self.p1)
        for k in range(2):
            self.own[s, rows, pl.ds(k * self.hw, self.hw)] = sums[k].astype(BF16)
        self.start(s, 'bxp', 'bxm', 'bdp', 'bdm')

    def rs2_relay(self, s):
        self.relay(s, 'b', self.ring2, self.p1 * self.l1, self.l2, self.p2)

    def norm_gather(self, s):
        _, sums = self.final(s, 'b', self.ring2, self.p1 * self.l1, self.l2, self.p2)
        self.local(s, 1).wait()
        self.local(s, 2).wait()
        mine = self.mine(s)
        mu = self.mu[mine, 0:1]
        r = self.rs[mine, 0:1]
        us, xs = [], []
        for k in range(2):
            cols = pl.ds(k * self.hw, self.hw)
            us.append(sums[k] * self.gain[:, cols])
            xs.append((self.zrow[s, :, cols].astype(F32) - mu) * r)
        inv = 1.0 / self.cols
        mean_u = (jnp.sum(us[0], axis=-1, keepdims=True) + jnp.sum(us[1], axis=-1, keepdims=True)) * inv
        mean_c = (jnp.sum(us[0] * xs[0], axis=-1, keepdims=True)
                  + jnp.sum(us[1] * xs[1], axis=-1, keepdims=True)) * inv
        for k in range(2):
            cols = pl.ds(k * self.hw, self.hw)
            grad = self.rrow[s, :, cols].astype(F32) + r * (us[k] - mean_u - xs[k] * mean_c)
            self.full[mine, cols] = grad.astype(BF16)
        self.start(s, 'csp', 'csm')

    def ag2_relay(self, s):
        self.arrived(s, 'csp')
        self.start(s, 'cyp')
        self.arrived(s, 'csm')
        self.start(s, 'cym')

    def ag1_start(self, s):
        self.arrived(s, 'cyp', 'cym')
        if self.part is None:
            pl.semaphore_wait(self.freed.at[s], 1)
        self.start(s, 'dsp', 'dsm', 'k0')

    def ag1_relay(self, s):
        self.arrived(s, 'dsp')
        self.start(s, 'dyp')
        self.arrived(s, 'dsm')
        self.start(s, 'dym', 'k3', 'k1')

    def ag1_final(self, s):
        self.arrived(s, 'dyp', 'dym')
        self.start(s, 'k2')
        self.local(s, 4).start()

    def finish(self, s):
        self.arrived(s, 'k0', 'k1', 'k2', 'k3')
        self.local(s, 5).start()

    def end(self):
        for s, name in self.sent:
            if name != 'pair' or self.part is not None:
                self.get(s, name).wait_send()
        for s in range(self.streams):
            self.local(s, 4).wait()
            self.local(s, 5).wait()

    def stages(self):
        x1, x2 = self.l1 * self.hw * 2, self.l2 * self.hw * 2
        return [
            ('rs1_start', ['pair', 'own'], [('axp', '+', x1), ('axm', '-', x1), ('adp', '+', x1), ('adm', '-', x1)]),
            ('rs1_relay', ['axp', 'axm'], [('arp', '+', x1), ('arm', '-', x1)]),
            ('rs2_start', ['arp', 'arm', 'adp', 'adm'],
             [('bxp', '+', x2), ('bxm', '-', x2), ('bdp', '+', x2), ('bdm', '-', x2)]),
            ('rs2_relay', ['bxp', 'bxm'], [('brp', '+', x2), ('brm', '-', x2)]),
            ('norm_gather', ['brp', 'brm', 'bdp', 'bdm'], [('csp', '+', 2 * x2), ('csm', '-', 2 * x2)]),
            ('ag2_relay', ['csp', 'csm'], [('cyp', '+', x2), ('cym', '-', x2)]),
            ('ag1_start', ['cyp', 'cym'], [('dsp', '+', 2 * x1), ('dsm', '-', 2 * x1), ('k0', 'D', 2 * x1)]),
            ('ag1_relay', ['dsp', 'dsm'], [('dyp', '+', x1), ('dym', '-', x1), ('k3', 'D', 2 * x1), ('k1', 'D', 2 * x1)]),
            ('ag1_final', ['dyp', 'dym'], [('k2', 'D', 2 * x1)]),
            ('finish', ['k0', 'k1', 'k2', 'k3'], []),
        ]

    def plan(self, points):
        stages = self.stages()
        pair_bytes = self.half * self.cols * 2
        free = dict.fromkeys(LINK, 0.0)
        done = {}
        at = [0] * self.streams
        now = 0.0

        def push(s, name, link, size):
            free[link] = max(free[link], now) + size / LINK[link]
            done[s, name] = free[link] + LATENCY

        def ready(s):
            if at[s] >= len(stages):
                return math.inf
            return max(done.get((s, need), math.inf) for need in stages[at[s]][1])

        plans = []
        for i, (cost, gives) in enumerate(points):
            now += cost
            todo = []
            for s, what in gives:
                if what == 'pair':
                    push(s, 'pair', 'D', pair_bytes)
                    if self.part_given is False:
                        todo.append(('send_pair', s))
                else:
                    done[s, 'own'] = now
            last = i == len(points) - 1
            while True:
                s = min(range(self.streams), key=ready)
                t = ready(s)
                if t == math.inf or (t > now and not last):
                    break
                now = max(now, t) + TICK
                name, _, sends = stages[at[s]]
                for copy, link, size in sends:
                    push(s, copy, link, size)
                at[s] += 1
                todo.append((name, s))
            plans.append(todo)
        assert all(a == len(stages) for a in at)
        self.estimate = now
        return plans

    def send_pair(self, s):
        self.start(s, 'pair')

    part_given = False


VMEM_LIMIT = 64 * 1024 * 1024 - 64 * 1024


def dot(a, b, ca=1, cb=0):
    return lax.dot_general(a, b, (((ca,), (cb,)), ((), ())), preferred_element_type=F32)


def mlp_stage(n, h1, dy, mean, rstd, gain, w_up, w_down, cid):
    rows, cols = h1.shape
    ffn = w_up.shape[1]
    comm = Comm(n, rows, cols)
    tile = comm.half
    n_tiles = rows // tile
    cb = 256
    n_cols = cols // cb
    grid = n_tiles + n_cols
    points = []
    for i in range(n_tiles):
        points += [(1.1 if i else 5.0, []), (0.7, []), (1.4, [(i // 2, 'pair' if i % 2 == 0 else 'own')])]
    for i in range(n_cols):
        points += [(0.5, []), (0.7, []), (0.6, [])]
    plans = comm.plan(points)

    def kernel(h1_tile, dy_tile, h1_col, dy_col, w1, w2, mean_ref, rstd_ref, gain_ref, h1_all, dy_all,
               dh1_ref, dw1_ref, dw2_ref, act, da, *scratch):
        comm.bind(None, h1_all, dy_all, mean_ref, rstd_ref, gain_ref, dh1_ref, scratch)
        i = pl.program_id(0)
        full, own = comm.full, comm.own

        def ticks(steps, k):
            for step in steps:
                todo = plans[step * 3 + k]
                if todo:
                    @pl.when(i == step)
                    def _():
                        for name, s in todo:
                            getattr(comm, name)(s)

        @pl.when(i == 0)
        def _():
            comm.begin()

        first = range(n_tiles)
        rest = range(n_tiles, grid)
        tidx = lax.div(i, 2) * 2 + lax.rem(i, 2) * comm.core + (1 - lax.rem(i, 2)) * (1 - comm.core)
        trow = pl.ds(pl.multiple_of(tidx * tile, tile), tile)
        pre_ref, dg_ref = comm.pre, comm.dg

        @pl.when(i < n_tiles)
        def _():
            z = (h1_tile[...].astype(F32) - comm.mu[trow, 0:1]) * comm.rs[trow, 0:1]
            n2 = (z * comm.gain[...]).astype(BF16)
            pre_ref[...] = dot(n2, w1[...])
        ticks(first, 0)

        @pl.when(i < n_tiles)
        def _():
            dg_ref[...] = dot(dy_tile[...], w2[...], 1, 1)
        ticks(first, 1)

        @pl.when(i < n_tiles)
        def _():
            pre = pre_ref[...]
            act[trow, :] = gelu_tanh(pre).astype(BF16)
            grad_pre = (dg_ref[...] * gelu_slope(pre)).astype(BF16)
            da[trow, :] = grad_pre
            part = dot(grad_pre, w1[...], 1, 1).astype(BF16)

            @pl.when(lax.rem(i, 2) == 0)
            def _():
                full[trow, :] = part

            @pl.when(lax.rem(i, 2) == 1)
            def _():
                own[lax.div(i, 2)] = part
        ticks(first, 2)

        @pl.when(i >= n_tiles)
        def _():
            c0 = pl.multiple_of((i - n_tiles) * cb, cb)
            z = (h1_col[...].astype(F32) - comm.mu[:, 0:1]) * comm.rs[:, 0:1]
            comm.n2c[...] = (z * comm.gain[:, pl.ds(c0, cb)]).astype(BF16)
        ticks(rest, 0)

        @pl.when(i >= n_tiles)
        def _():
            dw1_ref[...] = dot(comm.n2c[...], da[...], 0, 0).astype(BF16)
        ticks(rest, 1)

        @pl.when(i >= n_tiles)
        def _():
            dw2_ref[...] = dot(act[...], dy_col[...], 0, 0).astype(BF16)
        ticks(rest, 2)

        @pl.when(i == grid - 1)
        def _():
            comm.end()

    def wrapped(*refs):
        *most, pre, dg, n2c = refs
        comm.pre, comm.dg, comm.n2c = pre, dg, n2c
        kernel(*most)

    def tile_map(i):
        core = lax.rem(lax.axis_index('tp'), 2)
        ii = jnp.minimum(i, n_tiles - 1)
        odd = lax.rem(ii, 2)
        return lax.div(ii, 2) * 2 + odd * core + (1 - odd) * (1 - core), 0

    def col_at(i):
        return jnp.maximum(i - n_tiles, 0)

    whole = pl.BlockSpec(memory_space=VMEM)
    hbm = pl.BlockSpec(memory_space=ANY)
    return pl.pallas_call(
        wrapped,
        grid=(grid,),
        out_shape=(jax.ShapeDtypeStruct((rows, cols), BF16), jax.ShapeDtypeStruct((cols, ffn), BF16),
                   jax.ShapeDtypeStruct((ffn, cols), BF16)),
        in_specs=[pl.BlockSpec((tile, cols), tile_map), pl.BlockSpec((tile, cols), tile_map),
                  pl.BlockSpec((rows, cb), lambda i: (0, col_at(i))), pl.BlockSpec((rows, cb), lambda i: (0, col_at(i))),
                  whole, whole, whole, whole, whole, hbm, hbm],
        out_specs=(hbm, pl.BlockSpec((cb, ffn), lambda i: (col_at(i), 0)),
                   pl.BlockSpec((ffn, cb), lambda i: (0, col_at(i)))),
        scratch_shapes=[VMEM((rows, ffn), BF16), VMEM((rows, ffn), BF16)] + comm.scratch()
        + [VMEM((tile, ffn), F32), VMEM((tile, ffn), F32), VMEM((rows, cb), BF16)],
        compiler_params=pltpu.CompilerParams(collective_id=cid, has_side_effects=True, vmem_limit_bytes=VMEM_LIMIT,
                                             dimension_semantics=('arbitrary',)),
        name='mlp_stage',
    )(h1, dy, h1, dy, w_up, w_down, mean, rstd, gain, h1, dy)


def attention_stage(n, mbs, x, dh1, mean, rstd, gain, w_qkv, w_out, score_scale, cid):
    rows, cols = x.shape
    seq = rows // mbs
    width = w_out.shape[0]
    hd = width + -width % 128
    qkv_w = 3 * hd
    comm = Comm(n, rows, cols)
    tile = comm.half
    per_mb = seq // tile
    n_seq = 2 * per_mb * mbs
    cb = 256
    n_cols = cols // cb
    grid = n_seq + n_cols
    points = []
    for b in range(mbs):
        points += [(1.1 if b else 2.0, []), (0.4, []), (0.1, [])] * per_mb
        for j in range(per_mb - 1, -1, -1):
            s = b * (per_mb // 2) + j // 2
            points += [(0.8, []), (0.7, []), (1.1, [(s, 'pair'), (s, 'own')] if j % 2 == 0 else [])]
    for i in range(n_cols):
        points += [(0.5, []), (0.7, []), (0.4, [])]
    plans = comm.plan(points)

    def kernel(x_tile, dh_tile, x_col, dh_col, wqkv_in, wo_in, mean_ref, rstd_ref, gain_ref, x_all, dh_all,
               dx_ref, dwqkv_ref, dwo_ref, qkv, do, o_all, dqkv, dk_acc, dv_acc, n1c, p_ref, wqkv, wo, wsem, *scratch):
        comm.bind(None, x_all, dh_all, mean_ref, rstd_ref, gain_ref, dx_ref, scratch)
        i = pl.program_id(0)
        full, own = comm.full, comm.own

        def ticks(steps, k):
            for step in steps:
                todo = plans[step * 3 + k]
                if todo:
                    @pl.when(i == step)
                    def _():
                        for name, s in todo:
                            getattr(comm, name)(s)

        @pl.when(i == 0)
        def _():
            loads = [pltpu.make_async_copy(wqkv_in.at[pl.ds(c * width, width), :], wqkv.at[pl.ds(c * hd, width), :],
                                           wsem.at[c]) for c in range(3)]
            loads.append(pltpu.make_async_copy(wo_in, wo.at[pl.ds(0, width), :], wsem.at[3]))
            for load in loads:
                load.start()
            zero = jnp.zeros((hd - width, cols), BF16)
            for c in range(3):
                wqkv[pl.ds(c * hd + width, hd - width), :] = zero
            wo[pl.ds(width, hd - width), :] = zero
            comm.begin()
            for load in loads:
                load.wait()

        span = 2 * per_mb
        first = range(n_seq)
        rest = range(n_seq, grid)
        b = lax.div(i, span)
        at = lax.rem(i, span)
        in_seq = i < n_seq
        loading = jnp.logical_and(in_seq, at < per_mb)
        base = b * seq
        trow = pl.ds(pl.multiple_of(jnp.minimum(base + at * tile, rows - tile), tile), tile)

        @pl.when(loading)
        def _():
            z = (x_tile[...].astype(F32) - comm.mu[trow, 0:1]) * comm.rs[trow, 0:1]
            n1 = (z * comm.gain[...]).astype(BF16)
            qkv[trow, :] = dot(n1, wqkv[...], 1, 1).astype(BF16)

        def variants(fn):
            for j in range(per_mb):
                @pl.when(jnp.logical_and(in_seq, at == 2 * per_mb - 1 - j))
                def _():
                    fn(j)

        def part_a(j):
            size = (j + 1) * tile
            mine = pl.ds(pl.multiple_of(base + j * tile, tile), tile)
            keys = pl.ds(pl.multiple_of(base, tile), size)
            s = dot(qkv[mine, 0:hd], qkv[keys, hd:2 * hd], 1, 1) * score_scale
            row = lax.broadcasted_iota(jnp.int32, (tile, size), 0) + j * tile
            col = lax.broadcasted_iota(jnp.int32, (tile, size), 1)
            s = jnp.where(row >= col, s, -1e30)
            e = jnp.exp(s - jnp.max(s, axis=-1, keepdims=True))
            p = e / jnp.sum(e, axis=-1, keepdims=True)
            p_ref[:, 0:size] = p
            pb = p.astype(BF16)
            o_all[mine, :] = dot(pb, qkv[keys, 2 * hd:3 * hd]).astype(BF16)
            dv = dot(pb, do[mine, :], 0, 0)
            if j == per_mb - 1:
                dv_acc[...] = dv
            else:
                dv_acc[0:size, :] += dv

        def part_b(j):
            size = (j + 1) * tile
            mine = pl.ds(pl.multiple_of(base + j * tile, tile), tile)
            keys = pl.ds(pl.multiple_of(base, tile), size)
            p = p_ref[:, 0:size]
            dp = dot(do[mine, :], qkv[keys, 2 * hd:3 * hd], 1, 1)
            rd = jnp.sum(p * dp, axis=-1, keepdims=True)
            ds = (p * (dp - rd) * score_scale).astype(BF16)
            dqkv[mine, 0:hd] = dot(ds, qkv[keys, hd:2 * hd]).astype(BF16)
            dk = dot(ds, qkv[mine, 0:hd], 0, 0)
            if j == per_mb - 1:
                dk_acc[...] = dk
            else:
                dk_acc[0:size, :] += dk
            dqkv[mine, hd:2 * hd] = dk_acc[j * tile:size, :].astype(BF16)
            dqkv[mine, 2 * hd:3 * hd] = dv_acc[j * tile:size, :].astype(BF16)

        def part_c(j):
            mine = pl.ds(pl.multiple_of(base + j * tile, tile), tile)
            part = dot(dqkv[mine, :], wqkv[...]).astype(BF16)

            @pl.when(comm.core == j % 2)
            def _():
                own[b * (per_mb // 2) + j // 2] = part

            @pl.when(comm.core != j % 2)
            def _():
                full[mine, :] = part

        variants(part_a)
        ticks(first, 0)

        @pl.when(loading)
        def _():
            do[trow, :] = dot(dh_tile[...], wo[...], 1, 1).astype(BF16)

        variants(part_b)
        ticks(first, 1)
        variants(part_c)
        ticks(first, 2)

        @pl.when(i >= n_seq)
        def _():
            c0 = pl.multiple_of((i - n_seq) * cb, cb)
            z = (x_col[...].astype(F32) - comm.mu[:, 0:1]) * comm.rs[:, 0:1]
            n1c[...] = (z * comm.gain[:, pl.ds(c0, cb)]).astype(BF16)
        ticks(rest, 0)

        @pl.when(i >= n_seq)
        def _():
            dwqkv_ref[...] = dot(dqkv[...], n1c[...], 0, 0).astype(BF16)
        ticks(rest, 1)

        @pl.when(i >= n_seq)
        def _():
            dwo_ref[...] = dot(o_all[...], dh_col[...], 0, 0).astype(BF16)
        ticks(rest, 2)

        @pl.when(i == grid - 1)
        def _():
            comm.end()

    def tile_map(i):
        ii = jnp.minimum(i, n_seq - 1)
        return lax.div(ii, 2 * per_mb) * per_mb + jnp.minimum(lax.rem(ii, 2 * per_mb), per_mb - 1), 0

    def col_at(i):
        return jnp.maximum(i - n_seq, 0)

    whole = pl.BlockSpec(memory_space=VMEM)
    hbm = pl.BlockSpec(memory_space=ANY)
    return pl.pallas_call(
        kernel,
        grid=(grid,),
        out_shape=(jax.ShapeDtypeStruct((rows, cols), BF16), jax.ShapeDtypeStruct((qkv_w, cols), BF16),
                   jax.ShapeDtypeStruct((hd, cols), BF16)),
        in_specs=[pl.BlockSpec((tile, cols), tile_map), pl.BlockSpec((tile, cols), tile_map),
                  pl.BlockSpec((rows, cb), lambda i: (0, col_at(i))), pl.BlockSpec((rows, cb), lambda i: (0, col_at(i))),
                  hbm, hbm, whole, whole, whole, hbm, hbm],
        out_specs=(hbm, pl.BlockSpec((qkv_w, cb), lambda i: (0, col_at(i))),
                   pl.BlockSpec((hd, cb), lambda i: (0, col_at(i)))),
        scratch_shapes=[VMEM((rows, qkv_w), BF16), VMEM((rows, hd), BF16), VMEM((rows, hd), BF16),
                        VMEM((rows, qkv_w), BF16), VMEM((seq, hd), F32), VMEM((seq, hd), F32), VMEM((rows, cb), BF16),
                        VMEM((tile, seq), F32), VMEM((qkv_w, cols), BF16), VMEM((hd, cols), BF16),
                        pltpu.SemaphoreType.DMA((4,))] + comm.scratch(),
        compiler_params=pltpu.CompilerParams(collective_id=cid, has_side_effects=True, vmem_limit_bytes=VMEM_LIMIT,
                                             dimension_semantics=('arbitrary',)),
        name='attention_stage',
    )(x, dh1, x, dh1, w_qkv, w_out, mean, rstd, gain, x, dh1)


def spread_copy(dx, dw_up, dw_down, dw_qkv, dw_out, width):
    def rows_of(arr, parts):
        step = arr.shape[0] // parts
        return [(k * step, k * step, step) for k in range(parts)]

    hd = dw_out.shape[0]
    srcs = (dx, dw_up, dw_down, dw_qkv, dw_out)
    moves = (rows_of(dx, 8), rows_of(dw_up, 2), rows_of(dw_down, 2), [(c * hd, c * width, width) for c in range(3)],
             [(0, 0, width)])
    outs = [jax.ShapeDtypeStruct((sum(m[2] for m in mv), a.shape[1]), a.dtype) for a, mv in zip(srcs, moves)]
    total = sum(len(mv) for mv in moves)

    def kernel(*refs):
        ins, dsts, bufs, (in_sem, out_sem) = refs[:5], refs[5:10], refs[10:15], refs[15:]
        reads, writes = [], []
        for a, mv in enumerate(moves):
            for frm, to, size in mv:
                k = len(reads)
                here = bufs[a].at[pl.ds(to, size), :]
                reads.append(pltpu.make_async_copy(ins[a].at[pl.ds(frm, size), :], here, in_sem.at[k]))
                writes.append(pltpu.make_async_copy(here, dsts[a].at[pl.ds(to, size), :], out_sem.at[k]))
        for read in reads:
            read.start()
        for read, write in zip(reads, writes):
            read.wait()
            write.start()
        for write in writes:
            write.wait()

    hbm = pl.BlockSpec(memory_space=ANY)
    return pl.pallas_call(
        kernel,
        out_shape=outs,
        in_specs=[hbm] * 5,
        out_specs=[hbm] * 5,
        scratch_shapes=[VMEM(o.shape, o.dtype) for o in outs]
        + [pltpu.SemaphoreType.DMA((total,)), pltpu.SemaphoreType.DMA((total,))],
        compiler_params=pltpu.CompilerParams(vmem_limit_bytes=VMEM_LIMIT),
        name='spread_copy',
    )(*srcs)


def solution(mesh):
    act_spec = P('dp', None, None)
    stat_spec = P('dp', None)
    in_specs = (act_spec, act_spec, act_spec, stat_spec, stat_spec, stat_spec, stat_spec, P(), P(),
                P(None, 'tp', None, None), P('tp', None, None), P(None, 'tp'), P('tp', None))
    out_specs = (act_spec, P('dp', 'tp', None, None), P(('dp', 'tp'), None, None), P('dp', 'tp'),
                 P(('dp', 'tp'), None))
    n = mesh.shape['tp']

    def local_backward(x_saved, h1_saved, grad_y, mean_one, rstd_one, mean_two, rstd_two,
                       gain_one, gain_two, w_qkv, w_out, w_up, w_down):
        score_scale = w_qkv.shape[3] ** -0.5
        shape = x_saved.shape
        flat = (shape[0] * shape[1], shape[2])
        g1, g2 = gain_one, gain_two
        dh1, grad_up, grad_down = mlp_stage(n, h1_saved.reshape(flat), grad_y.reshape(flat), mean_two, rstd_two, g2,
                                            w_up, w_down, 0)
        heads, _, width = w_qkv.shape[1:]
        rows_qkv = w_qkv.transpose(1, 2, 3, 0).reshape(3 * width, flat[1])
        dx, dqkv_w, dout_w = attention_stage(n, shape[0], x_saved.reshape(flat), dh1, mean_one, rstd_one, g1,
                                             rows_qkv, w_out[0], score_scale, 1)
        dx, grad_up, grad_down, dqkv_w, dout_w = spread_copy(dx, grad_up, grad_down, dqkv_w, dout_w, width)
        grad_qkv_w = dqkv_w.reshape(heads, 3, width, flat[1]).transpose(3, 0, 1, 2)
        return dx.reshape(shape), grad_qkv_w, dout_w[None], grad_up, grad_down

    return jax.shard_map(local_backward, mesh=mesh, in_specs=in_specs, out_specs=out_specs, check_vma=False)
```

```python
import math
import jax
import jax.numpy as jnp
from jax import lax
from jax.experimental import pallas as pl
from jax.experimental.pallas import tpu as pltpu
from jax.sharding import PartitionSpec as P

GELU_C = 0.7978845608028654
GELU_A = 0.044715
F32 = jnp.float32
BF16 = jnp.bfloat16
ANY = pl.ANY
VMEM = pltpu.VMEM


def gelu_tanh(pre_act):
    inner_arg = GELU_C * (pre_act + GELU_A * pre_act * pre_act * pre_act)
    return 0.5 * pre_act * (1.0 + jnp.tanh(inner_arg))


def gelu_slope(pre_act):
    inner_arg = GELU_C * (pre_act + GELU_A * pre_act * pre_act * pre_act)
    tanh_val = jnp.tanh(inner_arg)
    return (0.5 * (1.0 + tanh_val)
            + 0.5 * pre_act * (1.0 - tanh_val * tanh_val) * GELU_C * (1.0 + 3.0 * GELU_A * pre_act * pre_act))


BLOCK = 512
SEMS = 32
LINK = {'+': 90e3, '-': 90e3, 'D': 450e3}
LATENCY = 2.6
TICK = 0.3


class Comm:
    def __init__(self, n, rows, cols):
        self.side = math.isqrt(n // 2)
        assert self.side == 4 and 2 * self.side * self.side == n
        self.rows, self.cols = rows, cols
        self.blk = BLOCK
        self.streams = rows // BLOCK
        self.half = self.blk // 2
        self.l1 = self.half // self.side
        self.l2 = self.l1 // self.side
        self.hw = cols // 2

    N_SCRATCH = 12

    def scratch(self):
        l1, l2, w, hw, ns = self.l1, self.l2, self.cols, self.hw, self.streams
        return [
            VMEM((ns, self.half, w), BF16),
            VMEM((ns, self.half, w), BF16),
            VMEM((ns, 6, l1, hw), BF16),
            VMEM((ns, 6, l2, hw), BF16),
            VMEM((self.rows, w), BF16),
            VMEM((ns, l2, w), BF16),
            VMEM((ns, l2, w), BF16),
            VMEM((self.rows, 128), F32),
            VMEM((1, w), F32),
            pltpu.SemaphoreType.DMA((ns, SEMS)),
            pltpu.SemaphoreType.DMA((ns, SEMS)),
            pltpu.SemaphoreType.DMA((ns, 8)),
            pltpu.SemaphoreType.REGULAR((ns,)),
        ]

    def bind(self, part, saved, resid, stats, gain, out, scratch):
        (self.own, self.pair, self.ring1, self.ring2, self.full, self.zrow, self.rrow, self.cols_of, self.gain,
         self.ssem, self.rsem, self.lsem, self.freed) = scratch
        self.part, self.saved, self.resid, self.gain_in, self.out = part, saved, resid, gain, out
        self.stats = stats
        side = self.side
        me = lax.axis_index('tp')
        core = lax.rem(me, 2)
        x = lax.rem(lax.div(me, 2), side)
        y = lax.div(me, 2 * side)
        self.core = core
        self.p1 = x * (1 - core) + y * core
        self.p2 = y * (1 - core) + x * core

        def dev(p1, p2):
            p1, p2 = lax.rem(p1 + side, side), lax.rem(p2 + side, side)
            xx = p1 * (1 - core) + p2 * core
            yy = p2 * (1 - core) + p1 * core
            return (yy * side + xx) * 2 + core

        self.partner = me + 1 - 2 * core
        self.ring_devs = {1: (dev(self.p1 + 1, self.p2), dev(self.p1 - 1, self.p2)),
                          2: (dev(self.p1, self.p2 + 1), dev(self.p1, self.p2 - 1))}
        self.sent = []

    def m(self, j):
        return lax.rem(j + self.side, self.side)

    def ds(self, off, size):
        return pl.ds(pl.multiple_of(off, 16), size)

    def half_rows(self, s, which):
        c = self.core if which == 0 else 1 - self.core
        return self.ds(s * self.blk + c * self.half, self.half)

    def copies(self, s):
        side, l1, l2, hw, w = self.side, self.l1, self.l2, self.hw, self.cols
        c, p1, p2, m, ds = self.core, self.p1, self.p2, self.m, self.ds
        left, right = pl.ds(0, hw), pl.ds(hw, hw)
        own, full = self.own.at[s], self.full
        row0 = s * self.blk
        out = {}
        source = self.full if self.part is None else self.part
        out['pair'] = (0, source.at[self.half_rows(s, 1), :], self.pair.at[s], self.partner)

        def ring(tag, first, base, size, p, bufs, devs):
            plus, minus = devs

            def chunk(j, cols):
                return own.at[ds(base + m(j) * size, size), cols]

            out[tag + 'xp'] = (first + 0, chunk(p + 2, left), bufs.at[s, 0], plus)
            out[tag + 'xm'] = (first + 1, chunk(p + 2, right), bufs.at[s, 1], minus)
            out[tag + 'dp'] = (first + 2, chunk(p + 1, right), bufs.at[s, 2], plus)
            out[tag + 'dm'] = (first + 3, chunk(p - 1, left), bufs.at[s, 3], minus)
            out[tag + 'rp'] = (first + 4, chunk(p + 1, left), bufs.at[s, 4], plus)
            out[tag + 'rm'] = (first + 5, chunk(p - 1, right), bufs.at[s, 5], minus)

        ring('a', 1, 0, l1, p1, self.ring1, self.ring_devs[1])
        ring('b', 7, p1 * l1, l2, p2, self.ring2, self.ring_devs[2])

        def gather(tag, first, base, size, p, devs):
            plus, minus = devs

            def chunk(j, cols):
                return full.at[ds(base + m(j) * size, size), cols]

            every = pl.ds(0, w)
            for name, idx, view, to in (('sp', 0, chunk(p, every), plus), ('sm', 1, chunk(p, every), minus),
                                        ('yp', 2, chunk(p - 1, left), plus), ('ym', 3, chunk(p + 1, right), minus)):
                out[tag + name] = (first + idx, view, view, to)

        half0 = row0 + c * self.half
        gather('c', 13, half0 + p1 * l1, l2, p2, self.ring_devs[2])
        gather('d', 17, half0, l1, p1, self.ring_devs[1])
        for j in range(side):
            view = full.at[ds(half0 + m(p1 + j) * l1, l1), :]
            out['k%d' % j] = (21 + j, view, view, self.partner)
        return out

    def get(self, s, name):
        idx, src, dst, to = self.copies(s)[name]
        return pltpu.make_async_remote_copy(src_ref=src, dst_ref=dst, send_sem=self.ssem.at[s, idx],
                                            recv_sem=self.rsem.at[s, idx], device_id={'tp': to},
                                            device_id_type=pl.DeviceIdType.MESH)

    def start(self, s, *names):
        for name in names:
            self.get(s, name).start()
            self.sent.append((s, name))

    def arrived(self, s, *names):
        for name in names:
            self.get(s, name).wait_recv()

    def mine(self, s):
        return self.ds(s * self.blk + self.core * self.half + self.p1 * self.l1 + self.p2 * self.l2, self.l2)

    def local(self, s, idx):
        if idx == 0:
            src, dst = self.part.at[self.half_rows(s, 0), :], self.own.at[s]
        elif idx == 1:
            src, dst = self.saved.at[self.mine(s), :], self.zrow.at[s]
        elif idx == 2:
            src, dst = self.resid.at[self.mine(s), :], self.rrow.at[s]
        else:
            rows = self.half_rows(s, idx - 4)
            src, dst = self.full.at[rows, :], self.out.at[rows, :]
        return pltpu.make_async_copy(src, dst, self.lsem.at[s, idx])

    def barrier(self):
        sem = pltpu.get_barrier_semaphore()
        peers = (self.partner,) + self.ring_devs[1] + self.ring_devs[2]
        for peer in peers:
            pl.semaphore_signal(sem, inc=1, device_id={'tp': peer}, device_id_type=pl.DeviceIdType.MESH)
        pl.semaphore_wait(sem, len(peers))

    def columns(self):
        self.gain[...] = self.gain_in[...].astype(F32)[None, :]
        per = self.stats[0].shape[1]
        lane = lax.broadcasted_iota(jnp.int32, (128, 128), 0)
        for i in range(self.rows // 128):
            b, off = divmod(i * 128, per)
            block = jnp.zeros((128, 128), F32)
            for k, src in enumerate(self.stats):
                block = jnp.where(lane == k, jnp.broadcast_to(src[b:b + 1, off:off + 128], (128, 128)), block)
            self.cols_of[pl.ds(i * 128, 128), :] = jnp.transpose(block)

    def normed(self, block, rows, k):
        return (block.astype(F32) - self.cols_of[rows, k:k + 1]) * self.cols_of[rows, k + 1:k + 2]

    def begin(self):
        for s in range(self.streams):
            if self.part is not None:
                self.local(s, 0).start()
            self.local(s, 1).start()
            self.local(s, 2).start()
        self.barrier()
        if self.part is not None:
            for s in range(self.streams):
                self.start(s, 'pair')
        self.columns()

    def rs1_start(self, s):
        if self.part is not None:
            self.local(s, 0).wait()
        self.arrived(s, 'pair')
        step = self.l1

        def add(i, carry):
            rows = pl.ds(pl.multiple_of(i * step, step), step)
            self.own[s, rows, :] = (self.own[s, rows, :].astype(F32) + self.pair[s, rows, :].astype(F32)).astype(BF16)
            return carry

        lax.fori_loop(0, self.half // step, add, 0)
        self.start(s, 'axp', 'axm', 'adp', 'adm')
        if self.part is None:
            self.get(s, 'pair').wait_send()
            pl.semaphore_signal(self.freed.at[s], inc=1, device_id={'tp': self.partner},
                                device_id_type=pl.DeviceIdType.MESH)

    def relay(self, s, tag, bufs, base, size, p):
        for buf, j, col0, got, nxt in ((0, p + 1, 0, 'xp', 'rp'), (1, p - 1, self.hw, 'xm', 'rm')):
            self.arrived(s, tag + got)
            rows = self.ds(base + self.m(j) * size, size)
            cols = pl.ds(col0, self.hw)
            self.own[s, rows, cols] = (self.own[s, rows, cols].astype(F32) + bufs[s, buf].astype(F32)).astype(BF16)
            self.start(s, tag + nxt)

    def final(self, s, tag, bufs, base, size, p):
        self.arrived(s, tag + 'rp', tag + 'dm', tag + 'rm', tag + 'dp')
        rows = self.ds(base + p * size, size)
        sums = []
        for col0, one, two in ((0, 4, 3), (self.hw, 5, 2)):
            sums.append(self.own[s, rows, pl.ds(col0, self.hw)].astype(F32)
                        + bufs[s, one].astype(F32) + bufs[s, two].astype(F32))
        return rows, sums

    def rs1_relay(self, s):
        self.relay(s, 'a', self.ring1, 0, self.l1, self.p1)

    def rs2_start(self, s):
        rows, sums = self.final(s, 'a', self.ring1, 0, self.l1, self.p1)
        for k in range(2):
            self.own[s, rows, pl.ds(k * self.hw, self.hw)] = sums[k].astype(BF16)
        self.start(s, 'bxp', 'bxm', 'bdp', 'bdm')

    def rs2_relay(self, s):
        self.relay(s, 'b', self.ring2, self.p1 * self.l1, self.l2, self.p2)

    def norm_gather(self, s):
        _, sums = self.final(s, 'b', self.ring2, self.p1 * self.l1, self.l2, self.p2)
        self.local(s, 1).wait()
        self.local(s, 2).wait()
        mine = self.mine(s)
        mu = self.cols_of[mine, 0:1]
        r = self.cols_of[mine, 1:2]
        us, xs = [], []
        for k in range(2):
            cols = pl.ds(k * self.hw, self.hw)
            us.append(sums[k] * self.gain[:, cols])
            xs.append((self.zrow[s, :, cols].astype(F32) - mu) * r)
        inv = 1.0 / self.cols
        mean_u = (jnp.sum(us[0], axis=-1, keepdims=True) + jnp.sum(us[1], axis=-1, keepdims=True)) * inv
        mean_c = (jnp.sum(us[0] * xs[0], axis=-1, keepdims=True)
                  + jnp.sum(us[1] * xs[1], axis=-1, keepdims=True)) * inv
        for k in range(2):
            cols = pl.ds(k * self.hw, self.hw)
            grad = self.rrow[s, :, cols].astype(F32) + r * (us[k] - mean_u - xs[k] * mean_c)
            self.full[mine, cols] = grad.astype(BF16)
        self.start(s, 'csp', 'csm')

    def ag2_relay(self, s):
        self.arrived(s, 'csp')
        self.start(s, 'cyp')
        self.arrived(s, 'csm')
        self.start(s, 'cym')

    def ag1_start(self, s):
        self.arrived(s, 'cyp', 'cym')
        if self.part is None:
            pl.semaphore_wait(self.freed.at[s], 1)
        self.start(s, 'dsp', 'dsm', 'k0')

    def ag1_relay(self, s):
        self.arrived(s, 'dsp')
        self.start(s, 'dyp')
        self.arrived(s, 'dsm')
        self.start(s, 'dym', 'k3', 'k1')

    def ag1_final(self, s):
        self.arrived(s, 'dyp', 'dym')
        self.start(s, 'k2')
        self.local(s, 4).start()

    def finish(self, s):
        self.arrived(s, 'k0', 'k1', 'k2', 'k3')
        self.local(s, 5).start()

    def end(self):
        for s, name in self.sent:
            if name != 'pair' or self.part is not None:
                self.get(s, name).wait_send()
        for s in range(self.streams):
            self.local(s, 4).wait()
            self.local(s, 5).wait()

    def stages(self):
        x1, x2 = self.l1 * self.hw * 2, self.l2 * self.hw * 2
        return [
            ('rs1_start', ['pair', 'own'], [('axp', '+', x1), ('axm', '-', x1), ('adp', '+', x1), ('adm', '-', x1)]),
            ('rs1_relay', ['axp', 'axm'], [('arp', '+', x1), ('arm', '-', x1)]),
            ('rs2_start', ['arp', 'arm', 'adp', 'adm'],
             [('bxp', '+', x2), ('bxm', '-', x2), ('bdp', '+', x2), ('bdm', '-', x2)]),
            ('rs2_relay', ['bxp', 'bxm'], [('brp', '+', x2), ('brm', '-', x2)]),
            ('norm_gather', ['brp', 'brm', 'bdp', 'bdm'], [('csp', '+', 2 * x2), ('csm', '-', 2 * x2)]),
            ('ag2_relay', ['csp', 'csm'], [('cyp', '+', x2), ('cym', '-', x2)]),
            ('ag1_start', ['cyp', 'cym'], [('dsp', '+', 2 * x1), ('dsm', '-', 2 * x1), ('k0', 'D', 2 * x1)]),
            ('ag1_relay', ['dsp', 'dsm'], [('dyp', '+', x1), ('dym', '-', x1), ('k3', 'D', 2 * x1), ('k1', 'D', 2 * x1)]),
            ('ag1_final', ['dyp', 'dym'], [('k2', 'D', 2 * x1)]),
            ('finish', ['k0', 'k1', 'k2', 'k3'], []),
        ]

    def plan(self, points):
        stages = self.stages()
        pair_bytes = self.half * self.cols * 2
        free = dict.fromkeys(LINK, 0.0)
        done = {}
        at = [0] * self.streams
        now = 0.0

        def push(s, name, link, size):
            free[link] = max(free[link], now) + size / LINK[link]
            done[s, name] = free[link] + LATENCY

        def ready(s):
            if at[s] >= len(stages):
                return math.inf
            return max(done.get((s, need), math.inf) for need in stages[at[s]][1])

        plans = []
        for i, (cost, gives) in enumerate(points):
            now += cost
            todo = []
            for s, what in gives:
                if what == 'pair':
                    push(s, 'pair', 'D', pair_bytes)
                    if self.part_given is False:
                        todo.append(('send_pair', s))
                else:
                    done[s, 'own'] = now
            last = i == len(points) - 1
            while True:
                s = min(range(self.streams), key=ready)
                t = ready(s)
                if t == math.inf or (t > now and not last):
                    break
                now = max(now, t) + TICK
                name, _, sends = stages[at[s]]
                for copy, link, size in sends:
                    push(s, copy, link, size)
                at[s] += 1
                todo.append((name, s))
            plans.append(todo)
        assert all(a == len(stages) for a in at)
        self.estimate = now
        return plans

    def tuned(self, table, points):
        self.points = points
        plans = self.plan(points)
        if not table or len(plans) != table[0]:
            return plans
        names = [stage[0] for stage in self.stages()]
        out = [[step for step in todo if step[0] == 'send_pair'] for todo in plans]
        for code in table[1]:
            point, rest = divmod(code, 64)
            out[point].append((names[rest // 4], rest % 4))
        return out

    def send_pair(self, s):
        self.start(s, 'pair')

    part_given = False


MLP_PLAN = (84, [
    448, 769, 965, 964, 1161, 1154, 1352, 1357, 1414, 1539, 1863, 1868, 1873, 1866, 2187, 2261, 2318, 2383,
    2384, 2457, 2706, 2899, 2900, 2909, 3030, 3096, 3351, 3418, 3740, 3931, 4190, 4256, 4639, 4834, 4833,
    5155, 5220, 5349, 5350, 5351])
ATT_PLAN = (84, [
    1409, 1989, 2441, 2432, 2701, 2692, 2833, 2883, 3016, 3015, 3020, 3074, 3280, 3398, 3541, 3668, 3659,
    3722, 3737, 3918, 3919, 4056, 4306, 4307, 4316, 4374, 4445, 4439, 4634, 4827, 4832, 4897, 4894, 5092,
    5151, 5282, 5349, 5347, 5350, 5351])
VMEM_LIMIT = 64 * 1024 * 1024 - 64 * 1024


def dot(a, b, ca=1, cb=0):
    return lax.dot_general(a, b, (((ca,), (cb,)), ((), ())), preferred_element_type=F32)


def mlp_stage(n, h1, dy, x, stats, gain, gain_x, w_up, w_down, w_qkv, width, cid):
    rows, cols = h1.shape
    ffn = w_up.shape[1]
    comm = Comm(n, rows, cols)
    tile = comm.half
    n_tiles = rows // tile
    cb = 256
    n_cols = cols // cb
    hd = width + -width % 128
    qkv_w = 3 * hd
    dw_end = n_tiles + n_cols
    grid = dw_end + n_tiles
    points = []
    for i in range(n_tiles):
        points += [(1.5 if i else 7.0, []), (0.9, []), (2.0, [(i // 2, 'pair' if i % 2 == 0 else 'own')])]
    for i in range(n_cols):
        points += [(0.6, []), (1.0, []), (0.85, [])]
    points += [(1.6, []), (0.0, []), (0.0, [])] * n_tiles
    plans = comm.tuned(MLP_PLAN, points)

    def kernel(h1_tile, dy_tile, h1_col, dy_col, x_tile, w1, w2, mean2, rstd2, mean1, rstd1, gain_ref, gain_x_ref,
               wqkv_in, h1_all, dy_all, dh1_ref, dw1_ref, dw2_ref, qkv_ref, act, da, wqkv, gx, wsem, *scratch):
        comm.bind(None, h1_all, dy_all, (mean2, rstd2, mean1, rstd1), gain_ref, dh1_ref, scratch)
        i = pl.program_id(0)
        full, own = comm.full, comm.own

        def ticks(steps, k):
            for step in steps:
                todo = plans[step * 3 + k]
                if todo:
                    @pl.when(i == step)
                    def _():
                        for name, s in todo:
                            getattr(comm, name)(s)

        loads = [pltpu.make_async_copy(wqkv_in.at[pl.ds(c * width, width), :], wqkv.at[pl.ds(c * hd, width), :],
                                       wsem.at[c]) for c in range(3)]

        @pl.when(i == 0)
        def _():
            for load in loads:
                load.start()
            for c in range(3):
                wqkv[pl.ds(c * hd + width, hd - width), :] = jnp.zeros((hd - width, cols), BF16)
            gx[...] = gain_x_ref[...].astype(F32)[None, :]
            comm.begin()

        first = range(n_tiles)
        rest = range(n_tiles, dw_end)
        last = range(dw_end, grid)
        tidx = lax.div(i, 2) * 2 + lax.rem(i, 2) * comm.core + (1 - lax.rem(i, 2)) * (1 - comm.core)
        trow = pl.ds(pl.multiple_of(tidx * tile, tile), tile)
        pre_ref, dg_ref = comm.pre, comm.dg

        @pl.when(i < n_tiles)
        def _():
            n2 = (comm.normed(h1_tile[...], trow, 0) * comm.gain[...]).astype(BF16)
            pre_ref[...] = dot(n2, w1[...])
        ticks(first, 0)

        @pl.when(i < n_tiles)
        def _():
            dg_ref[...] = dot(dy_tile[...], w2[...], 1, 1)
        ticks(first, 1)

        @pl.when(i < n_tiles)
        def _():
            pre = pre_ref[...]
            act[trow, :] = gelu_tanh(pre).astype(BF16)
            grad_pre = (dg_ref[...] * gelu_slope(pre)).astype(BF16)
            da[trow, :] = grad_pre
            part = dot(grad_pre, w1[...], 1, 1).astype(BF16)

            @pl.when(lax.rem(i, 2) == 0)
            def _():
                full[trow, :] = part

            @pl.when(lax.rem(i, 2) == 1)
            def _():
                own[lax.div(i, 2)] = part
        ticks(first, 2)

        @pl.when(jnp.logical_and(i >= n_tiles, i < dw_end))
        def _():
            c0 = pl.multiple_of((i - n_tiles) * cb, cb)
            comm.n2c[...] = (comm.normed(h1_col[...], pl.ds(0, rows), 0) * comm.gain[:, pl.ds(c0, cb)]).astype(BF16)
        ticks(rest, 0)

        @pl.when(jnp.logical_and(i >= n_tiles, i < dw_end))
        def _():
            dw1_ref[...] = dot(comm.n2c[...], da[...], 0, 0).astype(BF16)
        ticks(rest, 1)

        @pl.when(jnp.logical_and(i >= n_tiles, i < dw_end))
        def _():
            dw2_ref[...] = dot(act[...], dy_col[...], 0, 0).astype(BF16)
        ticks(rest, 2)

        @pl.when(i == dw_end)
        def _():
            for load in loads:
                load.wait()

        @pl.when(i >= dw_end)
        def _():
            xrow = pl.ds(pl.multiple_of((i - dw_end) * tile, tile), tile)
            n1 = (comm.normed(x_tile[...], xrow, 2) * gx[...]).astype(BF16)
            qkv_ref[...] = dot(n1, wqkv[...], 1, 1).astype(BF16)
        ticks(last, 0)
        ticks(last, 1)
        ticks(last, 2)

        @pl.when(i == grid - 1)
        def _():
            comm.end()

    def wrapped(*refs):
        *most, pre, dg, n2c = refs
        comm.pre, comm.dg, comm.n2c = pre, dg, n2c
        kernel(*most)

    def tile_map(i):
        core = lax.rem(lax.axis_index('tp'), 2)
        ii = jnp.minimum(i, n_tiles - 1)
        odd = lax.rem(ii, 2)
        return lax.div(ii, 2) * 2 + odd * core + (1 - odd) * (1 - core), 0

    def col_at(i):
        return jnp.clip(i - n_tiles, 0, n_cols - 1)

    def x_at(i):
        return jnp.maximum(i - dw_end, 0), 0

    whole = pl.BlockSpec(memory_space=VMEM)
    hbm = pl.BlockSpec(memory_space=ANY)
    return pl.pallas_call(
        wrapped,
        grid=(grid,),
        out_shape=(jax.ShapeDtypeStruct((rows, cols), BF16), jax.ShapeDtypeStruct((cols, ffn), BF16),
                   jax.ShapeDtypeStruct((ffn, cols), BF16), jax.ShapeDtypeStruct((rows, qkv_w), BF16)),
        in_specs=[pl.BlockSpec((tile, cols), tile_map), pl.BlockSpec((tile, cols), tile_map),
                  pl.BlockSpec((rows, cb), lambda i: (0, col_at(i))), pl.BlockSpec((rows, cb), lambda i: (0, col_at(i))),
                  pl.BlockSpec((tile, cols), x_at), whole, whole] + [whole] * 6 + [hbm] * 3,
        out_specs=(hbm, pl.BlockSpec((cb, ffn), lambda i: (col_at(i), 0)),
                   pl.BlockSpec((ffn, cb), lambda i: (0, col_at(i))), pl.BlockSpec((tile, qkv_w), x_at)),
        scratch_shapes=[VMEM((rows, ffn), BF16), VMEM((rows, ffn), BF16), VMEM((qkv_w, cols), BF16), VMEM((1, cols), F32),
                        pltpu.SemaphoreType.DMA((3,))] + comm.scratch()
        + [VMEM((tile, ffn), F32), VMEM((tile, ffn), F32), VMEM((rows, cb), BF16)],
        compiler_params=pltpu.CompilerParams(collective_id=cid, has_side_effects=True, vmem_limit_bytes=VMEM_LIMIT,
                                             dimension_semantics=('arbitrary',)),
        name='mlp_stage',
    )(h1, dy, h1, dy, x, w_up, w_down, *stats, gain, gain_x, w_qkv, h1, dy)


def attention_stage(n, mbs, x, dh1, qkv_all, stats, gain, w_qkv, w_out, score_scale, cid):
    rows, cols = x.shape
    seq = rows // mbs
    width = w_out.shape[0]
    hd = width + -width % 128
    qkv_w = 3 * hd
    comm = Comm(n, rows, cols)
    tile = comm.half
    per_mb = seq // tile
    n_seq = 2 * per_mb * mbs
    cb = 256
    n_cols = cols // cb
    grid = n_seq + n_cols
    points = []
    for b in range(mbs):
        points += [(0.0, []), (0.8, []), (0.0, [])] * per_mb
        for j in range(per_mb - 1, -1, -1):
            s = b * (per_mb // 2) + j // 2
            points += [(1.0, []), (0.9, []), (1.45, [(s, 'pair'), (s, 'own')] if j % 2 == 0 else [])]
    for i in range(n_cols):
        points += [(0.7, []), (1.0, []), (0.4, [])]
    points[0] = (5.5, [])
    plans = comm.tuned(ATT_PLAN, points)

    def kernel(dh_tile, x_col, dh_col, qkv, wqkv_in, wo_in, mean_ref, rstd_ref, gain_ref, x_all, dh_all,
               dx_ref, dwqkv_ref, dwo_ref, do, o_all, dqkv, dk_acc, dv_acc, n1c, p_ref, wqkv, wo, wsem, *scratch):
        comm.bind(None, x_all, dh_all, (mean_ref, rstd_ref), gain_ref, dx_ref, scratch)
        i = pl.program_id(0)
        full, own = comm.full, comm.own

        def ticks(steps, k):
            for step in steps:
                todo = plans[step * 3 + k]
                if todo:
                    @pl.when(i == step)
                    def _():
                        for name, s in todo:
                            getattr(comm, name)(s)

        @pl.when(i == 0)
        def _():
            loads = [pltpu.make_async_copy(wqkv_in.at[pl.ds(c * width, width), :], wqkv.at[pl.ds(c * hd, width), :],
                                           wsem.at[c]) for c in range(3)]
            loads.append(pltpu.make_async_copy(wo_in, wo.at[pl.ds(0, width), :], wsem.at[3]))
            for load in loads:
                load.start()
            zero = jnp.zeros((hd - width, cols), BF16)
            for c in range(3):
                wqkv[pl.ds(c * hd + width, hd - width), :] = zero
            wo[pl.ds(width, hd - width), :] = zero
            comm.begin()
            for load in loads:
                load.wait()

        span = 2 * per_mb
        first = range(n_seq)
        rest = range(n_seq, grid)
        b = lax.div(i, span)
        at = lax.rem(i, span)
        in_seq = i < n_seq
        loading = jnp.logical_and(in_seq, at < per_mb)
        base = b * seq
        trow = pl.ds(pl.multiple_of(jnp.minimum(base + at * tile, rows - tile), tile), tile)

        def variants(fn):
            for j in range(per_mb):
                @pl.when(jnp.logical_and(in_seq, at == 2 * per_mb - 1 - j))
                def _():
                    fn(j)

        def part_a(j):
            size = (j + 1) * tile
            mine = pl.ds(pl.multiple_of(base + j * tile, tile), tile)
            keys = pl.ds(pl.multiple_of(base, tile), size)
            s = dot(qkv[mine, 0:hd], qkv[keys, hd:2 * hd], 1, 1) * score_scale
            row = lax.broadcasted_iota(jnp.int32, (tile, size), 0) + j * tile
            col = lax.broadcasted_iota(jnp.int32, (tile, size), 1)
            s = jnp.where(row >= col, s, -1e30)
            e = jnp.exp(s - jnp.max(s, axis=-1, keepdims=True))
            p = e / jnp.sum(e, axis=-1, keepdims=True)
            p_ref[:, 0:size] = p
            pb = p.astype(BF16)
            o_all[mine, :] = dot(pb, qkv[keys, 2 * hd:3 * hd]).astype(BF16)
            dv = dot(pb, do[mine, :], 0, 0)
            if j == per_mb - 1:
                dv_acc[...] = dv
            else:
                dv_acc[0:size, :] += dv

        def part_b(j):
            size = (j + 1) * tile
            mine = pl.ds(pl.multiple_of(base + j * tile, tile), tile)
            keys = pl.ds(pl.multiple_of(base, tile), size)
            p = p_ref[:, 0:size]
            dp = dot(do[mine, :], qkv[keys, 2 * hd:3 * hd], 1, 1)
            rd = jnp.sum(p * dp, axis=-1, keepdims=True)
            ds = (p * (dp - rd) * score_scale).astype(BF16)
            dqkv[mine, 0:hd] = dot(ds, qkv[keys, hd:2 * hd]).astype(BF16)
            dk = dot(ds, qkv[mine, 0:hd], 0, 0)
            if j == per_mb - 1:
                dk_acc[...] = dk
            else:
                dk_acc[0:size, :] += dk
            dqkv[mine, hd:2 * hd] = dk_acc[j * tile:size, :].astype(BF16)
            dqkv[mine, 2 * hd:3 * hd] = dv_acc[j * tile:size, :].astype(BF16)

        def part_c(j):
            mine = pl.ds(pl.multiple_of(base + j * tile, tile), tile)
            part = dot(dqkv[mine, :], wqkv[...]).astype(BF16)

            @pl.when(comm.core == j % 2)
            def _():
                own[b * (per_mb // 2) + j // 2] = part

            @pl.when(comm.core != j % 2)
            def _():
                full[mine, :] = part

        variants(part_a)
        ticks(first, 0)

        @pl.when(loading)
        def _():
            do[trow, :] = dot(dh_tile[...], wo[...], 1, 1).astype(BF16)

        variants(part_b)
        ticks(first, 1)
        variants(part_c)
        ticks(first, 2)

        @pl.when(i >= n_seq)
        def _():
            c0 = pl.multiple_of((i - n_seq) * cb, cb)
            n1c[...] = (comm.normed(x_col[...], pl.ds(0, rows), 0) * comm.gain[:, pl.ds(c0, cb)]).astype(BF16)
        ticks(rest, 0)

        @pl.when(i >= n_seq)
        def _():
            dwqkv_ref[...] = dot(dqkv[...], n1c[...], 0, 0).astype(BF16)
        ticks(rest, 1)

        @pl.when(i >= n_seq)
        def _():
            dwo_ref[...] = dot(o_all[...], dh_col[...], 0, 0).astype(BF16)
        ticks(rest, 2)

        @pl.when(i == grid - 1)
        def _():
            comm.end()

    def tile_map(i):
        ii = jnp.minimum(i, n_seq - 1)
        return lax.div(ii, 2 * per_mb) * per_mb + jnp.minimum(lax.rem(ii, 2 * per_mb), per_mb - 1), 0

    def col_at(i):
        return jnp.maximum(i - n_seq, 0)

    whole = pl.BlockSpec(memory_space=VMEM)
    hbm = pl.BlockSpec(memory_space=ANY)
    return pl.pallas_call(
        kernel,
        grid=(grid,),
        out_shape=(jax.ShapeDtypeStruct((rows, cols), BF16), jax.ShapeDtypeStruct((qkv_w, cols), BF16),
                   jax.ShapeDtypeStruct((hd, cols), BF16)),
        in_specs=[pl.BlockSpec((tile, cols), tile_map),
                  pl.BlockSpec((rows, cb), lambda i: (0, col_at(i))), pl.BlockSpec((rows, cb), lambda i: (0, col_at(i))),
                  whole, hbm, hbm, whole, whole, whole, hbm, hbm],
        out_specs=(hbm, pl.BlockSpec((qkv_w, cb), lambda i: (0, col_at(i))),
                   pl.BlockSpec((hd, cb), lambda i: (0, col_at(i)))),
        scratch_shapes=[VMEM((rows, hd), BF16), VMEM((rows, hd), BF16),
                        VMEM((rows, qkv_w), BF16), VMEM((seq, hd), F32), VMEM((seq, hd), F32), VMEM((rows, cb), BF16),
                        VMEM((tile, seq), F32), VMEM((qkv_w, cols), BF16), VMEM((hd, cols), BF16),
                        pltpu.SemaphoreType.DMA((4,))] + comm.scratch(),
        compiler_params=pltpu.CompilerParams(collective_id=cid, has_side_effects=True, vmem_limit_bytes=VMEM_LIMIT,
                                             dimension_semantics=('arbitrary',)),
        name='attention_stage',
    )(dh1, x, dh1, qkv_all, w_qkv, w_out, *stats, gain, x, dh1)


def spread_copy(dx, dw_up, dw_down, dw_qkv, dw_out, width):
    def rows_of(arr, parts):
        step = arr.shape[0] // parts
        return [(k * step, k * step, step) for k in range(parts)]

    hd = dw_out.shape[0]
    srcs = (dx, dw_up, dw_down, dw_qkv, dw_out)
    moves = (rows_of(dx, 8), rows_of(dw_up, 2), rows_of(dw_down, 2), [(c * hd, c * width, width) for c in range(3)],
             [(0, 0, width)])
    outs = [jax.ShapeDtypeStruct((sum(m[2] for m in mv), a.shape[1]), a.dtype) for a, mv in zip(srcs, moves)]
    total = sum(len(mv) for mv in moves)

    def kernel(*refs):
        ins, dsts, bufs, (in_sem, out_sem) = refs[:5], refs[5:10], refs[10:15], refs[15:]
        reads, writes = [], []
        for a, mv in enumerate(moves):
            for frm, to, size in mv:
                k = len(reads)
                here = bufs[a].at[pl.ds(to, size), :]
                reads.append(pltpu.make_async_copy(ins[a].at[pl.ds(frm, size), :], here, in_sem.at[k]))
                writes.append(pltpu.make_async_copy(here, dsts[a].at[pl.ds(to, size), :], out_sem.at[k]))
        for read in reads:
            read.start()
        for read, write in zip(reads, writes):
            read.wait()
            write.start()
        for write in writes:
            write.wait()

    hbm = pl.BlockSpec(memory_space=ANY)
    return pl.pallas_call(
        kernel,
        out_shape=outs,
        in_specs=[hbm] * 5,
        out_specs=[hbm] * 5,
        scratch_shapes=[VMEM(o.shape, o.dtype) for o in outs]
        + [pltpu.SemaphoreType.DMA((total,)), pltpu.SemaphoreType.DMA((total,))],
        compiler_params=pltpu.CompilerParams(vmem_limit_bytes=VMEM_LIMIT),
        name='spread_copy',
    )(*srcs)


def solution(mesh):
    act_spec = P('dp', None, None)
    stat_spec = P('dp', None)
    in_specs = (act_spec, act_spec, act_spec, stat_spec, stat_spec, stat_spec, stat_spec, P(), P(),
                P(None, 'tp', None, None), P('tp', None, None), P(None, 'tp'), P('tp', None))
    out_specs = (act_spec, P('dp', 'tp', None, None), P(('dp', 'tp'), None, None), P('dp', 'tp'),
                 P(('dp', 'tp'), None))
    n = mesh.shape['tp']

    def local_backward(x_saved, h1_saved, grad_y, mean_one, rstd_one, mean_two, rstd_two,
                       gain_one, gain_two, w_qkv, w_out, w_up, w_down):
        score_scale = w_qkv.shape[3] ** -0.5
        shape = x_saved.shape
        flat = (shape[0] * shape[1], shape[2])
        heads, _, width = w_qkv.shape[1:]
        rows_qkv = w_qkv.transpose(1, 2, 3, 0).reshape(3 * width, flat[1])
        h1, dy, x = h1_saved.reshape(flat), grad_y.reshape(flat), x_saved.reshape(flat)
        dh1, grad_up, grad_down, qkv = mlp_stage(n, h1, dy, x, (mean_two, rstd_two, mean_one, rstd_one), gain_two,
                                                 gain_one, w_up, w_down, rows_qkv, width, 0)
        dx, dqkv_w, dout_w = attention_stage(n, shape[0], x, dh1, qkv, (mean_one, rstd_one), gain_one, rows_qkv,
                                             w_out[0], score_scale, 1)
        dx, grad_up, grad_down, dqkv_w, dout_w = spread_copy(dx, grad_up, grad_down, dqkv_w, dout_w, width)
        grad_qkv_w = dqkv_w.reshape(heads, 3, width, flat[1]).transpose(3, 0, 1, 2)
        return dx.reshape(shape), grad_qkv_w, dout_w[None], grad_up, grad_down

    return jax.shard_map(local_backward, mesh=mesh, in_specs=in_specs, out_specs=out_specs, check_vma=False)
```

```python
import math
import jax
import jax.numpy as jnp
from jax import lax
from jax.experimental import pallas as pl
from jax.experimental.pallas import tpu as pltpu
from jax.sharding import PartitionSpec as P

GELU_C = 0.7978845608028654
GELU_A = 0.044715
F32 = jnp.float32
BF16 = jnp.bfloat16
ANY = pl.ANY
VMEM = pltpu.VMEM


def gelu_tanh(pre_act):
    inner_arg = GELU_C * (pre_act + GELU_A * pre_act * pre_act * pre_act)
    return 0.5 * pre_act * (1.0 + jnp.tanh(inner_arg))


def gelu_slope(pre_act):
    inner_arg = GELU_C * (pre_act + GELU_A * pre_act * pre_act * pre_act)
    tanh_val = jnp.tanh(inner_arg)
    return (0.5 * (1.0 + tanh_val)
            + 0.5 * pre_act * (1.0 - tanh_val * tanh_val) * GELU_C * (1.0 + 3.0 * GELU_A * pre_act * pre_act))


BLOCK = 512
SEMS = 32
LINK = {'+': 90e3, '-': 90e3, 'D': 450e3}
LATENCY = 2.6
TICK = 0.3


class Comm:
    def __init__(self, n, rows, cols):
        self.side = math.isqrt(n // 2)
        assert self.side == 4 and 2 * self.side * self.side == n
        self.rows, self.cols = rows, cols
        self.blk = BLOCK
        self.streams = rows // BLOCK
        self.half = self.blk // 2
        self.l1 = self.half // self.side
        self.l2 = self.l1 // self.side
        self.hw = cols // 2

    N_SCRATCH = 12

    def scratch(self):
        l1, l2, w, hw, ns = self.l1, self.l2, self.cols, self.hw, self.streams
        return [
            VMEM((ns, self.half, w), BF16),
            VMEM((ns, 6, l1, hw), BF16),
            VMEM((ns, 6, l2, hw), BF16),
            VMEM((self.rows, w), BF16),
            VMEM((ns, l2, w), BF16),
            VMEM((ns, l2, w), BF16),
            VMEM((self.rows, 128), F32),
            VMEM((1, w), F32),
            pltpu.SemaphoreType.DMA((ns, SEMS)),
            pltpu.SemaphoreType.DMA((ns, SEMS)),
            pltpu.SemaphoreType.DMA((ns, 8)),
            pltpu.SemaphoreType.REGULAR((ns,)),
        ]

    def bind(self, part, saved, resid, stats, gain, out, scratch):
        (self.own, self.ring1, self.ring2, self.full, self.zrow, self.rrow, self.cols_of, self.gain,
         self.ssem, self.rsem, self.lsem, self.freed) = scratch
        self.part, self.saved, self.resid, self.gain_in, self.out = part, saved, resid, gain, out
        self.stats = stats
        side = self.side
        me = lax.axis_index('tp')
        core = lax.rem(me, 2)
        x = lax.rem(lax.div(me, 2), side)
        y = lax.div(me, 2 * side)
        self.core = core
        self.p1 = x * (1 - core) + y * core
        self.p2 = y * (1 - core) + x * core

        def dev(p1, p2):
            p1, p2 = lax.rem(p1 + side, side), lax.rem(p2 + side, side)
            xx = p1 * (1 - core) + p2 * core
            yy = p2 * (1 - core) + p1 * core
            return (yy * side + xx) * 2 + core

        self.partner = me + 1 - 2 * core
        self.ring_devs = {1: (dev(self.p1 + 1, self.p2), dev(self.p1 - 1, self.p2)),
                          2: (dev(self.p1, self.p2 + 1), dev(self.p1, self.p2 - 1))}
        self.sent = []

    def m(self, j):
        return lax.rem(j + self.side, self.side)

    def ds(self, off, size):
        return pl.ds(pl.multiple_of(off, 16), size)

    def half_rows(self, s, which):
        c = self.core if which == 0 else 1 - self.core
        return self.ds(s * self.blk + c * self.half, self.half)

    def copies(self, s):
        side, l1, l2, hw, w = self.side, self.l1, self.l2, self.hw, self.cols
        c, p1, p2, m, ds = self.core, self.p1, self.p2, self.m, self.ds
        left, right = pl.ds(0, hw), pl.ds(hw, hw)
        own, full = self.own.at[s], self.full
        row0 = s * self.blk
        out = {}
        theirs = full.at[self.half_rows(s, 1), :]
        out['pair'] = (0, theirs, theirs, self.partner)

        def ring(tag, first, base, size, p, bufs, devs):
            plus, minus = devs

            def chunk(j, cols):
                return own.at[ds(base + m(j) * size, size), cols]

            out[tag + 'xp'] = (first + 0, chunk(p + 2, left), bufs.at[s, 0], plus)
            out[tag + 'xm'] = (first + 1, chunk(p + 2, right), bufs.at[s, 1], minus)
            out[tag + 'dp'] = (first + 2, chunk(p + 1, right), bufs.at[s, 2], plus)
            out[tag + 'dm'] = (first + 3, chunk(p - 1, left), bufs.at[s, 3], minus)
            out[tag + 'rp'] = (first + 4, chunk(p + 1, left), bufs.at[s, 4], plus)
            out[tag + 'rm'] = (first + 5, chunk(p - 1, right), bufs.at[s, 5], minus)

        ring('a', 1, 0, l1, p1, self.ring1, self.ring_devs[1])
        ring('b', 7, p1 * l1, l2, p2, self.ring2, self.ring_devs[2])

        def gather(tag, first, base, size, p, devs):
            plus, minus = devs

            def chunk(j, cols):
                return full.at[ds(base + m(j) * size, size), cols]

            every = pl.ds(0, w)
            for name, idx, view, to in (('sp', 0, chunk(p, every), plus), ('sm', 1, chunk(p, every), minus),
                                        ('yp', 2, chunk(p - 1, left), plus), ('ym', 3, chunk(p + 1, right), minus)):
                out[tag + name] = (first + idx, view, view, to)

        half0 = row0 + c * self.half
        gather('c', 13, half0 + p1 * l1, l2, p2, self.ring_devs[2])
        gather('d', 17, half0, l1, p1, self.ring_devs[1])
        for j in range(side):
            view = full.at[ds(half0 + m(p1 + j) * l1, l1), :]
            out['k%d' % j] = (21 + j, view, view, self.partner)
        return out

    def get(self, s, name):
        idx, src, dst, to = self.copies(s)[name]
        return pltpu.make_async_remote_copy(src_ref=src, dst_ref=dst, send_sem=self.ssem.at[s, idx],
                                            recv_sem=self.rsem.at[s, idx], device_id={'tp': to},
                                            device_id_type=pl.DeviceIdType.MESH)

    def start(self, s, *names):
        for name in names:
            self.get(s, name).start()
            self.sent.append((s, name))

    def arrived(self, s, *names):
        for name in names:
            self.get(s, name).wait_recv()

    def mine(self, s):
        return self.ds(s * self.blk + self.core * self.half + self.p1 * self.l1 + self.p2 * self.l2, self.l2)

    def local(self, s, idx):
        if idx == 0:
            src, dst = self.part.at[self.half_rows(s, 0), :], self.own.at[s]
        elif idx == 1:
            src, dst = self.saved.at[self.mine(s), :], self.zrow.at[s]
        elif idx == 2:
            src, dst = self.resid.at[self.mine(s), :], self.rrow.at[s]
        else:
            rows = self.half_rows(s, idx - 4)
            src, dst = self.full.at[rows, :], self.out.at[rows, :]
        return pltpu.make_async_copy(src, dst, self.lsem.at[s, idx])

    def barrier(self):
        sem = pltpu.get_barrier_semaphore()
        peers = (self.partner,) + self.ring_devs[1] + self.ring_devs[2]
        for peer in peers:
            pl.semaphore_signal(sem, inc=1, device_id={'tp': peer}, device_id_type=pl.DeviceIdType.MESH)
        pl.semaphore_wait(sem, len(peers))

    def columns(self):
        self.gain[...] = self.gain_in[...].astype(F32)[None, :]
        per = self.stats[0].shape[1]
        lane = lax.broadcasted_iota(jnp.int32, (128, 128), 0)
        for i in range(self.rows // 128):
            b, off = divmod(i * 128, per)
            block = jnp.zeros((128, 128), F32)
            for k, src in enumerate(self.stats):
                block = jnp.where(lane == k, jnp.broadcast_to(src[b:b + 1, off:off + 128], (128, 128)), block)
            self.cols_of[pl.ds(i * 128, 128), :] = jnp.transpose(block)

    def normed(self, block, rows, k):
        return (block.astype(F32) - self.cols_of[rows, k:k + 1]) * self.cols_of[rows, k + 1:k + 2]

    def begin(self):
        for s in range(self.streams):
            if self.part is not None:
                self.local(s, 0).start()
            self.local(s, 1).start()
            self.local(s, 2).start()
        self.barrier()
        if self.part is not None:
            for s in range(self.streams):
                self.start(s, 'pair')
        self.columns()

    def rs1_start(self, s):
        if self.part is not None:
            self.local(s, 0).wait()
        self.arrived(s, 'pair')
        step = self.l1

        def add(i, carry):
            rows = pl.ds(pl.multiple_of(i * step, step), step)
            got = self.full[self.ds(s * self.blk + self.core * self.half + i * step, step), :]
            self.own[s, rows, :] = (self.own[s, rows, :].astype(F32) + got.astype(F32)).astype(BF16)
            return carry

        lax.fori_loop(0, self.half // step, add, 0)
        self.start(s, 'axp', 'axm', 'adp', 'adm')
        if self.part is None:
            self.get(s, 'pair').wait_send()
            pl.semaphore_signal(self.freed.at[s], inc=1, device_id={'tp': self.partner},
                                device_id_type=pl.DeviceIdType.MESH)

    def relay(self, s, tag, bufs, base, size, p):
        for buf, j, col0, got, nxt in ((0, p + 1, 0, 'xp', 'rp'), (1, p - 1, self.hw, 'xm', 'rm')):
            self.arrived(s, tag + got)
            rows = self.ds(base + self.m(j) * size, size)
            cols = pl.ds(col0, self.hw)
            self.own[s, rows, cols] = (self.own[s, rows, cols].astype(F32) + bufs[s, buf].astype(F32)).astype(BF16)
            self.start(s, tag + nxt)

    def final(self, s, tag, bufs, base, size, p):
        self.arrived(s, tag + 'rp', tag + 'dm', tag + 'rm', tag + 'dp')
        rows = self.ds(base + p * size, size)
        sums = []
        for col0, one, two in ((0, 4, 3), (self.hw, 5, 2)):
            sums.append(self.own[s, rows, pl.ds(col0, self.hw)].astype(F32)
                        + bufs[s, one].astype(F32) + bufs[s, two].astype(F32))
        return rows, sums

    def rs1_relay(self, s):
        self.relay(s, 'a', self.ring1, 0, self.l1, self.p1)

    def rs2_start(self, s):
        rows, sums = self.final(s, 'a', self.ring1, 0, self.l1, self.p1)
        for k in range(2):
            self.own[s, rows, pl.ds(k * self.hw, self.hw)] = sums[k].astype(BF16)
        self.start(s, 'bxp', 'bxm', 'bdp', 'bdm')

    def rs2_relay(self, s):
        self.relay(s, 'b', self.ring2, self.p1 * self.l1, self.l2, self.p2)

    def norm_gather(self, s):
        _, sums = self.final(s, 'b', self.ring2, self.p1 * self.l1, self.l2, self.p2)
        self.local(s, 1).wait()
        self.local(s, 2).wait()
        mine = self.mine(s)
        mu = self.cols_of[mine, 0:1]
        r = self.cols_of[mine, 1:2]
        us, xs = [], []
        for k in range(2):
            cols = pl.ds(k * self.hw, self.hw)
            us.append(sums[k] * self.gain[:, cols])
            xs.append((self.zrow[s, :, cols].astype(F32) - mu) * r)
        inv = 1.0 / self.cols
        mean_u = (jnp.sum(us[0], axis=-1, keepdims=True) + jnp.sum(us[1], axis=-1, keepdims=True)) * inv
        mean_c = (jnp.sum(us[0] * xs[0], axis=-1, keepdims=True)
                  + jnp.sum(us[1] * xs[1], axis=-1, keepdims=True)) * inv
        for k in range(2):
            cols = pl.ds(k * self.hw, self.hw)
            grad = self.rrow[s, :, cols].astype(F32) + r * (us[k] - mean_u - xs[k] * mean_c)
            self.full[mine, cols] = grad.astype(BF16)
        self.start(s, 'csp', 'csm')

    def ag2_relay(self, s):
        self.arrived(s, 'csp')
        self.start(s, 'cyp')
        self.arrived(s, 'csm')
        self.start(s, 'cym')

    def ag1_start(self, s):
        self.arrived(s, 'cyp', 'cym')
        if self.part is None:
            pl.semaphore_wait(self.freed.at[s], 1)
        self.start(s, 'dsp', 'dsm', 'k0')

    def ag1_relay(self, s):
        self.arrived(s, 'dsp')
        self.start(s, 'dyp')
        self.arrived(s, 'dsm')
        self.start(s, 'dym', 'k3', 'k1')

    def ag1_final(self, s):
        self.arrived(s, 'dyp', 'dym')
        self.start(s, 'k2')
        self.local(s, 4).start()

    def finish(self, s):
        self.arrived(s, 'k0', 'k1', 'k2', 'k3')
        self.local(s, 5).start()

    def end(self):
        for s, name in self.sent:
            if name != 'pair' or self.part is not None:
                self.get(s, name).wait_send()
        for s in range(self.streams):
            self.local(s, 4).wait()
            self.local(s, 5).wait()

    def stages(self):
        x1, x2 = self.l1 * self.hw * 2, self.l2 * self.hw * 2
        return [
            ('rs1_start', ['pair', 'own'], [('axp', '+', x1), ('axm', '-', x1), ('adp', '+', x1), ('adm', '-', x1)]),
            ('rs1_relay', ['axp', 'axm'], [('arp', '+', x1), ('arm', '-', x1)]),
            ('rs2_start', ['arp', 'arm', 'adp', 'adm'],
             [('bxp', '+', x2), ('bxm', '-', x2), ('bdp', '+', x2), ('bdm', '-', x2)]),
            ('rs2_relay', ['bxp', 'bxm'], [('brp', '+', x2), ('brm', '-', x2)]),
            ('norm_gather', ['brp', 'brm', 'bdp', 'bdm'], [('csp', '+', 2 * x2), ('csm', '-', 2 * x2)]),
            ('ag2_relay', ['csp', 'csm'], [('cyp', '+', x2), ('cym', '-', x2)]),
            ('ag1_start', ['cyp', 'cym'], [('dsp', '+', 2 * x1), ('dsm', '-', 2 * x1), ('k0', 'D', 2 * x1)]),
            ('ag1_relay', ['dsp', 'dsm'], [('dyp', '+', x1), ('dym', '-', x1), ('k3', 'D', 2 * x1), ('k1', 'D', 2 * x1)]),
            ('ag1_final', ['dyp', 'dym'], [('k2', 'D', 2 * x1)]),
            ('finish', ['k0', 'k1', 'k2', 'k3'], []),
        ]

    def plan(self, points):
        stages = self.stages()
        pair_bytes = self.half * self.cols * 2
        free = dict.fromkeys(LINK, 0.0)
        done = {}
        at = [0] * self.streams
        now = 0.0

        def push(s, name, link, size):
            free[link] = max(free[link], now) + size / LINK[link]
            done[s, name] = free[link] + LATENCY

        def ready(s):
            if at[s] >= len(stages):
                return math.inf
            return max(done.get((s, need), math.inf) for need in stages[at[s]][1])

        plans = []
        for i, (cost, gives) in enumerate(points):
            now += cost
            todo = []
            for s, what in gives:
                if what == 'pair':
                    push(s, 'pair', 'D', pair_bytes)
                    if self.part_given is False:
                        todo.append(('send_pair', s))
                else:
                    done[s, 'own'] = now
            last = i == len(points) - 1
            while True:
                s = min(range(self.streams), key=ready)
                t = ready(s)
                if t == math.inf or (t > now and not last):
                    break
                now = max(now, t) + TICK
                name, _, sends = stages[at[s]]
                for copy, link, size in sends:
                    push(s, copy, link, size)
                at[s] += 1
                todo.append((name, s))
            plans.append(todo)
        assert all(a == len(stages) for a in at)
        self.estimate = now
        return plans

    def tuned(self, table, points):
        self.points = points
        plans = self.plan(points)
        if not table or len(plans) != table[0]:
            return plans
        names = [stage[0] for stage in self.stages()]
        out = [[step for step in todo if step[0] == 'send_pair'] for todo in plans]
        for code in table[1]:
            point, rest = divmod(code, 64)
            out[point].append((names[rest // 4], rest % 4))
        return out

    def send_pair(self, s):
        self.start(s, 'pair')

    part_given = False


MLP_PLAN = (60, [
    512, 769, 964, 1029, 1154, 1352, 1417, 1414, 1549, 1539, 1674, 1799, 1934, 1932, 1937, 1995, 2002, 2064,
    2127, 2133, 2198, 2196, 2195, 2265, 2330, 2653, 2647, 2712, 2846, 2907, 3170, 3169, 3164, 3295, 3365,
    3488, 3494, 3555, 3684, 3751])
ATT_PLAN = (54, [
    1153, 1605, 1664, 1865, 1860, 2061, 2051, 2248, 2247, 2257, 2380, 2370, 2517, 2502, 2507, 2576, 2634,
    2639, 2649, 2766, 2771, 2836, 2845, 2834, 2903, 2904, 2977, 3030, 3035, 3098, 3167, 3228, 3294, 3363,
    3424, 3426, 3429, 3428, 3431, 3430])
VMEM_LIMIT = 64 * 1024 * 1024 - 64 * 1024


def dot(a, b, ca=1, cb=0):
    return lax.dot_general(a, b, (((ca,), (cb,)), ((), ())), preferred_element_type=F32)


def mlp_stage(n, h1, dy, x, stats, gain, gain_x, w_up, w_down, w_qkv, width, cid):
    rows, cols = h1.shape
    ffn = w_up.shape[1]
    comm = Comm(n, rows, cols)
    tile = comm.half
    n_tiles = rows // tile
    cb = 384
    n_cols = cols // cb
    hd = width + -width % 128
    qkv_w = 3 * hd
    dw_end = n_tiles + n_cols
    wide = 2 * tile
    grid = dw_end + rows // wide
    points = []
    for i in range(n_tiles):
        points += [(1.5 if i else 7.0, []), (0.9, []), (2.0, [(i // 2, 'pair' if i % 2 == 0 else 'own')])]
    for i in range(n_cols):
        points += [(1.0, []), (1.5, []), (1.2, [])]
    points += [(2.8, []), (0.0, []), (0.0, [])] * (rows // wide)
    plans = comm.tuned(MLP_PLAN, points)

    def kernel(h1_tile, dy_tile, h1_col, dy_col, x_tile, w1, w2, mean2, rstd2, mean1, rstd1, gain_ref, gain_x_ref,
               wqkv_in, h1_all, dy_all, dh1_ref, dw1_ref, dw2_ref, qkv_ref, act, da, wqkv, gx, wsem, *scratch):
        comm.bind(None, h1_all, dy_all, (mean2, rstd2, mean1, rstd1), gain_ref, dh1_ref, scratch)
        i = pl.program_id(0)
        full, own = comm.full, comm.own

        def ticks(steps, k):
            if any(plans[step * 3 + k] for step in steps):
                @pl.when(jnp.logical_and(i >= steps[0], i <= steps[-1]))
                def _():
                    for step in steps:
                        todo = plans[step * 3 + k]
                        if todo:
                            @pl.when(i == step)
                            def _():
                                for name, s in todo:
                                    getattr(comm, name)(s)

        loads = [pltpu.make_async_copy(wqkv_in.at[pl.ds(c * width, width), :], wqkv.at[pl.ds(c * hd, width), :],
                                       wsem.at[c]) for c in range(3)]

        @pl.when(i == 0)
        def _():
            for load in loads:
                load.start()
            for c in range(3):
                wqkv[pl.ds(c * hd + width, hd - width), :] = jnp.zeros((hd - width, cols), BF16)
            gx[...] = gain_x_ref[...].astype(F32)[None, :]
            comm.begin()

        first = range(n_tiles)
        rest = range(n_tiles, dw_end)
        last = range(dw_end, grid)
        tidx = lax.div(i, 2) * 2 + lax.rem(i, 2) * comm.core + (1 - lax.rem(i, 2)) * (1 - comm.core)
        trow = pl.ds(pl.multiple_of(tidx * tile, tile), tile)
        pre_ref, dg_ref = comm.pre, comm.dg

        @pl.when(i < n_tiles)
        def _():
            n2 = (comm.normed(h1_tile[...], trow, 0) * comm.gain[...]).astype(BF16)
            pre_ref[...] = dot(n2, w1[...])
        ticks(first, 0)

        @pl.when(i < n_tiles)
        def _():
            dg_ref[...] = dot(dy_tile[...], w2[...], 1, 1)
        ticks(first, 1)

        @pl.when(i < n_tiles)
        def _():
            pre = pre_ref[...]
            act[trow, :] = gelu_tanh(pre).astype(BF16)
            grad_pre = (dg_ref[...] * gelu_slope(pre)).astype(BF16)
            da[trow, :] = grad_pre
            part = dot(grad_pre, w1[...], 1, 1).astype(BF16)

            @pl.when(lax.rem(i, 2) == 0)
            def _():
                full[trow, :] = part

            @pl.when(lax.rem(i, 2) == 1)
            def _():
                own[lax.div(i, 2)] = part
        ticks(first, 2)

        @pl.when(jnp.logical_and(i >= n_tiles, i < dw_end))
        def _():
            c0 = pl.multiple_of((i - n_tiles) * cb, cb)
            comm.n2c[...] = (comm.normed(h1_col[...], pl.ds(0, rows), 0) * comm.gain[:, pl.ds(c0, cb)]).astype(BF16)
        ticks(rest, 0)

        @pl.when(jnp.logical_and(i >= n_tiles, i < dw_end))
        def _():
            dw1_ref[...] = dot(comm.n2c[...], da[...], 0, 0).astype(BF16)
        ticks(rest, 1)

        @pl.when(jnp.logical_and(i >= n_tiles, i < dw_end))
        def _():
            dw2_ref[...] = dot(act[...], dy_col[...], 0, 0).astype(BF16)
        ticks(rest, 2)

        @pl.when(i == dw_end)
        def _():
            for load in loads:
                load.wait()

        @pl.when(i >= dw_end)
        def _():
            xrow = pl.ds(pl.multiple_of((i - dw_end) * wide, wide), wide)
            n1 = (comm.normed(x_tile[...], xrow, 2) * gx[...]).astype(BF16)
            qkv_ref[...] = dot(n1, wqkv[...], 1, 1).astype(BF16)
        ticks(last, 0)
        ticks(last, 1)
        ticks(last, 2)

        @pl.when(i == grid - 1)
        def _():
            comm.end()

    def wrapped(*refs):
        *most, pre, dg, n2c = refs
        comm.pre, comm.dg, comm.n2c = pre, dg, n2c
        kernel(*most)

    def tile_map(i):
        core = lax.rem(lax.axis_index('tp'), 2)
        ii = jnp.minimum(i, n_tiles - 1)
        odd = lax.rem(ii, 2)
        return lax.div(ii, 2) * 2 + odd * core + (1 - odd) * (1 - core), 0

    def col_at(i):
        return jnp.clip(i - n_tiles, 0, n_cols - 1)

    def x_at(i):
        return jnp.maximum(i - dw_end, 0), 0

    whole = pl.BlockSpec(memory_space=VMEM)
    hbm = pl.BlockSpec(memory_space=ANY)
    return pl.pallas_call(
        wrapped,
        grid=(grid,),
        out_shape=(jax.ShapeDtypeStruct((rows, cols), BF16), jax.ShapeDtypeStruct((cols, ffn), BF16),
                   jax.ShapeDtypeStruct((ffn, cols), BF16), jax.ShapeDtypeStruct((rows, qkv_w), BF16)),
        in_specs=[pl.BlockSpec((tile, cols), tile_map), pl.BlockSpec((tile, cols), tile_map),
                  pl.BlockSpec((rows, cb), lambda i: (0, col_at(i))), pl.BlockSpec((rows, cb), lambda i: (0, col_at(i))),
                  pl.BlockSpec((wide, cols), x_at), whole, whole] + [whole] * 6 + [hbm] * 3,
        out_specs=(hbm, pl.BlockSpec((cb, ffn), lambda i: (col_at(i), 0)),
                   pl.BlockSpec((ffn, cb), lambda i: (0, col_at(i))), pl.BlockSpec((wide, qkv_w), x_at)),
        scratch_shapes=[VMEM((rows, ffn), BF16), VMEM((rows, ffn), BF16), VMEM((qkv_w, cols), BF16), VMEM((1, cols), F32),
                        pltpu.SemaphoreType.DMA((3,))] + comm.scratch()
        + [VMEM((tile, ffn), F32), VMEM((tile, ffn), F32), VMEM((rows, cb), BF16)],
        compiler_params=pltpu.CompilerParams(collective_id=cid, has_side_effects=True, vmem_limit_bytes=VMEM_LIMIT,
                                             dimension_semantics=('arbitrary',)),
        name='mlp_stage',
    )(h1, dy, h1, dy, x, w_up, w_down, *stats, gain, gain_x, w_qkv, h1, dy)


def attention_stage(n, mbs, x, dh1, qkv_all, stats, gain, w_qkv, w_out, score_scale, cid):
    rows, cols = x.shape
    seq = rows // mbs
    width = w_out.shape[0]
    hd = width + -width % 128
    qkv_w = 3 * hd
    comm = Comm(n, rows, cols)
    tile = comm.half
    per_mb = seq // tile
    wide = 2 * tile
    lead = seq // wide
    span = lead + per_mb
    n_seq = span * mbs
    cb = 512
    n_cols = cols // cb
    grid = n_seq + n_cols
    points = []
    for b in range(mbs):
        points += [(0.0, []), (1.4, []), (0.0, [])] * lead
        for j in range(per_mb - 1, -1, -1):
            s = b * (per_mb // 2) + j // 2
            points += [(1.0, []), (0.9, []), (1.45, [(s, 'pair'), (s, 'own')] if j % 2 == 0 else [])]
    for i in range(n_cols):
        points += [(1.4, []), (2.0, []), (0.7, [])]
    points[0] = (5.5, [])
    plans = comm.tuned(ATT_PLAN, points)

    def kernel(dh_tile, x_col, dh_col, qkv, wqkv_in, wo_in, mean_ref, rstd_ref, gain_ref, x_all, dh_all,
               dx_ref, dwqkv_ref, dwo_ref, do, o_all, dqkv, dk_acc, dv_acc, n1c, p_ref, wqkv, wo, wsem, *scratch):
        comm.bind(None, x_all, dh_all, (mean_ref, rstd_ref), gain_ref, dx_ref, scratch)
        i = pl.program_id(0)
        full, own = comm.full, comm.own

        def ticks(steps, k):
            if any(plans[step * 3 + k] for step in steps):
                @pl.when(jnp.logical_and(i >= steps[0], i <= steps[-1]))
                def _():
                    for step in steps:
                        todo = plans[step * 3 + k]
                        if todo:
                            @pl.when(i == step)
                            def _():
                                for name, s in todo:
                                    getattr(comm, name)(s)

        @pl.when(i == 0)
        def _():
            loads = [pltpu.make_async_copy(wqkv_in.at[pl.ds(c * width, width), :], wqkv.at[pl.ds(c * hd, width), :],
                                           wsem.at[c]) for c in range(3)]
            loads.append(pltpu.make_async_copy(wo_in, wo.at[pl.ds(0, width), :], wsem.at[3]))
            for load in loads:
                load.start()
            zero = jnp.zeros((hd - width, cols), BF16)
            for c in range(3):
                wqkv[pl.ds(c * hd + width, hd - width), :] = zero
            wo[pl.ds(width, hd - width), :] = zero
            comm.begin()
            for load in loads:
                load.wait()

        first = range(n_seq)
        rest = range(n_seq, grid)
        b = lax.div(i, span)
        at = lax.rem(i, span)
        in_seq = i < n_seq
        loading = jnp.logical_and(in_seq, at < lead)
        base = b * seq
        trow = pl.ds(pl.multiple_of(jnp.minimum(base + at * wide, rows - wide), wide), wide)

        def variants(fn):
            for j in range(per_mb):
                @pl.when(jnp.logical_and(in_seq, at == span - 1 - j))
                def _():
                    fn(j)

        def part_a(j):
            size = (j + 1) * tile
            mine = pl.ds(pl.multiple_of(base + j * tile, tile), tile)
            keys = pl.ds(pl.multiple_of(base, tile), size)
            s = dot(qkv[mine, 0:hd], qkv[keys, hd:2 * hd], 1, 1) * score_scale
            row = lax.broadcasted_iota(jnp.int32, (tile, size), 0) + j * tile
            col = lax.broadcasted_iota(jnp.int32, (tile, size), 1)
            s = jnp.where(row >= col, s, -1e30)
            e = jnp.exp(s - jnp.max(s, axis=-1, keepdims=True))
            p = e / jnp.sum(e, axis=-1, keepdims=True)
            p_ref[:, 0:size] = p
            pb = p.astype(BF16)
            o_all[mine, :] = dot(pb, qkv[keys, 2 * hd:3 * hd]).astype(BF16)
            dv = dot(pb, do[mine, :], 0, 0)
            if j == per_mb - 1:
                dv_acc[...] = dv
            else:
                dv_acc[0:size, :] += dv

        def part_b(j):
            size = (j + 1) * tile
            mine = pl.ds(pl.multiple_of(base + j * tile, tile), tile)
            keys = pl.ds(pl.multiple_of(base, tile), size)
            p = p_ref[:, 0:size]
            dp = dot(do[mine, :], qkv[keys, 2 * hd:3 * hd], 1, 1)
            rd = jnp.sum(p * dp, axis=-1, keepdims=True)
            ds = (p * (dp - rd) * score_scale).astype(BF16)
            dqkv[mine, 0:hd] = dot(ds, qkv[keys, hd:2 * hd]).astype(BF16)
            dk = dot(ds, qkv[mine, 0:hd], 0, 0)
            if j == per_mb - 1:
                dk_acc[...] = dk
            else:
                dk_acc[0:size, :] += dk
            dqkv[mine, hd:2 * hd] = dk_acc[j * tile:size, :].astype(BF16)
            dqkv[mine, 2 * hd:3 * hd] = dv_acc[j * tile:size, :].astype(BF16)

        def part_c(j):
            mine = pl.ds(pl.multiple_of(base + j * tile, tile), tile)
            part = dot(dqkv[mine, :], wqkv[...]).astype(BF16)

            @pl.when(comm.core == j % 2)
            def _():
                own[b * (per_mb // 2) + j // 2] = part

            @pl.when(comm.core != j % 2)
            def _():
                full[mine, :] = part

        variants(part_a)
        ticks(first, 0)

        @pl.when(loading)
        def _():
            do[trow, :] = dot(dh_tile[...], wo[...], 1, 1).astype(BF16)

        variants(part_b)
        ticks(first, 1)
        variants(part_c)
        ticks(first, 2)

        @pl.when(i >= n_seq)
        def _():
            c0 = pl.multiple_of((i - n_seq) * cb, cb)
            n1c[...] = (comm.normed(x_col[...], pl.ds(0, rows), 0) * comm.gain[:, pl.ds(c0, cb)]).astype(BF16)
        ticks(rest, 0)

        @pl.when(i >= n_seq)
        def _():
            dwqkv_ref[...] = dot(dqkv[...], n1c[...], 0, 0).astype(BF16)
        ticks(rest, 1)

        @pl.when(i >= n_seq)
        def _():
            dwo_ref[...] = dot(o_all[...], dh_col[...], 0, 0).astype(BF16)
        ticks(rest, 2)

        @pl.when(i == grid - 1)
        def _():
            comm.end()

    def tile_map(i):
        ii = jnp.minimum(i, n_seq - 1)
        return lax.div(ii, span) * lead + jnp.minimum(lax.rem(ii, span), lead - 1), 0

    def col_at(i):
        return jnp.maximum(i - n_seq, 0)

    whole = pl.BlockSpec(memory_space=VMEM)
    hbm = pl.BlockSpec(memory_space=ANY)
    return pl.pallas_call(
        kernel,
        grid=(grid,),
        out_shape=(jax.ShapeDtypeStruct((rows, cols), BF16), jax.ShapeDtypeStruct((qkv_w, cols), BF16),
                   jax.ShapeDtypeStruct((hd, cols), BF16)),
        in_specs=[pl.BlockSpec((wide, cols), tile_map),
                  pl.BlockSpec((rows, cb), lambda i: (0, col_at(i))), pl.BlockSpec((rows, cb), lambda i: (0, col_at(i))),
                  whole, hbm, hbm, whole, whole, whole, hbm, hbm],
        out_specs=(hbm, pl.BlockSpec((qkv_w, cb), lambda i: (0, col_at(i))),
                   pl.BlockSpec((hd, cb), lambda i: (0, col_at(i)))),
        scratch_shapes=[VMEM((rows, hd), BF16), VMEM((rows, hd), BF16),
                        VMEM((rows, qkv_w), BF16), VMEM((seq, hd), F32), VMEM((seq, hd), F32), VMEM((rows, cb), BF16),
                        VMEM((tile, seq), F32), VMEM((qkv_w, cols), BF16), VMEM((hd, cols), BF16),
                        pltpu.SemaphoreType.DMA((4,))] + comm.scratch(),
        compiler_params=pltpu.CompilerParams(collective_id=cid, has_side_effects=True, vmem_limit_bytes=VMEM_LIMIT,
                                             dimension_semantics=('arbitrary',)),
        name='attention_stage',
    )(dh1, x, dh1, qkv_all, w_qkv, w_out, *stats, gain, x, dh1)


def spread_copy(dx, dw_up, dw_down, dw_qkv, dw_out, width):
    def rows_of(arr, parts):
        step = arr.shape[0] // parts
        return [(k * step, k * step, step) for k in range(parts)]

    hd = dw_out.shape[0]
    srcs = (dx, dw_up, dw_down, dw_qkv, dw_out)
    moves = (rows_of(dx, 8), rows_of(dw_up, 2), rows_of(dw_down, 2), [(c * hd, c * width, width) for c in range(3)],
             [(0, 0, width)])
    outs = [jax.ShapeDtypeStruct((sum(m[2] for m in mv), a.shape[1]), a.dtype) for a, mv in zip(srcs, moves)]
    total = sum(len(mv) for mv in moves)

    def kernel(*refs):
        ins, dsts, bufs, (in_sem, out_sem) = refs[:5], refs[5:10], refs[10:15], refs[15:]
        reads, writes = [], []
        for a, mv in enumerate(moves):
            for frm, to, size in mv:
                k = len(reads)
                here = bufs[a].at[pl.ds(to, size), :]
                reads.append(pltpu.make_async_copy(ins[a].at[pl.ds(frm, size), :], here, in_sem.at[k]))
                writes.append(pltpu.make_async_copy(here, dsts[a].at[pl.ds(to, size), :], out_sem.at[k]))
        for read in reads:
            read.start()
        for read, write in zip(reads, writes):
            read.wait()
            write.start()
        for write in writes:
            write.wait()

    hbm = pl.BlockSpec(memory_space=ANY)
    return pl.pallas_call(
        kernel,
        out_shape=outs,
        in_specs=[hbm] * 5,
        out_specs=[hbm] * 5,
        scratch_shapes=[VMEM(o.shape, o.dtype) for o in outs]
        + [pltpu.SemaphoreType.DMA((total,)), pltpu.SemaphoreType.DMA((total,))],
        compiler_params=pltpu.CompilerParams(vmem_limit_bytes=VMEM_LIMIT),
        name='spread_copy',
    )(*srcs)


def solution(mesh):
    act_spec = P('dp', None, None)
    stat_spec = P('dp', None)
    in_specs = (act_spec, act_spec, act_spec, stat_spec, stat_spec, stat_spec, stat_spec, P(), P(),
                P(None, 'tp', None, None), P('tp', None, None), P(None, 'tp'), P('tp', None))
    out_specs = (act_spec, P('dp', 'tp', None, None), P(('dp', 'tp'), None, None), P('dp', 'tp'),
                 P(('dp', 'tp'), None))
    n = mesh.shape['tp']

    def local_backward(x_saved, h1_saved, grad_y, mean_one, rstd_one, mean_two, rstd_two,
                       gain_one, gain_two, w_qkv, w_out, w_up, w_down):
        score_scale = w_qkv.shape[3] ** -0.5
        shape = x_saved.shape
        flat = (shape[0] * shape[1], shape[2])
        heads, _, width = w_qkv.shape[1:]
        rows_qkv = w_qkv.transpose(1, 2, 3, 0).reshape(3 * width, flat[1])
        h1, dy, x = h1_saved.reshape(flat), grad_y.reshape(flat), x_saved.reshape(flat)
        dh1, grad_up, grad_down, qkv = mlp_stage(n, h1, dy, x, (mean_two, rstd_two, mean_one, rstd_one), gain_two,
                                                 gain_one, w_up, w_down, rows_qkv, width, 0)
        dx, dqkv_w, dout_w = attention_stage(n, shape[0], x, dh1, qkv, (mean_one, rstd_one), gain_one, rows_qkv,
                                             w_out[0], score_scale, 1)
        dx, grad_up, grad_down, dqkv_w, dout_w = spread_copy(dx, grad_up, grad_down, dqkv_w, dout_w, width)
        grad_qkv_w = dqkv_w.reshape(heads, 3, width, flat[1]).transpose(3, 0, 1, 2)
        return dx.reshape(shape), grad_qkv_w, dout_w[None], grad_up, grad_down

    return jax.shard_map(local_backward, mesh=mesh, in_specs=in_specs, out_specs=out_specs, check_vma=False)
```

```python
import math
import jax
import jax.numpy as jnp
from jax import lax
from jax.experimental import pallas as pl
from jax.experimental.pallas import tpu as pltpu
from jax.sharding import PartitionSpec as P

GELU_C = 0.7978845608028654
GELU_A = 0.044715
F32 = jnp.float32
BF16 = jnp.bfloat16
ANY = pl.ANY
VMEM = pltpu.VMEM


def gelu_tanh(pre_act):
    inner_arg = GELU_C * (pre_act + GELU_A * pre_act * pre_act * pre_act)
    return 0.5 * pre_act * (1.0 + jnp.tanh(inner_arg))


def gelu_slope(pre_act):
    inner_arg = GELU_C * (pre_act + GELU_A * pre_act * pre_act * pre_act)
    tanh_val = jnp.tanh(inner_arg)
    return (0.5 * (1.0 + tanh_val)
            + 0.5 * pre_act * (1.0 - tanh_val * tanh_val) * GELU_C * (1.0 + 3.0 * GELU_A * pre_act * pre_act))


BLOCK = 512
SEMS = 32
LINK = {'+': 90e3, '-': 90e3, 'D': 450e3}
LATENCY = 2.6
TICK = 0.3


class Comm:
    def __init__(self, n, rows, cols):
        self.side = math.isqrt(n // 2)
        assert self.side == 4 and 2 * self.side * self.side == n
        self.rows, self.cols = rows, cols
        self.blk = BLOCK
        self.streams = rows // BLOCK
        self.half = self.blk // 2
        self.l1 = self.half // self.side
        self.l2 = self.l1 // self.side
        self.hw = cols // 2

    N_SCRATCH = 12

    def scratch(self):
        l1, l2, w, hw, ns = self.l1, self.l2, self.cols, self.hw, self.streams
        return [
            VMEM((ns, self.half, w), BF16),
            VMEM((ns, 6, l1, hw), BF16),
            VMEM((ns, 6, l2, hw), BF16),
            VMEM((self.rows, w), BF16),
            VMEM((ns, l2, w), BF16),
            VMEM((ns, l2, w), BF16),
            VMEM((self.rows, 128), F32),
            VMEM((1, w), F32),
            pltpu.SemaphoreType.DMA((ns, SEMS)),
            pltpu.SemaphoreType.DMA((ns, SEMS)),
            pltpu.SemaphoreType.DMA((ns, 8)),
            pltpu.SemaphoreType.REGULAR((ns,)),
        ]

    def bind(self, part, saved, resid, stats, gain, out, scratch):
        (self.own, self.ring1, self.ring2, self.full, self.zrow, self.rrow, self.cols_of, self.gain,
         self.ssem, self.rsem, self.lsem, self.freed) = scratch
        self.part, self.saved, self.resid, self.gain_in, self.out = part, saved, resid, gain, out
        self.stats = stats
        side = self.side
        me = lax.axis_index('tp')
        core = lax.rem(me, 2)
        x = lax.rem(lax.div(me, 2), side)
        y = lax.div(me, 2 * side)
        self.core = core
        self.p1 = x * (1 - core) + y * core
        self.p2 = y * (1 - core) + x * core

        def dev(p1, p2):
            p1, p2 = lax.rem(p1 + side, side), lax.rem(p2 + side, side)
            xx = p1 * (1 - core) + p2 * core
            yy = p2 * (1 - core) + p1 * core
            return (yy * side + xx) * 2 + core

        self.partner = me + 1 - 2 * core
        self.ring_devs = {1: (dev(self.p1 + 1, self.p2), dev(self.p1 - 1, self.p2)),
                          2: (dev(self.p1, self.p2 + 1), dev(self.p1, self.p2 - 1))}
        self.sent = []

    def m(self, j):
        return lax.rem(j + self.side, self.side)

    def ds(self, off, size):
        return pl.ds(pl.multiple_of(off, 16), size)

    def half_rows(self, s, which):
        c = self.core if which == 0 else 1 - self.core
        return self.ds(s * self.blk + c * self.half, self.half)

    def copies(self, s):
        side, l1, l2, hw, w = self.side, self.l1, self.l2, self.hw, self.cols
        c, p1, p2, m, ds = self.core, self.p1, self.p2, self.m, self.ds
        left, right = pl.ds(0, hw), pl.ds(hw, hw)
        own, full = self.own.at[s], self.full
        row0 = s * self.blk
        out = {}
        theirs = full.at[self.half_rows(s, 1), :]
        out['pair'] = (0, theirs, theirs, self.partner)

        def ring(tag, first, base, size, p, bufs, devs):
            plus, minus = devs

            def chunk(j, cols):
                return own.at[ds(base + m(j) * size, size), cols]

            out[tag + 'xp'] = (first + 0, chunk(p + 2, left), bufs.at[s, 0], plus)
            out[tag + 'xm'] = (first + 1, chunk(p + 2, right), bufs.at[s, 1], minus)
            out[tag + 'dp'] = (first + 2, chunk(p + 1, right), bufs.at[s, 2], plus)
            out[tag + 'dm'] = (first + 3, chunk(p - 1, left), bufs.at[s, 3], minus)
            out[tag + 'rp'] = (first + 4, chunk(p + 1, left), bufs.at[s, 4], plus)
            out[tag + 'rm'] = (first + 5, chunk(p - 1, right), bufs.at[s, 5], minus)

        ring('a', 1, 0, l1, p1, self.ring1, self.ring_devs[1])
        ring('b', 7, p1 * l1, l2, p2, self.ring2, self.ring_devs[2])

        def gather(tag, first, base, size, p, devs):
            plus, minus = devs

            def chunk(j, cols):
                return full.at[ds(base + m(j) * size, size), cols]

            every = pl.ds(0, w)
            for name, idx, view, to in (('sp', 0, chunk(p, every), plus), ('sm', 1, chunk(p, every), minus),
                                        ('yp', 2, chunk(p - 1, left), plus), ('ym', 3, chunk(p + 1, right), minus)):
                out[tag + name] = (first + idx, view, view, to)

        half0 = row0 + c * self.half
        gather('c', 13, half0 + p1 * l1, l2, p2, self.ring_devs[2])
        gather('d', 17, half0, l1, p1, self.ring_devs[1])
        for j in range(side):
            view = full.at[ds(half0 + m(p1 + j) * l1, l1), :]
            out['k%d' % j] = (21 + j, view, view, self.partner)
        return out

    def get(self, s, name):
        idx, src, dst, to = self.copies(s)[name]
        return pltpu.make_async_remote_copy(src_ref=src, dst_ref=dst, send_sem=self.ssem.at[s, idx],
                                            recv_sem=self.rsem.at[s, idx], device_id={'tp': to},
                                            device_id_type=pl.DeviceIdType.MESH)

    def start(self, s, *names):
        for name in names:
            self.get(s, name).start()
            self.sent.append((s, name))

    def arrived(self, s, *names):
        for name in names:
            self.get(s, name).wait_recv()

    def mine(self, s):
        return self.ds(s * self.blk + self.core * self.half + self.p1 * self.l1 + self.p2 * self.l2, self.l2)

    def local(self, s, idx):
        if idx == 0:
            src, dst = self.part.at[self.half_rows(s, 0), :], self.own.at[s]
        elif idx == 1:
            src, dst = self.saved.at[self.mine(s), :], self.zrow.at[s]
        elif idx == 2:
            src, dst = self.resid.at[self.mine(s), :], self.rrow.at[s]
        else:
            rows = self.half_rows(s, idx - 4)
            src, dst = self.full.at[rows, :], self.out.at[rows, :]
        return pltpu.make_async_copy(src, dst, self.lsem.at[s, idx])

    def barrier(self):
        sem = pltpu.get_barrier_semaphore()
        peers = (self.partner,) + self.ring_devs[1] + self.ring_devs[2]
        for peer in peers:
            pl.semaphore_signal(sem, inc=1, device_id={'tp': peer}, device_id_type=pl.DeviceIdType.MESH)
        pl.semaphore_wait(sem, len(peers))

    def columns(self):
        self.gain[...] = self.gain_in[...].astype(F32)[None, :]
        per = self.stats[0].shape[1]
        lane = lax.broadcasted_iota(jnp.int32, (128, 128), 0)
        for i in range(self.rows // 128):
            b, off = divmod(i * 128, per)
            block = jnp.zeros((128, 128), F32)
            for k, src in enumerate(self.stats):
                block = jnp.where(lane == k, jnp.broadcast_to(src[b:b + 1, off:off + 128], (128, 128)), block)
            self.cols_of[pl.ds(i * 128, 128), :] = jnp.transpose(block)

    def normed(self, block, rows, k):
        return (block.astype(F32) - self.cols_of[rows, k:k + 1]) * self.cols_of[rows, k + 1:k + 2]

    def begin(self):
        for s in range(self.streams):
            if self.part is not None:
                self.local(s, 0).start()
            self.local(s, 1).start()
            self.local(s, 2).start()
        self.barrier()
        if self.part is not None:
            for s in range(self.streams):
                self.start(s, 'pair')
        self.columns()

    def rs1_start(self, s):
        if self.part is not None:
            self.local(s, 0).wait()
        self.arrived(s, 'pair')
        step = self.l1

        def add(i, carry):
            rows = pl.ds(pl.multiple_of(i * step, step), step)
            got = self.full[self.ds(s * self.blk + self.core * self.half + i * step, step), :]
            self.own[s, rows, :] = (self.own[s, rows, :].astype(F32) + got.astype(F32)).astype(BF16)
            return carry

        lax.fori_loop(0, self.half // step, add, 0)
        self.start(s, 'axp', 'axm', 'adp', 'adm')
        if self.part is None:
            self.get(s, 'pair').wait_send()
            pl.semaphore_signal(self.freed.at[s], inc=1, device_id={'tp': self.partner},
                                device_id_type=pl.DeviceIdType.MESH)

    def relay(self, s, tag, bufs, base, size, p):
        for buf, j, col0, got, nxt in ((0, p + 1, 0, 'xp', 'rp'), (1, p - 1, self.hw, 'xm', 'rm')):
            self.arrived(s, tag + got)
            rows = self.ds(base + self.m(j) * size, size)
            cols = pl.ds(col0, self.hw)
            self.own[s, rows, cols] = (self.own[s, rows, cols].astype(F32) + bufs[s, buf].astype(F32)).astype(BF16)
            self.start(s, tag + nxt)

    def final(self, s, tag, bufs, base, size, p):
        self.arrived(s, tag + 'rp', tag + 'dm', tag + 'rm', tag + 'dp')
        rows = self.ds(base + p * size, size)
        sums = []
        for col0, one, two in ((0, 4, 3), (self.hw, 5, 2)):
            sums.append(self.own[s, rows, pl.ds(col0, self.hw)].astype(F32)
                        + bufs[s, one].astype(F32) + bufs[s, two].astype(F32))
        return rows, sums

    def rs1_relay(self, s):
        self.relay(s, 'a', self.ring1, 0, self.l1, self.p1)

    def rs2_start(self, s):
        rows, sums = self.final(s, 'a', self.ring1, 0, self.l1, self.p1)
        for k in range(2):
            self.own[s, rows, pl.ds(k * self.hw, self.hw)] = sums[k].astype(BF16)
        self.start(s, 'bxp', 'bxm', 'bdp', 'bdm')

    def rs2_relay(self, s):
        self.relay(s, 'b', self.ring2, self.p1 * self.l1, self.l2, self.p2)

    def norm_gather(self, s):
        _, sums = self.final(s, 'b', self.ring2, self.p1 * self.l1, self.l2, self.p2)
        self.local(s, 1).wait()
        self.local(s, 2).wait()
        mine = self.mine(s)
        mu = self.cols_of[mine, 0:1]
        r = self.cols_of[mine, 1:2]
        us, xs = [], []
        for k in range(2):
            cols = pl.ds(k * self.hw, self.hw)
            us.append(sums[k] * self.gain[:, cols])
            xs.append((self.zrow[s, :, cols].astype(F32) - mu) * r)
        inv = 1.0 / self.cols
        mean_u = (jnp.sum(us[0], axis=-1, keepdims=True) + jnp.sum(us[1], axis=-1, keepdims=True)) * inv
        mean_c = (jnp.sum(us[0] * xs[0], axis=-1, keepdims=True)
                  + jnp.sum(us[1] * xs[1], axis=-1, keepdims=True)) * inv
        for k in range(2):
            cols = pl.ds(k * self.hw, self.hw)
            grad = self.rrow[s, :, cols].astype(F32) + r * (us[k] - mean_u - xs[k] * mean_c)
            self.full[mine, cols] = grad.astype(BF16)
        self.start(s, 'csp', 'csm')

    def ag2_relay(self, s):
        self.arrived(s, 'csp')
        self.start(s, 'cyp')
        self.arrived(s, 'csm')
        self.start(s, 'cym')

    def ag1_start(self, s):
        self.arrived(s, 'cyp', 'cym')
        if self.part is None:
            pl.semaphore_wait(self.freed.at[s], 1)
        self.start(s, 'dsp', 'dsm', 'k0')

    def ag1_relay(self, s):
        self.arrived(s, 'dsp')
        self.start(s, 'dyp')
        self.arrived(s, 'dsm')
        self.start(s, 'dym', 'k3', 'k1')

    def ag1_final(self, s):
        self.arrived(s, 'dyp', 'dym')
        self.start(s, 'k2')
        self.local(s, 4).start()

    def finish(self, s):
        self.arrived(s, 'k0', 'k1', 'k2', 'k3')
        self.local(s, 5).start()

    def end(self):
        for s, name in self.sent:
            if name != 'pair' or self.part is not None:
                self.get(s, name).wait_send()
        for s in range(self.streams):
            self.local(s, 4).wait()
            self.local(s, 5).wait()

    def stages(self):
        x1, x2 = self.l1 * self.hw * 2, self.l2 * self.hw * 2
        return [
            ('rs1_start', ['pair', 'own'], [('axp', '+', x1), ('axm', '-', x1), ('adp', '+', x1), ('adm', '-', x1)]),
            ('rs1_relay', ['axp', 'axm'], [('arp', '+', x1), ('arm', '-', x1)]),
            ('rs2_start', ['arp', 'arm', 'adp', 'adm'],
             [('bxp', '+', x2), ('bxm', '-', x2), ('bdp', '+', x2), ('bdm', '-', x2)]),
            ('rs2_relay', ['bxp', 'bxm'], [('brp', '+', x2), ('brm', '-', x2)]),
            ('norm_gather', ['brp', 'brm', 'bdp', 'bdm'], [('csp', '+', 2 * x2), ('csm', '-', 2 * x2)]),
            ('ag2_relay', ['csp', 'csm'], [('cyp', '+', x2), ('cym', '-', x2)]),
            ('ag1_start', ['cyp', 'cym'], [('dsp', '+', 2 * x1), ('dsm', '-', 2 * x1), ('k0', 'D', 2 * x1)]),
            ('ag1_relay', ['dsp', 'dsm'], [('dyp', '+', x1), ('dym', '-', x1), ('k3', 'D', 2 * x1), ('k1', 'D', 2 * x1)]),
            ('ag1_final', ['dyp', 'dym'], [('k2', 'D', 2 * x1)]),
            ('finish', ['k0', 'k1', 'k2', 'k3'], []),
        ]

    def plan(self, points):
        stages = self.stages()
        pair_bytes = self.half * self.cols * 2
        free = dict.fromkeys(LINK, 0.0)
        done = {}
        at = [0] * self.streams
        now = 0.0

        def push(s, name, link, size):
            free[link] = max(free[link], now) + size / LINK[link]
            done[s, name] = free[link] + LATENCY

        def ready(s):
            if at[s] >= len(stages):
                return math.inf
            return max(done.get((s, need), math.inf) for need in stages[at[s]][1])

        plans = []
        for i, (cost, gives) in enumerate(points):
            now += cost
            todo = []
            for s, what in gives:
                if what == 'pair':
                    push(s, 'pair', 'D', pair_bytes)
                    if self.part_given is False:
                        todo.append(('send_pair', s))
                else:
                    done[s, 'own'] = now
            last = i == len(points) - 1
            while True:
                s = min(range(self.streams), key=ready)
                t = ready(s)
                if t == math.inf or (t > now and not last):
                    break
                now = max(now, t) + TICK
                name, _, sends = stages[at[s]]
                for copy, link, size in sends:
                    push(s, copy, link, size)
                at[s] += 1
                todo.append((name, s))
            plans.append(todo)
        assert all(a == len(stages) for a in at)
        self.estimate = now
        return plans

    def tuned(self, table, points):
        self.points = points
        plans = self.plan(points)
        if not table or len(plans) != table[0]:
            return plans
        names = [stage[0] for stage in self.stages()]
        out = [[step for step in todo if step[0] == 'send_pair'] for todo in plans]
        for code in table[1]:
            point, rest = divmod(code, 64)
            out[point].append((names[rest // 4], rest % 4))
        return out

    def send_pair(self, s):
        self.start(s, 'pair')

    part_given = False


MLP_PLAN = (60, [
    512, 769, 964, 1029, 1154, 1352, 1417, 1414, 1549, 1539, 1674, 1799, 1934, 1932, 1937, 1995, 2002, 2064,
    2127, 2133, 2198, 2196, 2195, 2265, 2330, 2653, 2647, 2712, 2846, 2907, 3170, 3169, 3164, 3295, 3365,
    3488, 3494, 3555, 3684, 3751])
ATT_PLAN = (60, [
    1089, 1605, 1664, 1865, 1860, 2061, 2051, 2257, 2248, 2247, 2389, 2380, 2370, 2512, 2571, 2566, 2703,
    2708, 2713, 2771, 2762, 2840, 3022, 3037, 3218, 3223, 3228, 3297, 3286, 3291, 3424, 3418, 3429, 3551,
    3620, 3678, 3683, 3746, 3751, 3814])
VMEM_LIMIT = 64 * 1024 * 1024 - 64 * 1024


def dot(a, b, ca=1, cb=0):
    return lax.dot_general(a, b, (((ca,), (cb,)), ((), ())), preferred_element_type=F32)


def mlp_stage(n, h1, dy, x, stats, gain, gain_x, w_up, w_down, w_qkv, width, cid):
    rows, cols = h1.shape
    ffn = w_up.shape[1]
    comm = Comm(n, rows, cols)
    tile = comm.half
    n_tiles = rows // tile
    cb = 384
    n_cols = cols // cb
    hd = width + -width % 128
    qkv_w = 3 * hd
    dw_end = n_tiles + n_cols
    wide = 2 * tile
    grid = dw_end + rows // wide
    points = []
    for i in range(n_tiles):
        points += [(1.5 if i else 7.0, []), (0.9, []), (2.0, [(i // 2, 'pair' if i % 2 == 0 else 'own')])]
    for i in range(n_cols):
        points += [(1.0, []), (1.5, []), (1.2, [])]
    points += [(2.8, []), (0.0, []), (0.0, [])] * (rows // wide)
    plans = comm.tuned(MLP_PLAN, points)

    def kernel(h1_tile, dy_tile, h1_col, dy_col, x_tile, w1, w2, mean2, rstd2, mean1, rstd1, gain_ref, gain_x_ref,
               wqkv_in, h1_all, dy_all, dh1_ref, dw1_ref, dw2_ref, qkv_ref, act, da, wqkv, gx, wsem, *scratch):
        comm.bind(None, h1_all, dy_all, (mean2, rstd2, mean1, rstd1), gain_ref, dh1_ref, scratch)
        i = pl.program_id(0)
        full, own = comm.full, comm.own

        def ticks(steps, k):
            if any(plans[step * 3 + k] for step in steps):
                @pl.when(jnp.logical_and(i >= steps[0], i <= steps[-1]))
                def _():
                    for step in steps:
                        todo = plans[step * 3 + k]
                        if todo:
                            @pl.when(i == step)
                            def _():
                                for name, s in todo:
                                    getattr(comm, name)(s)

        loads = [pltpu.make_async_copy(wqkv_in.at[pl.ds(c * width, width), :], wqkv.at[pl.ds(c * hd, width), :],
                                       wsem.at[c]) for c in range(3)]

        @pl.when(i == 0)
        def _():
            for load in loads:
                load.start()
            for c in range(3):
                wqkv[pl.ds(c * hd + width, hd - width), :] = jnp.zeros((hd - width, cols), BF16)
            gx[...] = gain_x_ref[...].astype(F32)[None, :]
            comm.begin()

        first = range(n_tiles)
        rest = range(n_tiles, dw_end)
        last = range(dw_end, grid)
        tidx = lax.div(i, 2) * 2 + lax.rem(i, 2) * comm.core + (1 - lax.rem(i, 2)) * (1 - comm.core)
        trow = pl.ds(pl.multiple_of(tidx * tile, tile), tile)
        pre_ref, dg_ref = comm.pre, comm.dg

        @pl.when(i < n_tiles)
        def _():
            n2 = (comm.normed(h1_tile[...], trow, 0) * comm.gain[...]).astype(BF16)
            pre_ref[...] = dot(n2, w1[...])
        ticks(first, 0)

        @pl.when(i < n_tiles)
        def _():
            dg_ref[...] = dot(dy_tile[...], w2[...], 1, 1)
        ticks(first, 1)

        @pl.when(i < n_tiles)
        def _():
            pre = pre_ref[...]
            act[trow, :] = gelu_tanh(pre).astype(BF16)
            grad_pre = (dg_ref[...] * gelu_slope(pre)).astype(BF16)
            da[trow, :] = grad_pre
            part = dot(grad_pre, w1[...], 1, 1).astype(BF16)

            @pl.when(lax.rem(i, 2) == 0)
            def _():
                full[trow, :] = part

            @pl.when(lax.rem(i, 2) == 1)
            def _():
                own[lax.div(i, 2)] = part
        ticks(first, 2)

        @pl.when(jnp.logical_and(i >= n_tiles, i < dw_end))
        def _():
            c0 = pl.multiple_of((i - n_tiles) * cb, cb)
            comm.n2c[...] = (comm.normed(h1_col[...], pl.ds(0, rows), 0) * comm.gain[:, pl.ds(c0, cb)]).astype(BF16)
        ticks(rest, 0)

        @pl.when(jnp.logical_and(i >= n_tiles, i < dw_end))
        def _():
            dw1_ref[...] = dot(comm.n2c[...], da[...], 0, 0).astype(BF16)
        ticks(rest, 1)

        @pl.when(jnp.logical_and(i >= n_tiles, i < dw_end))
        def _():
            dw2_ref[...] = dot(act[...], dy_col[...], 0, 0).astype(BF16)
        ticks(rest, 2)

        @pl.when(i == dw_end)
        def _():
            for load in loads:
                load.wait()

        @pl.when(i >= dw_end)
        def _():
            xrow = pl.ds(pl.multiple_of((i - dw_end) * wide, wide), wide)
            n1 = (comm.normed(x_tile[...], xrow, 2) * gx[...]).astype(BF16)
            qkv_ref[...] = dot(n1, wqkv[...], 1, 1).astype(BF16)
        ticks(last, 0)
        ticks(last, 1)
        ticks(last, 2)

        @pl.when(i == grid - 1)
        def _():
            comm.end()

    def wrapped(*refs):
        *most, pre, dg, n2c = refs
        comm.pre, comm.dg, comm.n2c = pre, dg, n2c
        kernel(*most)

    def tile_map(i):
        core = lax.rem(lax.axis_index('tp'), 2)
        ii = jnp.minimum(i, n_tiles - 1)
        odd = lax.rem(ii, 2)
        return lax.div(ii, 2) * 2 + odd * core + (1 - odd) * (1 - core), 0

    def col_at(i):
        return jnp.clip(i - n_tiles, 0, n_cols - 1)

    def x_at(i):
        return jnp.maximum(i - dw_end, 0), 0

    whole = pl.BlockSpec(memory_space=VMEM)
    hbm = pl.BlockSpec(memory_space=ANY)
    return pl.pallas_call(
        wrapped,
        grid=(grid,),
        out_shape=(jax.ShapeDtypeStruct((rows, cols), BF16), jax.ShapeDtypeStruct((cols, ffn), BF16),
                   jax.ShapeDtypeStruct((ffn, cols), BF16), jax.ShapeDtypeStruct((rows, qkv_w), BF16)),
        in_specs=[pl.BlockSpec((tile, cols), tile_map), pl.BlockSpec((tile, cols), tile_map),
                  pl.BlockSpec((rows, cb), lambda i: (0, col_at(i))), pl.BlockSpec((rows, cb), lambda i: (0, col_at(i))),
                  pl.BlockSpec((wide, cols), x_at), whole, whole] + [whole] * 6 + [hbm] * 3,
        out_specs=(hbm, pl.BlockSpec((cb, ffn), lambda i: (col_at(i), 0)),
                   pl.BlockSpec((ffn, cb), lambda i: (0, col_at(i))), pl.BlockSpec((wide, qkv_w), x_at)),
        scratch_shapes=[VMEM((rows, ffn), BF16), VMEM((rows, ffn), BF16), VMEM((qkv_w, cols), BF16), VMEM((1, cols), F32),
                        pltpu.SemaphoreType.DMA((3,))] + comm.scratch()
        + [VMEM((tile, ffn), F32), VMEM((tile, ffn), F32), VMEM((rows, cb), BF16)],
        compiler_params=pltpu.CompilerParams(collective_id=cid, has_side_effects=True, vmem_limit_bytes=VMEM_LIMIT,
                                             dimension_semantics=('arbitrary',)),
        name='mlp_stage',
    )(h1, dy, h1, dy, x, w_up, w_down, *stats, gain, gain_x, w_qkv, h1, dy)


def attention_stage(n, mbs, x, dh1, qkv_all, stats, gain, w_qkv, w_out, score_scale, cid):
    rows, cols = x.shape
    seq = rows // mbs
    width = w_out.shape[0]
    hd = width + -width % 128
    qkv_w = 3 * hd
    comm = Comm(n, rows, cols)
    tile = comm.half
    per_mb = seq // tile
    wide = 2 * tile
    lead = seq // wide
    span = lead + per_mb
    n_seq = span * mbs
    cb = 384
    n_cols = cols // cb
    grid = n_seq + n_cols
    points = []
    for b in range(mbs):
        points += [(0.0, []), (1.4, []), (0.0, [])] * lead
        for j in range(per_mb - 1, -1, -1):
            s = b * (per_mb // 2) + j // 2
            points += [(1.0, []), (0.9, []), (1.45, [(s, 'pair'), (s, 'own')] if j % 2 == 0 else [])]
    for i in range(n_cols):
        points += [(1.05, []), (1.5, []), (0.55, [])]
    points[0] = (5.5, [])
    plans = comm.tuned(ATT_PLAN, points)

    def kernel(dh_tile, x_col, dh_col, qkv, wqkv_in, wo_in, mean_ref, rstd_ref, gain_ref, x_all, dh_all,
               dx_ref, dwqkv_ref, dwo_ref, do, o_all, dqkv, dk_acc, dv_acc, n1c, p_ref, wqkv, wo, wsem, *scratch):
        comm.bind(None, x_all, dh_all, (mean_ref, rstd_ref), gain_ref, dx_ref, scratch)
        i = pl.program_id(0)
        full, own = comm.full, comm.own

        def ticks(steps, k):
            if any(plans[step * 3 + k] for step in steps):
                @pl.when(jnp.logical_and(i >= steps[0], i <= steps[-1]))
                def _():
                    for step in steps:
                        todo = plans[step * 3 + k]
                        if todo:
                            @pl.when(i == step)
                            def _():
                                for name, s in todo:
                                    getattr(comm, name)(s)

        @pl.when(i == 0)
        def _():
            loads = [pltpu.make_async_copy(wqkv_in.at[pl.ds(c * width, width), :], wqkv.at[pl.ds(c * hd, width), :],
                                           wsem.at[c]) for c in range(3)]
            loads.append(pltpu.make_async_copy(wo_in, wo.at[pl.ds(0, width), :], wsem.at[3]))
            for load in loads:
                load.start()
            zero = jnp.zeros((hd - width, cols), BF16)
            for c in range(3):
                wqkv[pl.ds(c * hd + width, hd - width), :] = zero
            wo[pl.ds(width, hd - width), :] = zero
            comm.begin()
            for load in loads:
                load.wait()

        first = range(n_seq)
        rest = range(n_seq, grid)
        b = lax.div(i, span)
        at = lax.rem(i, span)
        in_seq = i < n_seq
        loading = jnp.logical_and(in_seq, at < lead)
        base = b * seq
        trow = pl.ds(pl.multiple_of(jnp.minimum(base + at * wide, rows - wide), wide), wide)

        def variants(fn):
            for j in range(per_mb):
                @pl.when(jnp.logical_and(in_seq, at == span - 1 - j))
                def _():
                    fn(j)

        def part_a(j):
            size = (j + 1) * tile
            mine = pl.ds(pl.multiple_of(base + j * tile, tile), tile)
            keys = pl.ds(pl.multiple_of(base, tile), size)
            s = dot(qkv[mine, 0:hd], qkv[keys, hd:2 * hd], 1, 1) * score_scale
            row = lax.broadcasted_iota(jnp.int32, (tile, size), 0) + j * tile
            col = lax.broadcasted_iota(jnp.int32, (tile, size), 1)
            s = jnp.where(row >= col, s, -1e30)
            e = jnp.exp(s - jnp.max(s, axis=-1, keepdims=True))
            p = e / jnp.sum(e, axis=-1, keepdims=True)
            p_ref[:, 0:size] = p
            pb = p.astype(BF16)
            o_all[mine, :] = dot(pb, qkv[keys, 2 * hd:3 * hd]).astype(BF16)
            dv = dot(pb, do[mine, :], 0, 0)
            if j == per_mb - 1:
                dv_acc[...] = dv
            else:
                dv_acc[0:size, :] += dv

        def part_b(j):
            size = (j + 1) * tile
            mine = pl.ds(pl.multiple_of(base + j * tile, tile), tile)
            keys = pl.ds(pl.multiple_of(base, tile), size)
            p = p_ref[:, 0:size]
            dp = dot(do[mine, :], qkv[keys, 2 * hd:3 * hd], 1, 1)
            rd = jnp.sum(p * dp, axis=-1, keepdims=True)
            ds = (p * (dp - rd) * score_scale).astype(BF16)
            dqkv[mine, 0:hd] = dot(ds, qkv[keys, hd:2 * hd]).astype(BF16)
            dk = dot(ds, qkv[mine, 0:hd], 0, 0)
            if j == per_mb - 1:
                dk_acc[...] = dk
            else:
                dk_acc[0:size, :] += dk
            dqkv[mine, hd:2 * hd] = dk_acc[j * tile:size, :].astype(BF16)
            dqkv[mine, 2 * hd:3 * hd] = dv_acc[j * tile:size, :].astype(BF16)

        def part_c(j):
            mine = pl.ds(pl.multiple_of(base + j * tile, tile), tile)
            part = dot(dqkv[mine, :], wqkv[...]).astype(BF16)

            @pl.when(comm.core == j % 2)
            def _():
                own[b * (per_mb // 2) + j // 2] = part

            @pl.when(comm.core != j % 2)
            def _():
                full[mine, :] = part

        variants(part_a)
        ticks(first, 0)

        @pl.when(loading)
        def _():
            do[trow, :] = dot(dh_tile[...], wo[...], 1, 1).astype(BF16)

        variants(part_b)
        ticks(first, 1)
        variants(part_c)
        ticks(first, 2)

        @pl.when(i >= n_seq)
        def _():
            c0 = pl.multiple_of((i - n_seq) * cb, cb)
            n1c[...] = (comm.normed(x_col[...], pl.ds(0, rows), 0) * comm.gain[:, pl.ds(c0, cb)]).astype(BF16)
        ticks(rest, 0)

        @pl.when(i >= n_seq)
        def _():
            dwqkv_ref[...] = dot(dqkv[...], n1c[...], 0, 0).astype(BF16)
        ticks(rest, 1)

        @pl.when(i >= n_seq)
        def _():
            dwo_ref[...] = dot(o_all[...], dh_col[...], 0, 0).astype(BF16)
        ticks(rest, 2)

        @pl.when(i == grid - 1)
        def _():
            comm.end()

    def tile_map(i):
        ii = jnp.minimum(i, n_seq - 1)
        return lax.div(ii, span) * lead + jnp.minimum(lax.rem(ii, span), lead - 1), 0

    def col_at(i):
        return jnp.maximum(i - n_seq, 0)

    whole = pl.BlockSpec(memory_space=VMEM)
    hbm = pl.BlockSpec(memory_space=ANY)
    return pl.pallas_call(
        kernel,
        grid=(grid,),
        out_shape=(VMEM((rows, cols), BF16), jax.ShapeDtypeStruct((qkv_w, cols), BF16),
                   jax.ShapeDtypeStruct((hd, cols), BF16)),
        in_specs=[pl.BlockSpec((wide, cols), tile_map),
                  pl.BlockSpec((rows, cb), lambda i: (0, col_at(i))), pl.BlockSpec((rows, cb), lambda i: (0, col_at(i))),
                  whole, hbm, hbm, whole, whole, whole, hbm, hbm],
        out_specs=(hbm, pl.BlockSpec((qkv_w, cb), lambda i: (0, col_at(i))),
                   pl.BlockSpec((hd, cb), lambda i: (0, col_at(i)))),
        scratch_shapes=[VMEM((rows, hd), BF16), VMEM((rows, hd), BF16),
                        VMEM((rows, qkv_w), BF16), VMEM((seq, hd), F32), VMEM((seq, hd), F32), VMEM((rows, cb), BF16),
                        VMEM((tile, seq), F32), VMEM((qkv_w, cols), BF16), VMEM((hd, cols), BF16),
                        pltpu.SemaphoreType.DMA((4,))] + comm.scratch(),
        compiler_params=pltpu.CompilerParams(collective_id=cid, has_side_effects=True, vmem_limit_bytes=VMEM_LIMIT - rows * cols * 2 - 256 * 1024,
                                             dimension_semantics=('arbitrary',)),
        name='attention_stage',
    )(dh1, x, dh1, qkv_all, w_qkv, w_out, *stats, gain, x, dh1)


def spread_copy(dx, dw_up, dw_down, dw_qkv, dw_out, width):
    def rows_of(arr, parts):
        step = arr.shape[0] // parts
        return [(k * step, k * step, step) for k in range(parts)]

    hd = dw_out.shape[0]
    srcs = (dx, dw_up, dw_down, dw_qkv, dw_out)
    moves = (rows_of(dx, 8), rows_of(dw_up, 2), rows_of(dw_down, 2), [(c * hd, c * width, width) for c in range(3)],
             [(0, 0, width)])
    outs = [jax.ShapeDtypeStruct((sum(m[2] for m in mv), a.shape[1]), a.dtype) for a, mv in zip(srcs, moves)]
    total = sum(len(mv) for mv in moves)

    def kernel(*refs):
        ins, dsts, bufs, (in_sem, out_sem) = refs[:5], refs[5:10], (refs[0],) + refs[10:14], refs[14:]
        reads, writes = [], []
        for a, mv in enumerate(moves):
            for frm, to, size in mv:
                k = len(reads)
                here = bufs[a].at[pl.ds(to, size), :]
                reads.append(pltpu.make_async_copy(ins[a].at[pl.ds(frm, size), :], here, in_sem.at[k]) if a else None)
                writes.append(pltpu.make_async_copy(here, dsts[a].at[pl.ds(to, size), :], out_sem.at[k]))
        for read in reads:
            if read is not None:
                read.start()
        for read, write in zip(reads, writes):
            if read is not None:
                read.wait()
            write.start()
        for write in writes:
            write.wait()

    hbm = pl.BlockSpec(memory_space=ANY)
    return pl.pallas_call(
        kernel,
        out_shape=outs,
        in_specs=[pl.BlockSpec(memory_space=VMEM)] + [hbm] * 4,
        out_specs=[hbm] * 5,
        scratch_shapes=[VMEM(o.shape, o.dtype) for o in outs[1:]]
        + [pltpu.SemaphoreType.DMA((total,)), pltpu.SemaphoreType.DMA((total,))],
        compiler_params=pltpu.CompilerParams(vmem_limit_bytes=32 * 1024 * 1024),
        name='spread_copy',
    )(*srcs)


def solution(mesh):
    act_spec = P('dp', None, None)
    stat_spec = P('dp', None)
    in_specs = (act_spec, act_spec, act_spec, stat_spec, stat_spec, stat_spec, stat_spec, P(), P(),
                P(None, 'tp', None, None), P('tp', None, None), P(None, 'tp'), P('tp', None))
    out_specs = (act_spec, P('dp', 'tp', None, None), P(('dp', 'tp'), None, None), P('dp', 'tp'),
                 P(('dp', 'tp'), None))
    n = mesh.shape['tp']

    def local_backward(x_saved, h1_saved, grad_y, mean_one, rstd_one, mean_two, rstd_two,
                       gain_one, gain_two, w_qkv, w_out, w_up, w_down):
        score_scale = w_qkv.shape[3] ** -0.5
        shape = x_saved.shape
        flat = (shape[0] * shape[1], shape[2])
        heads, _, width = w_qkv.shape[1:]
        rows_qkv = w_qkv.transpose(1, 2, 3, 0).reshape(3 * width, flat[1])
        h1, dy, x = h1_saved.reshape(flat), grad_y.reshape(flat), x_saved.reshape(flat)
        dh1, grad_up, grad_down, qkv = mlp_stage(n, h1, dy, x, (mean_two, rstd_two, mean_one, rstd_one), gain_two,
                                                 gain_one, w_up, w_down, rows_qkv, width, 0)
        dx, dqkv_w, dout_w = attention_stage(n, shape[0], x, dh1, qkv, (mean_one, rstd_one), gain_one, rows_qkv,
                                             w_out[0], score_scale, 1)
        dx, grad_up, grad_down, dqkv_w, dout_w = spread_copy(dx, grad_up, grad_down, dqkv_w, dout_w, width)
        grad_qkv_w = dqkv_w.reshape(heads, 3, width, flat[1]).transpose(3, 0, 1, 2)
        return dx.reshape(shape), grad_qkv_w, dout_w[None], grad_up, grad_down

    return jax.shard_map(local_backward, mesh=mesh, in_specs=in_specs, out_specs=out_specs, check_vma=False)
```
